128 devices in a mesh: gz: 128 (over y, z, x, core).
Axes of the slice: x: 4, y: 4, z: 4, core: 2. Of those that a mesh axis runs over, the one named last changes fastest.
Arguments:
- marker_positions: float32 [16384, 3, 256], P('gz'), may hold values from 0 to 1
- marker_forces: float32 [16384, 3, 256], P('gz'), may hold values from -48 to 48
- dest_slab: int32 [16384, 1], P('gz'), may hold values from 0 to 127; in each aligned block of 128 rows (0 to 127, 128 to 255, ...) at most 2 rows name the same one
- base_cells: int32 [16384, 2], P('gz'), may hold values from 0 to 127
- fluid_source: float32 [512, 3, 128, 128], P('gz'), may hold values from -7 to 7
Outputs:
- velocity: float32 [512, 3, 128, 128], P('gz')
- marker_velocity: float32 [16384, 3, 256], P('gz')
The draws below stay inside these ranges and needn't reach their ends.
Inputs may be any that keep to these rules, and one draw needn't show every extreme that they name: `dest_slab`: among the blocks of one device no slab is named more than 2 times.
All inputs are finite; a program needn't handle non-finite values.
Results may differ from the reference program's by a relative error of at most 0.00096.
Values may be sent and summed in bfloat16 or wider, within the bound.
No kernel may reach another device: no remote copies, remote signals or barrier semaphores. Data moves between devices by JAX's collectives and lax.ppermute only.
A program may use at most 256 MiB of HBM per device.

```python
import math
import jax
import jax.numpy as jnp
import numpy as np
from jax import lax

CELLS_XY = 128
CZ = 4
NZ = 512
BLK_DEV = 128
BLOCKS = 16384
MARK = 256
BOX = 16
CAP = 2
SWEEPS = 2
CSWEEPS = 6
N_GZ = 128


def draw_fluid_source(key, part):
    rough_key, level_key = jax.random.split(jax.random.fold_in(key, 11))
    rough = jax.random.truncated_normal(rough_key, -6.0, 6.0, (NZ, 3, CELLS_XY, CELLS_XY), jnp.float32)
    levels = jax.random.uniform(level_key, (NZ // CZ,), jnp.float32, 0.01, 0.05)
    return rough + jnp.repeat(levels, CZ)[:, None, None, None]


def with_ends(drawn, stream_key, smallest, high):
    spot = [jax.random.randint(jax.random.fold_in(stream_key, axis), (), 0, length) for axis, length in enumerate(drawn.shape)]
    main_axis = drawn.shape.index(max(drawn.shape))
    neighbour = spot[:main_axis] + [(spot[main_axis] + 1) % drawn.shape[main_axis]] + spot[main_axis + 1:]
    return drawn.at[tuple(spot)].set(smallest).at[tuple(neighbour)].set(high)


def steps_of(stream_key, shape, cuts, least, top_value):
    gain = 1.0
    for position, shards_of in cuts:
        steps = jax.random.uniform(jax.random.fold_in(jax.random.fold_in(stream_key, 6), position), (shards_of,), jnp.float32, least / len(cuts), top_value / len(cuts))
        gain = gain * jnp.repeat(jnp.exp(steps), shape[position] // shards_of).reshape((-1,) + (1,) * (len(shape) - 1 - position))
    return gain


def shared_out(own_key, own, number, rows, number_of, top, most, lean):
    sequence = jax.random.permutation(own_key, number_of)
    heavy_load, ordinary = shares(number_of, rows * top, most, lean, True), shares(number_of, rows * top, most, lean, False)
    places = jnp.arange(number_of)

    def named(tallies, offset_by):
        used = int((tallies > 0).sum())
        fixed = max(1, used // 4)
        moved = fixed + (places - fixed + offset_by * (used - fixed)) % max(1, number_of - fixed)
        return jnp.zeros((number_of,), jnp.int32).at[sequence[jnp.where(places < fixed, places, moved)]].set(jnp.asarray(tallies, jnp.int32))

    tallies = jnp.where(number % 4 == 0, named(heavy_load, number // 4), named(ordinary, number - number // 4 - 1))
    mixed = jax.random.permutation(jax.random.fold_in(own, 3), number_of)
    giver, taker = mixed[0:number_of // 2 * 2:2], mixed[1:number_of // 2 * 2:2]
    margin = jnp.minimum(tallies[giver] - 1, most - tallies[taker]) // 2
    margin = jnp.where((giver == sequence[0]) | (taker == sequence[0]) | (tallies[taker] == 0), 0, jnp.maximum(margin, 0))
    moved = jax.random.randint(jax.random.fold_in(own, 4), (number_of // 2,), 0, 1 << 20) % (margin + 1)
    tallies = tallies.at[giver].add(-moved).at[taker].add(moved)
    labels = jnp.searchsorted(jnp.cumsum(tallies), jnp.arange(rows * top), side="right").astype(jnp.int32)
    grid = labels.reshape(top, rows).T
    grid = grid[jax.random.permutation(jax.random.fold_in(own, 1), rows)]
    offset_by = jax.random.randint(jax.random.fold_in(own, 2), (rows, 1), 0, top)
    return jnp.take_along_axis(grid, (jnp.arange(top)[None, :] + offset_by) % top, axis=1)


def shares(count, total, bound, slope, full):
    loads = [(1 << 20) // math.isqrt(standing ** slope) + 1 for standing in range(1, count + 1)]
    largest = bound if full else min(bound, max(-(-total // count), total * loads[0] // sum(loads)))
    least = 1 if total - largest >= count - 1 else 0
    counts, rest = [largest] + [least] * (count - 1), total - largest - least * (count - 1)
    while rest > 0:
        movable = [i for i in range(1, count) if counts[i] < largest] or [i for i in range(1, count) if counts[i] < bound]
        whole, left = sum([loads[i] for i in movable]), rest
        for i in movable:
            more = min(bound - counts[i], max(1, left * loads[i] // whole), rest)
            counts[i] = counts[i] + more
            rest = rest - more
    return np.array(counts)


def normal_values(own_key, extent, deviation, reach, cuts=(), kind=jnp.bfloat16):
    loudness = steps_of(own_key, extent, cuts, -0.22, 0.18) if cuts else 1.0
    values = jax.random.normal(own_key, extent, jnp.float32) * deviation * loudness
    return jnp.minimum(jnp.maximum(values, -reach), reach).astype(kind)


def setup_inputs(seed: int = 0) -> dict:
    streams_of = jax.random.split(jax.random.key(seed), 6)
    marker_positions = jnp.clip(1.0 * jax.random.uniform(streams_of[0], (BLOCKS, 3, MARK), jnp.float32) ** steps_of(streams_of[0], (BLOCKS, 3, MARK), ((0, 128),), -0.2, 0.2), 0.0, 1.0)
    marker_forces = normal_values(streams_of[1], (BLOCKS, 3, MARK), 8.0, 48.0, ((0, 128),), jnp.float32)
    dest_slab_keys = jax.random.split(jax.random.fold_in(streams_of[2], 1), BLOCKS // BLK_DEV)
    dest_slab_turns = jax.random.permutation(jax.random.fold_in(streams_of[2], 3), BLOCKS // BLK_DEV)
    dest_slab = jax.vmap(lambda own, number: shared_out(jax.random.fold_in(streams_of[2], 2), own, number, BLK_DEV, N_GZ, 1, CAP, 2))(dest_slab_keys, dest_slab_turns).reshape((BLOCKS, 1))
    base_cells = with_ends(jax.random.randint(streams_of[3], (BLOCKS, 2), 0, CELLS_XY), jax.random.fold_in(streams_of[3], 1), 0, CELLS_XY - 1).astype(jnp.int32)
    fluid_source = draw_fluid_source(jax.random.fold_in(streams_of[5], 71), 0)
    return {"marker_positions": marker_positions, "marker_forces": marker_forces, "dest_slab": dest_slab, "base_cells": base_cells, "fluid_source": fluid_source}


screening = 1.0 / 64.0
relaxation = 2.0 / 3.0


def kernel_phi(offset):
    inside = jnp.abs(offset) < 2.0
    return jnp.where(inside, 0.25 * (1.0 + jnp.cos(0.5 * jnp.pi * offset)), 0.0 * offset)


def kernel_tables(positions):
    box_cells = jnp.arange(BOX, dtype=positions.dtype)
    slab_cells = jnp.arange(CZ, dtype=positions.dtype)
    across = 2.0 + (BOX - 5) * positions[:, 0, :]
    along_y = 2.0 + (BOX - 5) * positions[:, 1, :]
    height = (CZ - 1) * positions[:, 2, :]
    weight_x = kernel_phi(across[:, :, None] - box_cells)
    weight_y = kernel_phi(along_y[:, :, None] - box_cells)
    weight_z = kernel_phi(height[:, :, None] - slab_cells)
    plane_weight = (weight_x[:, :, :, None] * weight_y[:, :, None, :]).reshape(positions.shape[0], positions.shape[2], BOX * BOX)
    return weight_z, plane_weight


def build_boxes(positions, forces):
    weight_z, plane_weight = kernel_tables(positions)
    loaded = jnp.einsum('bmk,bcm->bkcm', weight_z, forces, precision=lax.Precision.HIGHEST)
    box_values = jnp.einsum('bkcm,bmq->bkcq', loaded, plane_weight, precision=lax.Precision.HIGHEST)
    return box_values.reshape(positions.shape[0], -1).astype(jnp.bfloat16)


def read_boxes(positions, box_velocity):
    weight_z, plane_weight = kernel_tables(positions)
    block_total = positions.shape[0]
    box_values = box_velocity.astype(jnp.float32).reshape(block_total, CZ, 3, BOX * BOX)
    spread = jnp.einsum('bkcq,bmq->bkcm', box_values, plane_weight, precision=lax.Precision.HIGHEST)
    return jnp.einsum('bmk,bkcm->bcm', weight_z, spread, precision=lax.Precision.HIGHEST)


def grouped(function, arrays, group_rows):
    block_total = arrays[0].shape[0]
    stacked = tuple(member.reshape((block_total // group_rows, group_rows) + member.shape[1:]) for member in arrays)
    result = lax.map(lambda pieces: function(*pieces), stacked)
    return result.reshape((block_total,) + result.shape[2:])


def box_index(target, bases):
    layer_index = target[:, None] * CZ + jnp.arange(CZ, dtype=jnp.int32)[None, :]
    column_x = (bases[:, 0:1] + jnp.arange(BOX, dtype=jnp.int32)[None, :]) % CELLS_XY
    column_y = (bases[:, 1:2] + jnp.arange(BOX, dtype=jnp.int32)[None, :]) % CELLS_XY
    component = jnp.arange(3, dtype=jnp.int32)
    return (layer_index[:, :, None, None, None], component[None, None, :, None, None],
            column_x[:, None, None, :, None], column_y[:, None, None, None, :])


def operate(solution, level_index):
    beside = jnp.roll(solution, -1, 0) + jnp.roll(solution, 1, 0)
    beside = beside + jnp.roll(solution, -1, 2) + jnp.roll(solution, 1, 2)
    beside = beside + jnp.roll(solution, -1, 3) + jnp.roll(solution, 1, 3)
    return screening * solution - 0.25 ** level_index * (beside - 6.0 * solution)


def relax_factor(level_index):
    return relaxation / (screening + 6.0 * 0.25 ** level_index)


def restrict(solution):
    shape_now = solution.shape
    folded = solution.reshape(shape_now[0] // 2, 2, shape_now[1], shape_now[2] // 2, 2, shape_now[3] // 2, 2)
    return jnp.mean(folded, axis=(1, 4, 6))


def prolong(solution):
    return jnp.repeat(jnp.repeat(jnp.repeat(solution, 2, 0), 2, 2), 2, 3)


def descend(source, level_index):
    factor = relax_factor(level_index)
    solution = factor * source
    for sweep_turn in range(SWEEPS - 1):
        solution = solution + factor * (source - operate(solution, level_index))
    return solution, source - operate(solution, level_index)


def ascend(solution, source, level_index):
    factor = relax_factor(level_index)
    for sweep_turn in range(SWEEPS):
        solution = solution + factor * (source - operate(solution, level_index))
    return solution


def coarsest(source):
    factor = relax_factor(3)
    solution = factor * source
    for sweep_turn in range(CSWEEPS - 1):
        solution = solution + factor * (source - operate(solution, 3))
    leftover = source - operate(solution, 3)
    level_mean = jnp.mean(leftover, axis=(0, 2, 3), keepdims=True)
    return solution + level_mean / screening


def reference(marker_positions, marker_forces, dest_slab, base_cells, fluid_source):
    group_rows = math.gcd(BLOCKS, 256)
    own_boxes = grouped(build_boxes, (marker_positions, marker_forces), group_rows)
    target = dest_slab[:, 0]
    group_count = BLOCKS // group_rows

    def place(grid_sum, pieces):
        group_boxes, group_target, group_base = pieces
        box_values = group_boxes.astype(jnp.float32).reshape(group_rows, CZ, 3, BOX, BOX)
        grid_sum = grid_sum.at[box_index(group_target, group_base)].add(box_values)
        return grid_sum, None

    start_grid = jnp.zeros((NZ, 3, CELLS_XY, CELLS_XY), jnp.float32)
    force_grid, unused = lax.scan(place, start_grid, (
        own_boxes.reshape(group_count, group_rows, -1),
        target.reshape(group_count, group_rows),
        base_cells.reshape(group_count, group_rows, 2)))
    source = fluid_source + force_grid
    fine_sol, fine_res = descend(source, 0)
    middle_rhs = restrict(fine_res)
    middle_sol, middle_res = descend(middle_rhs, 1)
    third_rhs = restrict(middle_res)
    third_sol, third_res = descend(third_rhs, 2)
    coarse_sol = coarsest(restrict(third_res))
    third_sol = ascend(third_sol + prolong(coarse_sol), third_rhs, 2)
    middle_sol = ascend(middle_sol + prolong(third_sol), middle_rhs, 1)
    velocity = ascend(fine_sol + prolong(middle_sol), source, 0)
    velocity_low = velocity.astype(jnp.bfloat16)

    def pick(group_target, group_base):
        return velocity_low[box_index(group_target, group_base)].reshape(group_target.shape[0], -1)

    picked = grouped(pick, (target, base_cells), group_rows)
    marker_velocity = grouped(read_boxes, (marker_positions, picked), group_rows)
    return velocity, marker_velocity
```

```python
import jax
import jax.numpy as jnp
from jax import lax
from jax.experimental import pallas as pl
from jax.experimental.pallas import tpu as pltpu
from jax.sharding import PartitionSpec as P

AX = "gz"
BOX = 16
CZ = 4
ROWS = 24
SCREEN = 1.0 / 64.0
RELAX = 2.0 / 3.0
INTERPRET = False
F32 = jnp.float32
BF16 = jnp.bfloat16
HIGH = lax.Precision.HIGHEST


def level(index):
    q = 0.25**index
    return q, SCREEN + 6.0 * q, RELAX / (SCREEN + 6.0 * q)


def call(body, out_shape, in_specs=None, scratch=(), name=None, out_specs=None):
    options = {}
    if in_specs is not None:
        options["in_specs"] = in_specs
    if out_specs is not None:
        options["out_specs"] = out_specs
    return pl.pallas_call(
        body,
        out_shape=out_shape,
        scratch_shapes=list(scratch),
        name=name,
        interpret=INTERPRET,
        **options,
    )


VMEM = pl.BlockSpec(memory_space=pltpu.VMEM)
SMEM = pl.BlockSpec(memory_space=pltpu.SMEM)


def iota(shape, dim):
    return lax.broadcasted_iota(jnp.int32, shape, dim)


COS = (
    0.99999999999999999,
    -0.30842513753404244,
    0.015854344243815498,
    -0.00032599188692738954,
    3.5908604459003885e-06,
    -2.4611369504941976e-08,
    1.1500234922e-10,
)


def phi(offset):
    square = jnp.minimum(offset * offset, 4.0)
    value = jnp.full_like(square, COS[-1])
    for coefficient in COS[-2::-1]:
        value = value * square + coefficient
    value = 0.5 * (value * value)
    return jnp.where(square < 4.0, value, 0.0)


def split(value):
    high = value.astype(BF16)
    return high, (value - high.astype(F32)).astype(BF16)


def box_weights(pos_ref, block):
    cells = iota((BOX, 256), 0).astype(F32)
    levels = iota((8, 256), 0).astype(F32)
    row = pl.ds(block, 1)
    along_x = 2.0 + (BOX - 5) * pos_ref[0, row, :]
    along_y = 2.0 + (BOX - 5) * pos_ref[1, row, :]
    height = (CZ - 1) * pos_ref[2, row, :]
    return phi(along_x - cells), phi(along_y - cells), phi(height - levels)


def build_kernel(dest_ref, base_ref, pos_ref, frc_ref, out_ref, stage_ref, count_ref):
    slots = out_ref.shape[0]
    blocks = pos_ref.shape[1]

    def clear(t, carry):
        count_ref[t] = 0
        stage_ref[t] = jnp.zeros((2 * ROWS, 128), F32)
        return carry

    lax.fori_loop(0, slots, clear, 0)
    lane = iota((8, 128), 1)
    sub = iota((8, 128), 0)

    def one(block, carry):
        weight_x, weight_y, weight_z = box_weights(pos_ref, block)
        parts = []
        loaded = [weight_z * frc_ref[c, pl.ds(block, 1), :] for c in range(3)]
        for k in range(CZ):
            for c in range(3):
                parts.append(loaded[c][k : k + 1, :] * weight_x)
        whole = jnp.concatenate(parts, axis=0)
        high, low = split(whole)
        right = jnp.concatenate(split(weight_y), axis=0)
        dims = (((1,), (1,)), ((), ()))
        first = lax.dot_general(high, right, dims, preferred_element_type=F32)
        second = lax.dot_general(low, right[:BOX], dims, preferred_element_type=F32)
        box = first[:, :BOX] + first[:, BOX:] + second
        target = dest_ref[0, block]
        order = count_ref[target]
        count_ref[target] = order + 1
        base_x = base_ref[0, block].astype(F32) + 1.0
        base_y = base_ref[1, block].astype(F32)
        for q in range(3):
            packed = jnp.concatenate(
                [box[(8 * q + g) * 8 : (8 * q + g + 1) * 8] for g in range(8)], axis=1
            )
            if q == 0:
                top = sub == 0
                packed = jnp.where(top & (lane == 0), base_x, packed)
                packed = jnp.where(top & (lane == BOX), base_y, packed)
            stage_ref[target, pl.ds(pl.multiple_of(order * ROWS + 8 * q, 8), 8), :] = packed
        return carry

    lax.fori_loop(0, blocks, one, 0, unroll=2)

    def finish(t, carry):
        out_ref[t] = stage_ref[t].astype(BF16)
        return carry

    lax.fori_loop(0, slots, finish, 0, unroll=4)


def build(dest, base, positions, forces, slots):
    return call(
        build_kernel,
        jax.ShapeDtypeStruct((slots, 2 * ROWS, 128), BF16),
        [SMEM, SMEM, VMEM, VMEM],
        [pltpu.VMEM((slots, 2 * ROWS, 128), F32), pltpu.SMEM((slots,), jnp.int32)],
        "build",
    )(dest, base, positions, forces)


def place_kernel(meta_ref, pay_ref, fluid_ref, src_ref, bottom_ref, top_ref, grid_ref):
    slots = pay_ref.shape[0]
    lane = iota((8, 128), 1)
    sub = iota((8, 128), 0)
    for z in range(CZ):
        for c in range(3):
            grid_ref[3 * z + c, 0:128, :] = fluid_ref[z, c]
            grid_ref[3 * z + c, 128:144, :] = jnp.zeros((16, 128), F32)

    def add(tile, base_x, base_y):
        shift = base_x & 7
        row = pl.multiple_of(base_x - shift, 8)
        window = (lane - base_y) & 127
        inside = (window >= 1) & (window <= BOX - 2)
        late = inside & (sub >= shift)
        early = inside & (sub < shift)
        rolled = [pltpu.roll(tile[8 * q : 8 * q + 8], shift, 0) for q in range(3)]
        for kc in range(12):
            v = 2 * kc
            first = pltpu.roll(rolled[v // 8], (base_y - BOX * (v % 8)) & 127, 1)
            second = pltpu.roll(rolled[v // 8], (base_y - BOX * (v % 8 + 1)) & 127, 1)
            grid_ref[kc, pl.ds(row, 8), :] += jnp.where(late, first, 0.0)
            grid_ref[kc, pl.ds(row + 8, 8), :] += jnp.where(
                early, first, jnp.where(late, second, 0.0)
            )
            grid_ref[kc, pl.ds(row + 16, 8), :] += jnp.where(early, second, 0.0)

    def source_of(d, carry):
        for order in range(2):

            @pl.when(meta_ref[4 * d + 2 * order] > 0)
            def _():
                tile = pay_ref[d].astype(F32)
                add(
                    tile[order * ROWS : (order + 1) * ROWS],
                    meta_ref[4 * d + 2 * order] - 1,
                    meta_ref[4 * d + 2 * order + 1],
                )

        return carry

    lax.fori_loop(0, slots, source_of, 0)
    for z in range(CZ):
        for c in range(3):
            kc = 3 * z + c
            grid_ref[kc, 0:16, :] += grid_ref[kc, 128:144, :]
            value = grid_ref[kc, 0:128, :]
            src_ref[z, c] = value
            if z < 3:
                bottom_ref[z, c] = value
            if z > 0:
                top_ref[z - 1, c] = value


def place(meta, payload, fluid):
    width = fluid.shape[2]
    return call(
        place_kernel,
        (
            jax.ShapeDtypeStruct(fluid.shape, F32),
            jax.ShapeDtypeStruct((3, 3, width, width), F32),
            jax.ShapeDtypeStruct((3, 3, width, width), F32),
        ),
        [SMEM, VMEM, VMEM],
        [pltpu.VMEM((12, 144, 128), F32)],
        "place",
    )(meta, payload, fluid)


def flat_ring(x):
    rows = x.shape[-2]
    ax = x.ndim - 2
    return (
        pltpu.roll(x, 1, ax)
        + pltpu.roll(x, rows - 1, ax)
        + (pltpu.roll(x, 1, ax + 1) + pltpu.roll(x, 127, ax + 1))
    )


def group_ring(x):
    rows = x.shape[-2]
    ax = x.ndim - 2
    lane = iota(x.shape, ax + 1) & 31
    before = jnp.where(lane == 0, pltpu.roll(x, 97, ax + 1), pltpu.roll(x, 1, ax + 1))
    after = jnp.where(lane == 31, pltpu.roll(x, 31, ax + 1), pltpu.roll(x, 127, ax + 1))
    return pltpu.roll(x, 1, ax) + pltpu.roll(x, rows - 1, ax) + (before + after)


def start_of(b, below, above, ring, index):
    q, _, w = level(index)
    return w * ((4.0 / 3.0) * b + (w * q) * (ring(b) + (below + above)))


def left_of(b, u, below, above, ring, index):
    q, diag, _ = level(index)
    return b - diag * u + q * (ring(u) + (below + above))


def sweep_of(b, u, below, above, ring, index):
    q, _, w = level(index)
    return (1.0 - RELAX) * u + (w * b + (w * q) * (ring(u) + (below + above)))


def dot(left, right):
    return lax.dot_general(
        left, right, (((1,), (0,)), ((), ())), precision=HIGH, preferred_element_type=F32
    )


def lanes(test):
    return test(iota((128, 128), 0), iota((128, 128), 1))


def fine_kernel(low_ref, own_ref, high_ref, out_ref, u_ref, sum_ref):
    def b_at(z, c):
        if z < 0:
            return low_ref[z + 3, c]
        return own_ref[z, c] if z < CZ else high_ref[z - CZ, c]

    pool = [
        jnp.where(
            lanes(lambda r, l: (r // 2 == (l & 63)) & (l // 64 == half)), 0.125, 0.0
        )
        for half in range(2)
    ]

    def component(c, carry):
        for z in range(-1, CZ + 1):
            u_ref[z + 1] = start_of(b_at(z, c), b_at(z - 1, c), b_at(z + 1, c), flat_ring, 0)
        total = None
        for half in range(2):
            for z in (2 * half, 2 * half + 1):
                value = left_of(
                    own_ref[z, c], u_ref[z + 1], u_ref[z], u_ref[z + 2], flat_ring, 0
                )
                sum_ref[...] = value if z == 2 * half else sum_ref[...] + value
            rows = sum_ref[pl.ds(0, 64, 2), :] + sum_ref[pl.ds(1, 64, 2), :]
            part = dot(rows, pool[half])
            total = part if total is None else total + part
        out_ref[c] = total
        return carry

    lax.fori_loop(0, 3, component, 0)


def fine_down(low, own, high):
    return call(
        fine_kernel,
        jax.ShapeDtypeStruct((3, 64, 128), F32),
        None,
        [pltpu.VMEM((CZ + 2, 128, 128), F32), pltpu.VMEM((128, 128), F32)],
        "fine_down",
    )(low, own, high)


def both_layers(tile):
    lane = iota(tile.shape, tile.ndim - 1)
    turned = pltpu.roll(tile, 64, tile.ndim - 1)
    return jnp.where(lane < 64, tile, turned), jnp.where(lane < 64, turned, tile)


def pack_coarse(value):
    last = value[24:32]
    lane = iota((8, 128), 1)
    return [
        jnp.where(lane < 96, value[8 * c : 8 * c + 8], pltpu.roll(last, 96 - 32 * c, 1))
        for c in range(3)
    ]


def unpack_coarse(tile):
    lane = iota((8, 128), 1)
    last = jnp.zeros((8, 128), F32)
    rows = []
    for c in range(3):
        piece = tile[8 * c : 8 * c + 8]
        turned = pltpu.roll(piece, (32 * c - 96) % 128, 1)
        last = jnp.where(lane // 32 == c, turned, last)
        rows.append(jnp.where(lane < 96, piece, 0.0))
    return jnp.concatenate(rows + [last], axis=0)


def middle_kernel(low_ref, own_ref, high_ref, out_ref, sum_ref):
    total = None
    for c in range(3):
        b = []
        for ref in (low_ref, own_ref, high_ref):
            b.extend(both_layers(ref[c]))
        u = [start_of(b[i], b[i - 1], b[i + 1], flat_ring, 1) for i in range(1, 5)]
        left = [left_of(b[i + 1], u[i], u[i - 1], u[i + 1], flat_ring, 1) for i in (1, 2)]
        sum_ref[...] = left[0] + left[1]
        rows = sum_ref[pl.ds(0, 32, 2), :] + sum_ref[pl.ds(1, 32, 2), :]
        pool = jnp.where(
            lanes(lambda r, l: (r // 2 == (l & 31)) & (l // 32 == c) & (r < 64)), 0.125, 0.0
        )
        part = dot(rows, pool)
        total = part if total is None else total + part
    packed = jnp.concatenate(pack_coarse(total), axis=0)

    def copy(d, carry):
        out_ref[d] = packed
        return carry

    lax.fori_loop(0, out_ref.shape[0], copy, 0, unroll=8)


def middle_down(low, own, high, slots):
    return call(
        middle_kernel,
        jax.ShapeDtypeStruct((slots, 24, 128), F32),
        None,
        [pltpu.VMEM((64, 128), F32)],
        "middle_down",
    )(low, own, high)


def inner(x):
    return x[1:-1]


def coarse_part(me, g2_ref, pool_ref, final_ref):
    slots = g2_ref.shape[0]
    parity = me % 2
    first = me - parity - 16 + 16 * slots
    b2 = jnp.stack([unpack_coarse(g2_ref[(first + t) % slots]) for t in range(34)])
    total = lax.fori_loop(
        0, slots, lambda d, sums: sums + g2_ref[d], jnp.zeros((24, 128), F32)
    )
    column = jnp.sum(unpack_coarse(total), axis=0, keepdims=True)
    same = jnp.where(lanes(lambda r, l: r // 32 == l // 32), 1.0, 0.0)
    mean_b2 = dot(jnp.broadcast_to(column, (8, 128)), same)[0:1] * (1.0 / (slots * 1024.0))
    _, _, w2 = level(2)
    q3, _, w3 = level(3)
    factor = (1.0 - w3 * SCREEN) ** 6 * (1.0 - w2 * SCREEN) ** 2 / SCREEN
    lift = mean_b2 * factor
    u2 = start_of(inner(b2), b2[:-2], b2[2:], group_ring, 2)
    r2 = left_of(b2[2:-2], inner(u2), u2[:-2], u2[2:], group_ring, 2)
    pairs = r2.reshape(15, 2, 32, 128)
    pool_ref[...] = (pairs[:, 0] + pairs[:, 1]).reshape(480, 128)
    rows = pool_ref[pl.ds(0, 240, 2), :] + pool_ref[pl.ds(1, 240, 2), :]
    pool = jnp.where(
        lanes(lambda r, l: ((r & 31) // 2 == (l & 15)) & (r // 32 == l // 32)), 0.125, 0.0
    )
    b3 = dot(rows, pool).reshape(15, 16, 128)
    u3 = w3 * b3
    for _ in range(5):
        b3 = inner(b3)
        u3 = sweep_of(b3, inner(u3), u3[:-2], u3[2:], group_ring, 3)
    u3 = (u3 + lift[None]).reshape(80, 128)
    spread = jnp.where(
        lanes(lambda r, l: ((l & 31) // 2 == (r & 31)) & (r // 32 == l // 32)), 1.0, 0.0
    )
    wide = dot(u3, spread)
    pool_ref[pl.ds(0, 80, 2), :] = wide
    pool_ref[pl.ds(1, 80, 2), :] = wide
    lifted = pool_ref[0:160, :].reshape(5, 1, 32, 128)
    u = (u2[11:21].reshape(5, 2, 32, 128) + lifted).reshape(10, 32, 128)
    u = sweep_of(b2[13:21], inner(u), u[:-2], u[2:], group_ring, 2)
    u = sweep_of(b2[14:20], inner(u), u[:-2], u[2:], group_ring, 2)
    final_ref[...] = u
    return jnp.concatenate([final_ref[parity + h] for h in range(5)], axis=0)


def up_kernel(
    me_ref, meta_ref, g2_ref, m2_ref, m1_ref, m0_ref, p1_ref, p2_ref, low_ref, own_ref,
    high_ref, vel_ref, pay_ref,
    pool_ref, final_ref, lift1_ref, b1_ref, u1_ref, v1_ref, lift0_ref, u0_ref, v0_ref,
    ext_ref, stage_ref,
):
    coarse = coarse_part(me_ref[0], g2_ref, pool_ref, final_ref)
    for c in range(3):
        spread = jnp.where(lanes(lambda r, l: r == 32 * c + (l & 63) // 2), 1.0, 0.0)
        wide = dot(coarse, spread)
        lift1_ref[c, pl.ds(0, 160, 2), :] = wide
        lift1_ref[c, pl.ds(1, 160, 2), :] = wide
    spread0 = jnp.where(lanes(lambda r, l: r == l // 2), 1.0, 0.0)

    def b_at(z, c):
        if z < 0:
            return low_ref[z + 3, c]
        return own_ref[z, c] if z < CZ else high_ref[z - CZ, c]

    def component(c, carry):
        for j, ref in enumerate((m2_ref, m1_ref, m0_ref, p1_ref, p2_ref)):
            b1_ref[2 * j], b1_ref[2 * j + 1] = both_layers(ref[c])
        for z in range(-3, 5):
            i = z + 4
            h = z // 2 + 2
            u1_ref[z + 3] = (
                start_of(b1_ref[i], b1_ref[i - 1], b1_ref[i + 1], flat_ring, 1)
                + lift1_ref[c, 64 * h : 64 * h + 64, :]
            )
        for z in range(-2, 4):
            i = z + 3
            v1_ref[z + 2] = sweep_of(
                b1_ref[z + 4], u1_ref[i], u1_ref[i - 1], u1_ref[i + 1], flat_ring, 1
            )
        for z in range(-1, 3):
            i = z + 2
            value = sweep_of(
                b1_ref[z + 4], v1_ref[i], v1_ref[i - 1], v1_ref[i + 1], flat_ring, 1
            )
            wide = dot(value, spread0)
            lift0_ref[z + 1, pl.ds(0, 64, 2), :] = wide
            lift0_ref[z + 1, pl.ds(1, 64, 2), :] = wide
        for z in range(-2, 6):
            u0_ref[z + 2] = (
                start_of(b_at(z, c), b_at(z - 1, c), b_at(z + 1, c), flat_ring, 0)
                + lift0_ref[z // 2 + 1]
            )
        for z in range(-1, 5):
            i = z + 2
            v0_ref[z + 1] = sweep_of(
                b_at(z, c), u0_ref[i], u0_ref[i - 1], u0_ref[i + 1], flat_ring, 0
            )
        for z in range(CZ):
            i = z + 1
            value = sweep_of(
                own_ref[z, c], v0_ref[i], v0_ref[i - 1], v0_ref[i + 1], flat_ring, 0
            )
            vel_ref[z, c] = value
            rounded = value.astype(BF16).astype(F32)
            ext_ref[3 * z + c, 0:128, :] = rounded
            ext_ref[3 * z + c, 128:144, :] = rounded[0:16]
        return carry

    lax.fori_loop(0, 3, component, 0)
    lane = iota((8, 128), 1)
    sub = iota((8, 128), 0)

    def pick(d, carry):
        for order in range(2):

            @pl.when(meta_ref[4 * d + 2 * order] > 0)
            def _():
                base_x = meta_ref[4 * d + 2 * order] - 1
                base_y = meta_ref[4 * d + 2 * order + 1]
                shift = base_x & 7
                row = pl.multiple_of(base_x - shift, 8)
                late = sub >= shift
                for q in range(3):
                    packed = jnp.zeros((8, 128), F32)
                    for g in range(8):
                        v = 8 * q + g
                        start = row + 8 * (v % 2)
                        value = jnp.where(
                            late,
                            ext_ref[v // 2, pl.ds(start, 8), :],
                            ext_ref[v // 2, pl.ds(start + 8, 8), :],
                        )
                        turned = pltpu.roll(value, (BOX * g - base_y) & 127, 1)
                        packed = jnp.where(lane // BOX == g, turned, packed)
                    stage_ref[d, pl.ds(order * ROWS + 8 * q, 8), :] = pltpu.roll(
                        packed, (8 - shift) & 7, 0
                    )

        return carry

    lax.fori_loop(0, pay_ref.shape[0], pick, 0)

    def finish(t, carry):
        pay_ref[t] = stage_ref[t].astype(BF16)
        return carry

    lax.fori_loop(0, pay_ref.shape[0], finish, 0, unroll=4)


def way_up(me, meta, gathered, tiles, low, own, high):
    slots = gathered.shape[0]
    return call(
        up_kernel,
        (
            jax.ShapeDtypeStruct(own.shape, F32),
            jax.ShapeDtypeStruct((slots, 2 * ROWS, 128), BF16),
        ),
        [SMEM, SMEM] + [VMEM] * 9,
        [
            pltpu.VMEM((480, 128), F32),
            pltpu.VMEM((6, 32, 128), F32),
            pltpu.VMEM((3, 320, 128), F32),
            pltpu.VMEM((10, 64, 128), F32),
            pltpu.VMEM((8, 64, 128), F32),
            pltpu.VMEM((6, 64, 128), F32),
            pltpu.VMEM((4, 128, 128), F32),
            pltpu.VMEM((8, 128, 128), F32),
            pltpu.VMEM((6, 128, 128), F32),
            pltpu.VMEM((12, 144, 128), F32),
            pltpu.VMEM((slots, 2 * ROWS, 128), F32),
        ],
        "way_up",
    )(me, meta, gathered, *tiles, low, own, high)


def read_kernel(dest_ref, pay_ref, pos_ref, out_ref, stage_ref, count_ref):
    slots = pay_ref.shape[0]

    def widen(t, carry):
        count_ref[t] = 0
        stage_ref[t] = pay_ref[t].astype(F32)
        return carry

    lax.fori_loop(0, slots, widen, 0, unroll=4)
    lane = iota((8, 128), 1)

    def one(block, carry):
        target = dest_ref[0, block]
        order = count_ref[target]
        count_ref[target] = order + 1
        weight_x, weight_y, weight_z = box_weights(pos_ref, block)
        rows = []
        for q in range(3):
            packed = stage_ref[target, pl.ds(pl.multiple_of(order * ROWS + 8 * q, 8), 8), :]
            turned = [pltpu.roll(packed, (128 - BOX * g) % 128, 1) for g in range(8)]
            for g in range(8):
                rows.append(jnp.where(lane < BOX, turned[g], turned[(g + 7) % 8]))
        left = jnp.concatenate(rows, axis=0)[:, : 2 * BOX].astype(BF16)
        right = jnp.concatenate(split(weight_y), axis=0)
        spread = lax.dot_general(
            left, right, (((1,), (0,)), ((), ())), preferred_element_type=F32
        )
        for c in range(3):
            total = None
            for k in range(CZ):
                kc = 3 * k + c
                part = spread[BOX * kc : BOX * kc + BOX] * weight_z[k : k + 1]
                total = part if total is None else total + part
            out_ref[c, pl.ds(block, 1), :] = jnp.sum(total * weight_x, axis=0, keepdims=True)
        return carry

    lax.fori_loop(0, pos_ref.shape[1], one, 0, unroll=2)


def read(dest, payload, positions):
    slots = payload.shape[0]
    return call(
        read_kernel,
        jax.ShapeDtypeStruct(positions.shape, F32),
        [SMEM, VMEM, VMEM],
        [pltpu.VMEM((slots, 2 * ROWS, 128), F32), pltpu.SMEM((slots,), jnp.int32)],
        "read",
    )(dest, payload, positions)


def moved(value, step):
    size = lax.axis_size(AX)
    return lax.ppermute(value, AX, [(i, (i + step) % size) for i in range(size)])


def exchanged(value):
    return lax.all_to_all(value, AX, split_axis=0, concat_axis=0, tiled=True)


def shards(marker_positions, marker_forces, dest_slab, base_cells, fluid_source):
    slots = lax.axis_size(AX)
    positions = marker_positions.transpose(1, 0, 2)
    forces = marker_forces.transpose(1, 0, 2)
    dest = dest_slab.T
    me = lax.axis_index(AX).astype(jnp.int32).reshape(1)
    payload = exchanged(build(dest, base_cells.T, positions, forces, slots))
    heads = payload[:, 0 : ROWS + 1 : ROWS, 0 : BOX + 1 : BOX]
    meta = heads.astype(jnp.int32).reshape(4 * slots)
    source, bottom, top = place(meta, payload, fluid_source)
    low = moved(top, 1)
    high = moved(bottom, -1)
    tile = fine_down(low, source, high)
    m1, p1 = moved(tile, 1), moved(tile, -1)
    m2, p2 = moved(tile, 2), moved(tile, -2)
    gathered = exchanged(middle_down(m1, tile, p1, slots))
    velocity, picked = way_up(
        me, meta, gathered, (m2, m1, tile, p1, p2), low, source, high
    )
    out = read(dest, exchanged(picked), positions)
    return velocity, out.transpose(1, 0, 2)


def solution(mesh):
    return jax.shard_map(
        shards,
        mesh=mesh,
        in_specs=(P(AX), P(AX), P(AX), P(AX), P(AX)),
        out_specs=(P(AX), P(AX)),
        check_vma=False,
    )
```

```python
import math

import jax
import jax.numpy as jnp
from jax import lax
from jax.experimental import pallas as pl
from jax.experimental.pallas import tpu as pltpu
from jax.sharding import PartitionSpec as P

AX = "gz"
BOX = 16
CZ = 4
ROWS = 24
SCREEN = 1.0 / 64.0
RELAX = 2.0 / 3.0
INTERPRET = False
F32 = jnp.float32
BF16 = jnp.bfloat16
HIGH = lax.Precision.HIGHEST


def level(index):
    q = 0.25**index
    return q, SCREEN + 6.0 * q, RELAX / (SCREEN + 6.0 * q)


def call(body, out_shape, in_specs=None, scratch=(), name=None, megabytes=24):
    options = {} if in_specs is None else {"in_specs": in_specs}
    return pl.pallas_call(
        body,
        out_shape=out_shape,
        scratch_shapes=list(scratch),
        name=name,
        interpret=INTERPRET,
        compiler_params=pltpu.CompilerParams(vmem_limit_bytes=megabytes << 20),
        **options,
    )


def shaped(shape, dtype, near=True):
    if near and not INTERPRET:
        return pltpu.VMEM(shape, dtype)
    return jax.ShapeDtypeStruct(shape, dtype)


def near(value):
    return value if INTERPRET else pltpu.with_memory_space_constraint(value, pltpu.VMEM)


VMEM = pl.BlockSpec(memory_space=pltpu.VMEM)
SMEM = pl.BlockSpec(memory_space=pltpu.SMEM)


def iota(shape, dim):
    return lax.broadcasted_iota(jnp.int32, shape, dim)


COS = (
    0.13884009367929634,
    0.008677498753340366,
    0.0001925760632832398,
    2.2059131886721028e-06,
    1.644977822379996e-08,
)


def phi(offset):
    inside = jnp.maximum(4.0 - offset * offset, 0.0)
    value = inside * COS[-1] + COS[-2]
    for coefficient in COS[-3::-1]:
        value = value * inside + coefficient
    value = value * inside
    return value * value


def split(value):
    high = value.astype(BF16)
    return high, (value - high.astype(F32)).astype(BF16)


def box_weights(pos_ref, block):
    cells = iota((BOX, 256), 0).astype(F32)
    levels = iota((8, 256), 0).astype(F32)
    row = pl.ds(block, 1)
    along_x = 2.0 + (BOX - 5) * pos_ref[0, row, :]
    along_y = 2.0 + (BOX - 5) * pos_ref[1, row, :]
    height = (CZ - 1) * pos_ref[2, row, :]
    return phi(along_x - cells), phi(along_y - cells), phi(height - levels)


def by_levels(weight_y, weight_z):
    return split(jnp.concatenate([weight_z[k : k + 1] * weight_y for k in range(CZ)], axis=0))


def together(count, most):
    return math.gcd(count, most)


def build_kernel(dest_ref, base_ref, pos_ref, frc_ref, out_ref, stage_ref, count_ref):
    slots = out_ref.shape[0]
    blocks = pos_ref.shape[1]
    group = together(blocks, 4)

    def clear(t, carry):
        count_ref[t] = 0
        for order in range(2):
            stage_ref[t, order * ROWS : order * ROWS + 8, :] = jnp.zeros((8, 128), F32)
        return carry

    lax.fori_loop(0, slots, clear, 0, unroll=4)
    lane = iota((8, 128), 1)
    top = iota((8, 128), 0) == 0

    def one(block):
        weight_x, weight_y, weight_z = box_weights(pos_ref, block)
        loaded = [frc_ref[c, pl.ds(block, 1), :] * weight_x for c in range(3)]
        high, low = split(jnp.concatenate(loaded, axis=0))
        right = jnp.concatenate(by_levels(weight_y, weight_z), axis=0)
        dims = (((1,), (1,)), ((), ()))
        box = lax.dot_general(high, right, dims, preferred_element_type=F32)
        box = box + lax.dot_general(low, right, dims, preferred_element_type=F32)
        box = box + pltpu.roll(box, 64, 1)
        base_x = base_ref[0, block].astype(F32) + 1.0
        base_y = base_ref[1, block].astype(F32)
        tiles = []
        for c in range(3):
            tile = jnp.where(
                lane < 64, box[BOX * c : BOX * c + 8], box[BOX * c + 8 : BOX * c + 16]
            )
            if c == 0:
                tile = jnp.where(top & (lane == 0), base_x, tile)
                tile = jnp.where(top & (lane == BOX), base_y, tile)
            tiles.append(tile)
        return tiles

    def several(step, carry):
        results = [one(step * group + n) for n in range(group)]
        for n in range(group):
            target = dest_ref[0, step * group + n]
            order = count_ref[target]
            count_ref[target] = order + 1
            for c in range(3):
                row = pl.multiple_of(order * ROWS + 8 * c, 8)
                stage_ref[target, pl.ds(row, 8), :] = results[n][c]
        return carry

    lax.fori_loop(0, blocks // group, several, 0)

    def finish(t, carry):
        out_ref[t] = stage_ref[t].astype(BF16)
        return carry

    lax.fori_loop(0, slots, finish, 0, unroll=4)


def build(dest, base, positions, forces, slots):
    return call(
        build_kernel,
        shaped((slots, 2 * ROWS, 128), BF16),
        [SMEM, SMEM, VMEM, VMEM],
        [pltpu.VMEM((slots, 2 * ROWS, 128), F32), pltpu.SMEM((slots,), jnp.int32)],
        "build",
    )(dest, base, positions, forces)


def place_kernel(meta_ref, pay_ref, fluid_ref, src_ref, bottom_ref, top_ref, grid_ref):
    slots = pay_ref.shape[0]
    lane = iota((8, 128), 1)
    sub = iota((8, 128), 0)
    for z in range(CZ):
        for c in range(3):
            grid_ref[3 * z + c, 0:128, :] = fluid_ref[z, c]
            grid_ref[3 * z + c, 128:144, :] = jnp.zeros((16, 128), F32)

    def turned(tile, head, base_y):
        base_x = jnp.maximum(head - 1, 0)
        shift = base_x & 7
        row = pl.multiple_of(base_x - shift, 8)
        window = (lane - base_y) & 127
        inside = (window >= 1) & (window <= BOX - 2) & (head > 0)
        late = inside & (sub >= shift)
        early = inside & (sub < shift)
        values = []
        for c in range(3):
            piece = pltpu.roll(tile[8 * c : 8 * c + 8], shift, 0)
            for g in range(8):
                values.append(pltpu.roll(piece, (base_y - BOX * g) & 127, 1))
        return row, late, early, values

    def add(row, late, early, values):
        for k in range(CZ):
            for c in range(3):
                first = values[8 * c + k]
                second = values[8 * c + 4 + k]
                kc = 3 * k + c
                grid_ref[kc, pl.ds(row, 8), :] += jnp.where(late, first, 0.0)
                grid_ref[kc, pl.ds(row + 8, 8), :] += jnp.where(
                    early, first, jnp.where(late, second, 0.0)
                )
                grid_ref[kc, pl.ds(row + 16, 8), :] += jnp.where(early, second, 0.0)

    group = together(slots, 2)

    def several(step, carry):
        found = []
        for n in range(group):
            d = step * group + n
            tile = pay_ref[d].astype(F32)
            for order in range(2):
                found.append(
                    turned(
                        tile[order * ROWS : (order + 1) * ROWS],
                        meta_ref[4 * d + 2 * order],
                        meta_ref[4 * d + 2 * order + 1],
                    )
                )
        for one in found:
            add(*one)
        return carry

    lax.fori_loop(0, slots // group, several, 0)
    for z in range(CZ):
        for c in range(3):
            kc = 3 * z + c
            grid_ref[kc, 0:16, :] += grid_ref[kc, 128:144, :]
            value = grid_ref[kc, 0:128, :]
            src_ref[z, c] = value
            if z < 3:
                bottom_ref[z, c] = value
            if z > 0:
                top_ref[z - 1, c] = value


def place(meta, payload, fluid):
    width = fluid.shape[2]
    return call(
        place_kernel,
        (
            shaped(fluid.shape, F32),
            shaped((3, 3, width, width), F32),
            shaped((3, 3, width, width), F32),
        ),
        [SMEM, VMEM, VMEM],
        [pltpu.VMEM((12, 144, 128), F32)],
        "place",
    )(meta, near(payload), fluid)


def flat_ring(x):
    rows = x.shape[-2]
    ax = x.ndim - 2
    return (
        pltpu.roll(x, 1, ax)
        + pltpu.roll(x, rows - 1, ax)
        + (pltpu.roll(x, 1, ax + 1) + pltpu.roll(x, 127, ax + 1))
    )


def group_ring(x):
    rows = x.shape[-2]
    ax = x.ndim - 2
    lane = iota(x.shape, ax + 1) & 31
    before = jnp.where(lane == 0, pltpu.roll(x, 97, ax + 1), pltpu.roll(x, 1, ax + 1))
    after = jnp.where(lane == 31, pltpu.roll(x, 31, ax + 1), pltpu.roll(x, 127, ax + 1))
    return pltpu.roll(x, 1, ax) + pltpu.roll(x, rows - 1, ax) + (before + after)


def start_of(b, below, above, ring, index):
    q, _, w = level(index)
    return w * ((4.0 / 3.0) * b + (w * q) * (ring(b) + (below + above)))


def left_of(b, u, below, above, ring, index):
    q, diag, _ = level(index)
    return b - diag * u + q * (ring(u) + (below + above))


def sweep_of(b, u, below, above, ring, index):
    q, _, w = level(index)
    return (1.0 - RELAX) * u + (w * b + (w * q) * (ring(u) + (below + above)))


def dot(left, right):
    return lax.dot_general(
        left, right, (((1,), (0,)), ((), ())), precision=HIGH, preferred_element_type=F32
    )


def lanes(test):
    return test(iota((128, 128), 0), iota((128, 128), 1))


def fine_kernel(low_ref, own_ref, high_ref, out_ref, u_ref, sum_ref):
    def b_at(z, c):
        if z < 0:
            return low_ref[z + 3, c]
        return own_ref[z, c] if z < CZ else high_ref[z - CZ, c]

    pool = [
        jnp.where(
            lanes(lambda r, l: (r // 2 == (l & 63)) & (l // 64 == half)), 0.125, 0.0
        )
        for half in range(2)
    ]

    def component(c, carry):
        for z in range(-1, CZ + 1):
            u_ref[z + 1] = start_of(b_at(z, c), b_at(z - 1, c), b_at(z + 1, c), flat_ring, 0)
        total = None
        for half in range(2):
            for z in (2 * half, 2 * half + 1):
                value = left_of(
                    own_ref[z, c], u_ref[z + 1], u_ref[z], u_ref[z + 2], flat_ring, 0
                )
                sum_ref[...] = value if z == 2 * half else sum_ref[...] + value
            rows = sum_ref[pl.ds(0, 64, 2), :] + sum_ref[pl.ds(1, 64, 2), :]
            part = dot(rows, pool[half])
            total = part if total is None else total + part
        out_ref[c] = total
        return carry

    lax.fori_loop(0, 3, component, 0)


def fine_down(low, own, high):
    return call(
        fine_kernel,
        shaped((3, 64, 128), F32),
        None,
        [pltpu.VMEM((CZ + 2, 128, 128), F32), pltpu.VMEM((128, 128), F32)],
        "fine_down",
    )(near(low), near(own), near(high))


def both_layers(tile):
    lane = iota(tile.shape, tile.ndim - 1)
    turned = pltpu.roll(tile, 64, tile.ndim - 1)
    return jnp.where(lane < 64, tile, turned), jnp.where(lane < 64, turned, tile)


def pack_coarse(value):
    last = value[24:32]
    lane = iota((8, 128), 1)
    return [
        jnp.where(lane < 96, value[8 * c : 8 * c + 8], pltpu.roll(last, 96 - 32 * c, 1))
        for c in range(3)
    ]


def unpack_coarse(tile):
    lane = iota((8, 128), 1)
    last = jnp.zeros((8, 128), F32)
    rows = []
    for c in range(3):
        piece = tile[8 * c : 8 * c + 8]
        turned = pltpu.roll(piece, (32 * c - 96) % 128, 1)
        last = jnp.where(lane // 32 == c, turned, last)
        rows.append(jnp.where(lane < 96, piece, 0.0))
    return jnp.concatenate(rows + [last], axis=0)


def middle_kernel(low_ref, own_ref, high_ref, out_ref, sum_ref):
    total = None
    for c in range(3):
        b = []
        for ref in (low_ref, own_ref, high_ref):
            b.extend(both_layers(ref[c]))
        u = [start_of(b[i], b[i - 1], b[i + 1], flat_ring, 1) for i in range(1, 5)]
        left = [left_of(b[i + 1], u[i], u[i - 1], u[i + 1], flat_ring, 1) for i in (1, 2)]
        sum_ref[...] = left[0] + left[1]
        rows = sum_ref[pl.ds(0, 32, 2), :] + sum_ref[pl.ds(1, 32, 2), :]
        pool = jnp.where(
            lanes(lambda r, l: (r // 2 == (l & 31)) & (l // 32 == c) & (r < 64)), 0.125, 0.0
        )
        part = dot(rows, pool)
        total = part if total is None else total + part
    packed = jnp.concatenate(pack_coarse(total), axis=0)

    def copy(d, carry):
        out_ref[d] = packed
        return carry

    lax.fori_loop(0, out_ref.shape[0], copy, 0, unroll=8)


def middle_down(low, own, high, slots):
    return call(
        middle_kernel,
        shaped((slots, 24, 128), F32),
        None,
        [pltpu.VMEM((64, 128), F32)],
        "middle_down",
    )(near(low), near(own), near(high))


def inner(x):
    return x[1:-1]


def coarse_part(me, g2_ref, pool_ref, final_ref):
    slots = g2_ref.shape[0]
    parity = me % 2
    first = me - parity - 16 + 16 * slots
    b2 = jnp.stack([unpack_coarse(g2_ref[(first + t) % slots]) for t in range(34)])
    total = lax.fori_loop(
        0, slots, lambda d, sums: sums + g2_ref[d], jnp.zeros((24, 128), F32)
    )
    column = jnp.sum(unpack_coarse(total), axis=0, keepdims=True)
    same = jnp.where(lanes(lambda r, l: r // 32 == l // 32), 1.0, 0.0)
    mean_b2 = dot(jnp.broadcast_to(column, (8, 128)), same)[0:1] * (1.0 / (slots * 1024.0))
    _, _, w2 = level(2)
    q3, _, w3 = level(3)
    factor = (1.0 - w3 * SCREEN) ** 6 * (1.0 - w2 * SCREEN) ** 2 / SCREEN
    lift = mean_b2 * factor
    u2 = start_of(inner(b2), b2[:-2], b2[2:], group_ring, 2)
    r2 = left_of(b2[2:-2], inner(u2), u2[:-2], u2[2:], group_ring, 2)
    pairs = r2.reshape(15, 2, 32, 128)
    pool_ref[...] = (pairs[:, 0] + pairs[:, 1]).reshape(480, 128)
    rows = pool_ref[pl.ds(0, 240, 2), :] + pool_ref[pl.ds(1, 240, 2), :]
    pool = jnp.where(
        lanes(lambda r, l: ((r & 31) // 2 == (l & 15)) & (r // 32 == l // 32)), 0.125, 0.0
    )
    b3 = dot(rows, pool).reshape(15, 16, 128)
    u3 = w3 * b3
    for _ in range(5):
        b3 = inner(b3)
        u3 = sweep_of(b3, inner(u3), u3[:-2], u3[2:], group_ring, 3)
    u3 = (u3 + lift[None]).reshape(80, 128)
    spread = jnp.where(
        lanes(lambda r, l: ((l & 31) // 2 == (r & 31)) & (r // 32 == l // 32)), 1.0, 0.0
    )
    wide = dot(u3, spread)
    pool_ref[pl.ds(0, 80, 2), :] = wide
    pool_ref[pl.ds(1, 80, 2), :] = wide
    lifted = pool_ref[0:160, :].reshape(5, 1, 32, 128)
    u = (u2[11:21].reshape(5, 2, 32, 128) + lifted).reshape(10, 32, 128)
    u = sweep_of(b2[13:21], inner(u), u[:-2], u[2:], group_ring, 2)
    u = sweep_of(b2[14:20], inner(u), u[:-2], u[2:], group_ring, 2)
    final_ref[...] = u
    return jnp.concatenate([final_ref[parity + h] for h in range(5)], axis=0)


def up_kernel(
    me_ref, meta_ref, g2_ref, m2_ref, m1_ref, m0_ref, p1_ref, p2_ref, low_ref, own_ref,
    high_ref, vel_ref, pay_ref,
    pool_ref, final_ref, lift1_ref, b1_ref, u1_ref, v1_ref, lift0_ref, u0_ref, v0_ref,
    ext_ref,
):
    coarse = coarse_part(me_ref[0], g2_ref, pool_ref, final_ref)
    for c in range(3):
        spread = jnp.where(lanes(lambda r, l: r == 32 * c + (l & 63) // 2), 1.0, 0.0)
        wide = dot(coarse, spread)
        lift1_ref[c, pl.ds(0, 160, 2), :] = wide
        lift1_ref[c, pl.ds(1, 160, 2), :] = wide
    spread0 = jnp.where(lanes(lambda r, l: r == l // 2), 1.0, 0.0)

    def b_at(z, c):
        if z < 0:
            return low_ref[z + 3, c]
        return own_ref[z, c] if z < CZ else high_ref[z - CZ, c]

    def component(c, carry):
        for j, ref in enumerate((m2_ref, m1_ref, m0_ref, p1_ref, p2_ref)):
            b1_ref[2 * j], b1_ref[2 * j + 1] = both_layers(ref[c])
        for z in range(-3, 5):
            i = z + 4
            h = z // 2 + 2
            u1_ref[z + 3] = (
                start_of(b1_ref[i], b1_ref[i - 1], b1_ref[i + 1], flat_ring, 1)
                + lift1_ref[c, 64 * h : 64 * h + 64, :]
            )
        for z in range(-2, 4):
            i = z + 3
            v1_ref[z + 2] = sweep_of(
                b1_ref[z + 4], u1_ref[i], u1_ref[i - 1], u1_ref[i + 1], flat_ring, 1
            )
        for z in range(-1, 3):
            i = z + 2
            value = sweep_of(
                b1_ref[z + 4], v1_ref[i], v1_ref[i - 1], v1_ref[i + 1], flat_ring, 1
            )
            wide = dot(value, spread0)
            lift0_ref[z + 1, pl.ds(0, 64, 2), :] = wide
            lift0_ref[z + 1, pl.ds(1, 64, 2), :] = wide
        for z in range(-2, 6):
            u0_ref[z + 2] = (
                start_of(b_at(z, c), b_at(z - 1, c), b_at(z + 1, c), flat_ring, 0)
                + lift0_ref[z // 2 + 1]
            )
        for z in range(-1, 5):
            i = z + 2
            v0_ref[z + 1] = sweep_of(
                b_at(z, c), u0_ref[i], u0_ref[i - 1], u0_ref[i + 1], flat_ring, 0
            )
        for z in range(CZ):
            i = z + 1
            value = sweep_of(
                own_ref[z, c], v0_ref[i], v0_ref[i - 1], v0_ref[i + 1], flat_ring, 0
            )
            vel_ref[z, c] = value
            rounded = value.astype(BF16).astype(F32)
            ext_ref[3 * z + c, 0:128, :] = rounded
            ext_ref[3 * z + c, 128:144, :] = rounded[0:16]
        return carry

    lax.fori_loop(0, 3, component, 0)
    lane = iota((8, 128), 1)
    sub = iota((8, 128), 0)

    half = [lane // BOX == g for g in range(8)]

    def gather(head, base_y):
        base_x = jnp.maximum(head - 1, 0)
        shift = base_x & 7
        row = pl.multiple_of(base_x - shift, 8)
        late = sub >= shift
        values = []
        for k in range(CZ):
            for c in range(3):
                tiles = [ext_ref[3 * k + c, pl.ds(row + 8 * n, 8), :] for n in range(3)]
                for upper in range(2):
                    value = jnp.where(late, tiles[upper], tiles[upper + 1])
                    g = 4 * upper + k
                    values.append((c, g, pltpu.roll(value, (BOX * g - base_y) & 127, 1)))
        return (8 - shift) & 7, values

    group = together(pay_ref.shape[0], 2)

    def several(step, carry):
        found = []
        for n in range(group):
            d = step * group + n
            for order in range(2):
                found.append(
                    gather(meta_ref[4 * d + 2 * order], meta_ref[4 * d + 2 * order + 1])
                )
        for n in range(group):
            pieces = []
            for order in range(2):
                back, values = found[2 * n + order]
                for c in range(3):
                    packed = jnp.zeros((8, 128), F32)
                    for own_c, g, value in values:
                        if own_c == c:
                            packed = jnp.where(half[g], value, packed)
                    pieces.append(pltpu.roll(packed, back, 0))
            pay_ref[step * group + n] = jnp.concatenate(pieces, axis=0).astype(BF16)
        return carry

    lax.fori_loop(0, pay_ref.shape[0] // group, several, 0)


def way_up(me, meta, gathered, tiles, low, own, high):
    slots = gathered.shape[0]
    return call(
        up_kernel,
        (
            shaped(own.shape, F32, False),
            shaped((slots, 2 * ROWS, 128), BF16),
        ),
        [SMEM, SMEM] + [VMEM] * 9,
        [
            pltpu.VMEM((480, 128), F32),
            pltpu.VMEM((6, 32, 128), F32),
            pltpu.VMEM((3, 320, 128), F32),
            pltpu.VMEM((10, 64, 128), F32),
            pltpu.VMEM((8, 64, 128), F32),
            pltpu.VMEM((6, 64, 128), F32),
            pltpu.VMEM((4, 128, 128), F32),
            pltpu.VMEM((8, 128, 128), F32),
            pltpu.VMEM((6, 128, 128), F32),
            pltpu.VMEM((12, 144, 128), F32),
        ],
        "way_up",
    )(me, meta, near(gathered), *map(near, tiles), near(low), near(own), near(high))


def read_kernel(dest_ref, pay_ref, pos_ref, out_ref, stage_ref, count_ref):
    slots = pay_ref.shape[0]

    def widen(t, carry):
        count_ref[t] = 0
        stage_ref[t] = pay_ref[t].astype(F32)
        return carry

    lax.fori_loop(0, slots, widen, 0, unroll=4)
    lane = iota((8, 128), 1)

    group = together(pos_ref.shape[1], 4)

    def one(block, target, order):
        weight_x, weight_y, weight_z = box_weights(pos_ref, block)
        lower, upper = [], []
        for c in range(3):
            row = pl.multiple_of(order * ROWS + 8 * c, 8)
            packed = stage_ref[target, pl.ds(row, 8), :]
            swapped = pltpu.roll(packed, 64, 1)
            lower.append(jnp.where(lane < 64, packed, swapped))
            upper.append(jnp.where(lane < 64, swapped, packed))
        left = jnp.concatenate(
            [half for pair in zip(lower, upper) for half in pair], axis=0
        ).astype(BF16)
        right = jnp.concatenate(by_levels(weight_y, weight_z), axis=0)
        spread = lax.dot_general(
            left, right, (((1,), (0,)), ((), ())), preferred_element_type=F32
        )
        for c in range(3):
            value = spread[BOX * c : BOX * c + BOX] * weight_x
            out_ref[c, pl.ds(block, 1), :] = jnp.sum(value, axis=0, keepdims=True)

    def several(step, carry):
        places = []
        for n in range(group):
            target = dest_ref[0, step * group + n]
            order = count_ref[target]
            count_ref[target] = order + 1
            places.append((target, order))
        for n in range(group):
            one(step * group + n, *places[n])
        return carry

    lax.fori_loop(0, pos_ref.shape[1] // group, several, 0)


def read(dest, payload, positions):
    slots = payload.shape[0]
    return call(
        read_kernel,
        shaped(positions.shape, F32, False),
        [SMEM, VMEM, VMEM],
        [pltpu.VMEM((slots, 2 * ROWS, 128), F32), pltpu.SMEM((slots,), jnp.int32)],
        "read",
    )(dest, near(payload), positions)


def moved(value, step):
    size = lax.axis_size(AX)
    return lax.ppermute(value, AX, [(i, (i + step) % size) for i in range(size)])


def exchanged(value):
    return lax.all_to_all(value, AX, split_axis=0, concat_axis=0, tiled=True)


def shards(marker_positions, marker_forces, dest_slab, base_cells, fluid_source):
    slots = lax.axis_size(AX)
    positions = marker_positions.transpose(1, 0, 2)
    forces = marker_forces.transpose(1, 0, 2)
    dest = dest_slab.T
    me = lax.axis_index(AX).astype(jnp.int32).reshape(1)
    payload = exchanged(build(dest, base_cells.T, positions, forces, slots))
    heads = payload[:, 0 : ROWS + 1 : ROWS, 0 : BOX + 1 : BOX]
    meta = heads.astype(jnp.int32).reshape(4 * slots)
    source, bottom, top = place(meta, payload, fluid_source)
    low = moved(top, 1)
    high = moved(bottom, -1)
    tile = fine_down(low, source, high)
    m1, p1 = moved(tile, 1), moved(tile, -1)
    m2, p2 = moved(tile, 2), moved(tile, -2)
    gathered = exchanged(middle_down(m1, tile, p1, slots))
    velocity, picked = way_up(
        me, meta, gathered, (m2, m1, tile, p1, p2), low, source, high
    )
    out = read(dest, exchanged(picked), positions)
    return velocity, out.transpose(1, 0, 2)


def solution(mesh):
    return jax.shard_map(
        shards,
        mesh=mesh,
        in_specs=(P(AX), P(AX), P(AX), P(AX), P(AX)),
        out_specs=(P(AX), P(AX)),
        check_vma=False,
    )
```

```python
import math

import jax
import jax.numpy as jnp
from jax import lax
from jax.experimental import pallas as pl
from jax.experimental.pallas import tpu as pltpu
from jax.sharding import Mesh
from jax.sharding import PartitionSpec as P

AX = ("hi", "lo")
LOCAL = 8
BOX = 16
CZ = 4
ROWS = 24
SCREEN = 1.0 / 64.0
RELAX = 2.0 / 3.0
INTERPRET = False
F32 = jnp.float32
BF16 = jnp.bfloat16
HIGH = lax.Precision.HIGHEST


def level(index):
    q = 0.25**index
    return q, SCREEN + 6.0 * q, RELAX / (SCREEN + 6.0 * q)


def call(body, out_shape, in_specs=None, scratch=(), name=None, megabytes=24):
    options = {} if in_specs is None else {"in_specs": in_specs}
    return pl.pallas_call(
        body,
        out_shape=out_shape,
        scratch_shapes=list(scratch),
        name=name,
        interpret=INTERPRET,
        compiler_params=pltpu.CompilerParams(vmem_limit_bytes=megabytes << 20),
        **options,
    )


def shaped(shape, dtype, near=True):
    if near and not INTERPRET:
        return pltpu.VMEM(shape, dtype)
    return jax.ShapeDtypeStruct(shape, dtype)


def near(value):
    return value if INTERPRET else pltpu.with_memory_space_constraint(value, pltpu.VMEM)


VMEM = pl.BlockSpec(memory_space=pltpu.VMEM)
SMEM = pl.BlockSpec(memory_space=pltpu.SMEM)


def iota(shape, dim):
    return lax.broadcasted_iota(jnp.int32, shape, dim)


COS = (
    0.13884009367929634,
    0.008677498753340366,
    0.0001925760632832398,
    2.2059131886721028e-06,
    1.644977822379996e-08,
)


def phi(offset):
    inside = jnp.maximum(4.0 - offset * offset, 0.0)
    value = inside * COS[-1] + COS[-2]
    for coefficient in COS[-3::-1]:
        value = value * inside + coefficient
    value = value * inside
    return value * value


def split(value):
    high = value.astype(BF16)
    return high, (value - high.astype(F32)).astype(BF16)


def box_weights(pos_ref, block):
    cells = iota((BOX, 256), 0).astype(F32)
    levels = iota((8, 256), 0).astype(F32)
    row = pl.ds(block, 1)
    along_x = 2.0 + (BOX - 5) * pos_ref[0, row, :]
    along_y = 2.0 + (BOX - 5) * pos_ref[1, row, :]
    height = (CZ - 1) * pos_ref[2, row, :]
    return phi(along_x - cells), phi(along_y - cells), phi(height - levels)


def by_levels(weight_y, weight_z):
    return split(jnp.concatenate([weight_z[k : k + 1] * weight_y for k in range(CZ)], axis=0))


PIECES = (2 * BOX, 3 * BOX, 4 * BOX)


def together(count, most):
    return math.gcd(count, most)


def build_kernel(
    dest_ref, base_ref, pos_ref, frc_ref, fluid_ref, out_ref, stage_ref, count_ref
):
    slots = out_ref.shape[0]
    blocks = pos_ref.shape[1]
    group = together(blocks, 4)

    def clear(t, carry):
        count_ref[t] = 0
        for order in range(2):
            stage_ref[t, order * ROWS : order * ROWS + 8, :] = jnp.zeros((8, 128), F32)
        return carry

    lax.fori_loop(0, slots, clear, 0, unroll=4)
    lane = iota((8, 128), 1)
    top = iota((8, 128), 0) == 0

    def one(block):
        weight_x, weight_y, weight_z = box_weights(pos_ref, block)
        loaded = [frc_ref[c, pl.ds(block, 1), :] * weight_x for c in range(3)]
        high, low = split(jnp.concatenate(loaded, axis=0))
        right = jnp.concatenate(by_levels(weight_y, weight_z), axis=0)
        dims = (((1,), (1,)), ((), ()))
        box = lax.dot_general(high, right, dims, preferred_element_type=F32)
        box = box + lax.dot_general(low, right, dims, preferred_element_type=F32)
        box = box + pltpu.roll(box, 64, 1)
        base_x = base_ref[0, block].astype(F32) + 1.0
        base_y = base_ref[1, block].astype(F32)
        tiles, sums = [], []
        for c in range(3):
            tile = jnp.where(
                lane < 64, box[BOX * c : BOX * c + 8], box[BOX * c + 8 : BOX * c + 16]
            )
            sums.append(tile.astype(BF16).astype(F32))
            if c == 0:
                tile = jnp.where(top & (lane == 0), base_x, tile)
                tile = jnp.where(top & (lane == BOX), base_y, tile)
            tiles.append(tile)
        return tiles, sums

    def several(step, carry):
        results = []
        for n in range(group):
            tiles, sums = one(step * group + n)
            results.append(tiles)
            carry = tuple(a + b for a, b in zip(carry, sums))
        for n in range(group):
            target = dest_ref[0, step * group + n]
            order = count_ref[target]
            count_ref[target] = order + 1
            for c in range(3):
                row = pl.multiple_of(order * ROWS + 8 * c, 8)
                stage_ref[target, pl.ds(row, 8), :] = results[n][c]
        return carry

    fluid = []
    for c in range(3):
        column = fluid_ref[0, c] + fluid_ref[1, c] + (fluid_ref[2, c] + fluid_ref[3, c])
        fluid.append(jnp.sum(column.reshape(16, 8, 128), axis=0))
    fluid = lax.fori_loop(0, blocks // group, several, tuple(fluid))
    pieces = []
    for c in range(3):
        rest = jnp.broadcast_to(jnp.sum(fluid[c], axis=(0, 1), keepdims=True), (8, 128))
        marked = jnp.zeros((8, 128), F32)
        for place_of in PIECES:
            part = rest.astype(BF16).astype(F32)
            marked = jnp.where(lane == place_of, part, marked)
            rest = rest - part
        pieces.append(marked)
    held = top & ((lane == PIECES[0]) | (lane == PIECES[1]) | (lane == PIECES[2]))

    def finish(t, carry):
        tiles = [
            jnp.where(held, pieces[c], stage_ref[t, 8 * c : 8 * c + 8, :]) for c in range(3)
        ]
        tiles.append(stage_ref[t, ROWS : 2 * ROWS, :])
        out_ref[t] = jnp.concatenate(tiles, axis=0).astype(BF16)
        return carry

    lax.fori_loop(0, slots, finish, 0, unroll=4)


def build(dest, base, positions, forces, fluid, slots):
    return call(
        build_kernel,
        shaped((slots, 2 * ROWS, 128), BF16),
        [SMEM, SMEM, VMEM, VMEM, VMEM],
        [pltpu.VMEM((slots, 2 * ROWS, 128), F32), pltpu.SMEM((slots,), jnp.int32)],
        "build",
    )(dest, base, positions, forces, fluid)


def flat_ring(x):
    rows = x.shape[-2]
    ax = x.ndim - 2
    return (
        pltpu.roll(x, 1, ax)
        + pltpu.roll(x, rows - 1, ax)
        + (pltpu.roll(x, 1, ax + 1) + pltpu.roll(x, 127, ax + 1))
    )


def group_ring(x):
    rows = x.shape[-2]
    ax = x.ndim - 2
    lane = iota(x.shape, ax + 1) & 31
    before = jnp.where(lane == 0, pltpu.roll(x, 97, ax + 1), pltpu.roll(x, 1, ax + 1))
    after = jnp.where(lane == 31, pltpu.roll(x, 31, ax + 1), pltpu.roll(x, 127, ax + 1))
    return pltpu.roll(x, 1, ax) + pltpu.roll(x, rows - 1, ax) + (before + after)


def start_of(b, below, above, ring, index):
    q, _, w = level(index)
    return w * ((4.0 / 3.0) * b + (w * q) * (ring(b) + (below + above)))


def left_of(b, u, below, above, ring, index):
    q, diag, _ = level(index)
    return b - diag * u + q * (ring(u) + (below + above))


def sweep_of(b, u, below, above, ring, index):
    q, _, w = level(index)
    return (1.0 - RELAX) * u + (w * b + (w * q) * (ring(u) + (below + above)))


def dot(left, right):
    return lax.dot_general(
        left, right, (((1,), (0,)), ((), ())), precision=HIGH, preferred_element_type=F32
    )


def lanes(test):
    return test(iota((128, 128), 0), iota((128, 128), 1))


def place_kernel(
    meta_ref, pay_ref, fluid_ref,
    src_ref, bottom_ref, top_ref, up_ref, down_ref, up2_ref, down2_ref, lift_ref,
    grid_ref, u_ref, sum_ref,
):
    slots = pay_ref.shape[0]
    lane = iota((8, 128), 1)
    sub = iota((8, 128), 0)
    for z in range(CZ):
        for c in range(3):
            grid_ref[3 * z + c, 0:128, :] = fluid_ref[z, c]
            grid_ref[3 * z + c, 128:144, :] = jnp.zeros((16, 128), F32)

    def turned(tile, head, base_y):
        base_x = jnp.maximum(head - 1, 0)
        shift = base_x & 7
        row = pl.multiple_of(base_x - shift, 8)
        window = (lane - base_y) & 127
        inside = (window >= 1) & (window <= BOX - 2) & (head > 0)
        late = inside & (sub >= shift)
        early = inside & (sub < shift)
        values = []
        for c in range(3):
            piece = pltpu.roll(tile[8 * c : 8 * c + 8], shift, 0)
            for g in range(8):
                values.append(pltpu.roll(piece, (base_y - BOX * g) & 127, 1))
        return row, late, early, values

    def add(row, late, early, values):
        for k in range(CZ):
            for c in range(3):
                first = values[8 * c + k]
                second = values[8 * c + 4 + k]
                kc = 3 * k + c
                grid_ref[kc, pl.ds(row, 8), :] += jnp.where(late, first, 0.0)
                grid_ref[kc, pl.ds(row + 8, 8), :] += jnp.where(
                    early, first, jnp.where(late, second, 0.0)
                )
                grid_ref[kc, pl.ds(row + 16, 8), :] += jnp.where(early, second, 0.0)

    group = together(slots, 2)

    def several(step, carry):
        found = []
        for n in range(group):
            d = step * group + n
            tile = pay_ref[d].astype(F32)
            carry = tuple(
                carry[c] + jnp.where(held, tile[8 * c : 8 * c + 8], 0.0) for c in range(3)
            )
            for order in range(2):
                found.append(
                    turned(
                        tile[order * ROWS : (order + 1) * ROWS],
                        meta_ref[4 * d + 2 * order],
                        meta_ref[4 * d + 2 * order + 1],
                    )
                )
        for one in found:
            add(*one)
        return carry

    held = (sub == 0) & ((lane == PIECES[0]) | (lane == PIECES[1]) | (lane == PIECES[2]))
    zero = jnp.zeros((8, 128), F32)
    totals = lax.fori_loop(0, slots // group, several, (zero, zero, zero))
    factor = (1.0 - level(3)[2] * SCREEN) ** 6 / SCREEN
    for index in range(3):
        factor = factor * (1.0 - level(index)[2] * SCREEN) ** 2
    scale = factor / (slots * CZ * 128.0 * 128.0)
    lift_ref[...] = zero
    for c in range(3):
        total = jnp.sum(totals[c], axis=(0, 1), keepdims=True)
        lift_ref[c : c + 1, :] = jnp.broadcast_to(total * scale, (1, 128))
    pool = [
        jnp.where(lanes(lambda r, l: (r // 2 == (l & 63)) & (l // 64 == half)), 0.125, 0.0)
        for half in range(2)
    ]
    q, diag, w = level(0)
    spill_up, spill_down = [], []
    for c in range(3):
        for z in range(CZ):
            kc = 3 * z + c
            grid_ref[kc, 0:16, :] += grid_ref[kc, 128:144, :]
            value = grid_ref[kc, 0:128, :]
            src_ref[z, c] = value
            if z < 3:
                bottom_ref[z, c] = value
            if z > 0:
                top_ref[z - 1, c] = value

        def b_at(z):
            return src_ref[z, c] if 0 <= z < CZ else 0.0

        for z in range(CZ):
            u_ref[z + 1] = start_of(src_ref[z, c], b_at(z - 1), b_at(z + 1), flat_ring, 0)
        u_ref[0] = (w * w * q) * src_ref[0, c]
        u_ref[CZ + 1] = (w * w * q) * src_ref[CZ - 1, c]

        def left(z):
            if z == -2:
                return q * u_ref[0]
            if z == CZ + 1:
                return q * u_ref[CZ + 1]
            below = u_ref[z] if z > -1 else 0.0
            above = u_ref[z + 2] if z < CZ else 0.0
            return left_of(b_at(z), u_ref[z + 1], below, above, flat_ring, 0)

        rows = []
        for pair in range(-1, 3):
            sum_ref[...] = left(2 * pair) + left(2 * pair + 1)
            rows.append(sum_ref[pl.ds(0, 64, 2), :] + sum_ref[pl.ds(1, 64, 2), :])
        own = dot(rows[1], pool[0]) + dot(rows[2], pool[1])
        up_ref[c] = own
        down_ref[c] = own
        spill_down.append(dot(rows[0], pool[c % 2]))
        spill_up.append(dot(rows[3], pool[c % 2]))
    for ref, far_ref, spill in ((up_ref, up2_ref, spill_up), (down_ref, down2_ref, spill_down)):
        both = spill[0] + spill[1]
        ref[3] = both
        ref[4] = spill[2]
        far_ref[0] = both
        far_ref[1] = spill[2]


def place(meta, payload, fluid):
    width = fluid.shape[2]
    return call(
        place_kernel,
        (
            shaped(fluid.shape, F32),
            shaped((3, 3, width, width), F32),
            shaped((3, 3, width, width), F32),
            shaped((5, 64, 128), F32),
            shaped((5, 64, 128), F32),
            shaped((2, 64, 128), F32),
            shaped((2, 64, 128), F32),
            shaped((8, 128), F32),
        ),
        [SMEM, VMEM, VMEM],
        [
            pltpu.VMEM((12, 144, 128), F32),
            pltpu.VMEM((CZ + 2, 128, 128), F32),
            pltpu.VMEM((128, 128), F32),
        ],
        "place",
    )(meta, near(payload), fluid)


def both_layers(tile):
    lane = iota(tile.shape, tile.ndim - 1)
    turned = pltpu.roll(tile, 64, tile.ndim - 1)
    return jnp.where(lane < 64, tile, turned), jnp.where(lane < 64, turned, tile)


def pack_coarse(value):
    last = value[24:32]
    lane = iota((8, 128), 1)
    return [
        jnp.where(lane < 96, value[8 * c : 8 * c + 8], pltpu.roll(last, 96 - 32 * c, 1))
        for c in range(3)
    ]


def unpack_coarse(tile):
    lane = iota((8, 128), 1)
    last = jnp.zeros((8, 128), F32)
    rows = []
    for c in range(3):
        piece = tile[8 * c : 8 * c + 8]
        turned = pltpu.roll(piece, (32 * c - 96) % 128, 1)
        last = jnp.where(lane // 32 == c, turned, last)
        rows.append(jnp.where(lane < 96, piece, 0.0))
    return jnp.concatenate(rows + [last], axis=0)


def spilled(ref, c, first=0):
    return both_layers(ref[first + c // 2])[c % 2]


def middle_kernel(
    up_ref, down_ref, m1_ref, p1_ref, m2_ref, p2_ref, pairs_ref, own_ref, out_ref, sum_ref
):
    total = None
    lane = iota((64, 128), 1)
    for c in range(3):
        m1, own, p1 = both_layers(m1_ref[c]), both_layers(up_ref[c]), both_layers(p1_ref[c])
        b = [
            m1[0] + spilled(m2_ref, c),
            m1[1] + spilled(down_ref, c, 3),
            own[0] + spilled(m1_ref, c, 3),
            own[1] + spilled(p1_ref, c, 3),
            p1[0] + spilled(up_ref, c, 3),
            p1[1] + spilled(p2_ref, c),
        ]
        for j in range(3):
            pair = jnp.where(lane < 64, b[2 * j], b[2 * j + 1])
            pairs_ref[j, c] = pair
            if j == 1:
                own_ref[c] = pair
        u = [start_of(b[i], b[i - 1], b[i + 1], flat_ring, 1) for i in range(1, 5)]
        left = [left_of(b[i + 1], u[i], u[i - 1], u[i + 1], flat_ring, 1) for i in (1, 2)]
        sum_ref[...] = left[0] + left[1]
        rows = sum_ref[pl.ds(0, 32, 2), :] + sum_ref[pl.ds(1, 32, 2), :]
        pool = jnp.where(
            lanes(lambda r, l: (r // 2 == (l & 31)) & (l // 32 == c) & (r < 64)), 0.125, 0.0
        )
        part = dot(rows, pool)
        total = part if total is None else total + part
    packed = jnp.concatenate(pack_coarse(total), axis=0)
    for d in range(out_ref.shape[0]):
        out_ref[d] = packed


def middle_down(up, down, m1, p1, m2, p2):
    return call(
        middle_kernel,
        (
            shaped((3, 3, 64, 128), F32),
            shaped((3, 64, 128), F32),
            shaped((LOCAL, 24, 128), F32),
        ),
        None,
        [pltpu.VMEM((64, 128), F32)],
        "middle_down",
    )(*map(near, (up, down, m1, p1, m2, p2)))


def inner(x):
    return x[1:-1]


def coarse_part(me, blocks, lift_ref, window_ref, pool_ref, final_ref):
    parity = me % 2
    first = me % LOCAL - parity
    for n, ref in enumerate(blocks):
        window_ref[LOCAL * n : LOCAL * n + LOCAL] = ref[...]
    b2 = jnp.stack([unpack_coarse(window_ref[first + t]) for t in range(34)])
    group = iota((1, 128), 1) // 32
    lift = jnp.zeros((1, 128), F32)
    for c in range(3):
        lift = jnp.where(group == c, lift_ref[c : c + 1, :], lift)
    _, _, w3 = level(3)
    u2 = start_of(inner(b2), b2[:-2], b2[2:], group_ring, 2)
    r2 = left_of(b2[2:-2], inner(u2), u2[:-2], u2[2:], group_ring, 2)
    pairs = r2.reshape(15, 2, 32, 128)
    pool_ref[...] = (pairs[:, 0] + pairs[:, 1]).reshape(480, 128)
    rows = pool_ref[pl.ds(0, 240, 2), :] + pool_ref[pl.ds(1, 240, 2), :]
    pool = jnp.where(
        lanes(lambda r, l: ((r & 31) // 2 == (l & 15)) & (r // 32 == l // 32)), 0.125, 0.0
    )
    b3 = dot(rows, pool).reshape(15, 16, 128)
    u3 = w3 * b3
    for _ in range(5):
        b3 = inner(b3)
        u3 = sweep_of(b3, inner(u3), u3[:-2], u3[2:], group_ring, 3)
    u3 = (u3 + lift[None]).reshape(80, 128)
    spread = jnp.where(
        lanes(lambda r, l: ((l & 31) // 2 == (r & 31)) & (r // 32 == l // 32)), 1.0, 0.0
    )
    wide = dot(u3, spread)
    pool_ref[pl.ds(0, 80, 2), :] = wide
    pool_ref[pl.ds(1, 80, 2), :] = wide
    lifted = pool_ref[0:160, :].reshape(5, 1, 32, 128)
    u = (u2[11:21].reshape(5, 2, 32, 128) + lifted).reshape(10, 32, 128)
    u = sweep_of(b2[13:21], inner(u), u[:-2], u[2:], group_ring, 2)
    u = sweep_of(b2[14:20], inner(u), u[:-2], u[2:], group_ring, 2)
    final_ref[...] = u
    return jnp.concatenate([final_ref[parity + h] for h in range(5)], axis=0)


def up_kernel(
    me_ref, meta_ref, lift_ref, g0_ref, g1_ref, g2_ref, g3_ref, g4_ref,
    m2_ref, pairs_ref, p2_ref, low_ref, own_ref, high_ref, vel_ref, pay_ref,
    window_ref, pool_ref, final_ref, lift1_ref, b1_ref, u1_ref, v1_ref, lift0_ref, u0_ref,
    v0_ref, ext_ref,
):
    blocks = (g0_ref, g1_ref, g2_ref, g3_ref, g4_ref)
    coarse = coarse_part(me_ref[0], blocks, lift_ref, window_ref, pool_ref, final_ref)
    for c in range(3):
        spread = jnp.where(lanes(lambda r, l: r == 32 * c + (l & 63) // 2), 1.0, 0.0)
        wide = dot(coarse, spread)
        lift1_ref[c, pl.ds(0, 160, 2), :] = wide
        lift1_ref[c, pl.ds(1, 160, 2), :] = wide
    spread0 = jnp.where(lanes(lambda r, l: r == l // 2), 1.0, 0.0)

    def b_at(z, c):
        if z < 0:
            return low_ref[z + 3, c]
        return own_ref[z, c] if z < CZ else high_ref[z - CZ, c]

    def component(c, carry):
        tiles = [m2_ref[c]] + [pairs_ref[j, c] for j in range(3)] + [p2_ref[c]]
        for j, tile in enumerate(tiles):
            b1_ref[2 * j], b1_ref[2 * j + 1] = both_layers(tile)
        for z in range(-3, 5):
            i = z + 4
            h = z // 2 + 2
            u1_ref[z + 3] = (
                start_of(b1_ref[i], b1_ref[i - 1], b1_ref[i + 1], flat_ring, 1)
                + lift1_ref[c, 64 * h : 64 * h + 64, :]
            )
        for z in range(-2, 4):
            i = z + 3
            v1_ref[z + 2] = sweep_of(
                b1_ref[z + 4], u1_ref[i], u1_ref[i - 1], u1_ref[i + 1], flat_ring, 1
            )
        for z in range(-1, 3):
            i = z + 2
            value = sweep_of(
                b1_ref[z + 4], v1_ref[i], v1_ref[i - 1], v1_ref[i + 1], flat_ring, 1
            )
            wide = dot(value, spread0)
            lift0_ref[z + 1, pl.ds(0, 64, 2), :] = wide
            lift0_ref[z + 1, pl.ds(1, 64, 2), :] = wide
        for z in range(-2, 6):
            u0_ref[z + 2] = (
                start_of(b_at(z, c), b_at(z - 1, c), b_at(z + 1, c), flat_ring, 0)
                + lift0_ref[z // 2 + 1]
            )
        for z in range(-1, 5):
            i = z + 2
            v0_ref[z + 1] = sweep_of(
                b_at(z, c), u0_ref[i], u0_ref[i - 1], u0_ref[i + 1], flat_ring, 0
            )
        for z in range(CZ):
            i = z + 1
            value = sweep_of(
                own_ref[z, c], v0_ref[i], v0_ref[i - 1], v0_ref[i + 1], flat_ring, 0
            )
            vel_ref[z, c] = value
            rounded = value.astype(BF16).astype(F32)
            ext_ref[3 * z + c, 0:128, :] = rounded
            ext_ref[3 * z + c, 128:144, :] = rounded[0:16]
        return carry

    lax.fori_loop(0, 3, component, 0)
    lane = iota((8, 128), 1)
    sub = iota((8, 128), 0)

    half = [lane // BOX == g for g in range(8)]

    def gather(head, base_y):
        base_x = jnp.maximum(head - 1, 0)
        shift = base_x & 7
        row = pl.multiple_of(base_x - shift, 8)
        late = sub >= shift
        values = []
        for k in range(CZ):
            for c in range(3):
                tiles = [ext_ref[3 * k + c, pl.ds(row + 8 * n, 8), :] for n in range(3)]
                for upper in range(2):
                    value = jnp.where(late, tiles[upper], tiles[upper + 1])
                    g = 4 * upper + k
                    values.append((c, g, pltpu.roll(value, (BOX * g - base_y) & 127, 1)))
        return (8 - shift) & 7, values

    group = together(pay_ref.shape[0], 2)

    def several(step, carry):
        found = []
        for n in range(group):
            d = step * group + n
            for order in range(2):
                found.append(
                    gather(meta_ref[4 * d + 2 * order], meta_ref[4 * d + 2 * order + 1])
                )
        for n in range(group):
            pieces = []
            for order in range(2):
                back, values = found[2 * n + order]
                for c in range(3):
                    packed = jnp.zeros((8, 128), F32)
                    for own_c, g, value in values:
                        if own_c == c:
                            packed = jnp.where(half[g], value, packed)
                    pieces.append(pltpu.roll(packed, back, 0))
            pay_ref[step * group + n] = jnp.concatenate(pieces, axis=0).astype(BF16)
        return carry

    lax.fori_loop(0, pay_ref.shape[0] // group, several, 0)


def way_up(me, meta, lift, blocks, m2, pairs, p2, low, own, high, slots):
    return call(
        up_kernel,
        (
            shaped(own.shape, F32, False),
            shaped((slots, 2 * ROWS, 128), BF16),
        ),
        [SMEM, SMEM] + [VMEM] * 12,
        [
            pltpu.VMEM((5 * LOCAL, 24, 128), F32),
            pltpu.VMEM((480, 128), F32),
            pltpu.VMEM((6, 32, 128), F32),
            pltpu.VMEM((3, 320, 128), F32),
            pltpu.VMEM((10, 64, 128), F32),
            pltpu.VMEM((8, 64, 128), F32),
            pltpu.VMEM((6, 64, 128), F32),
            pltpu.VMEM((4, 128, 128), F32),
            pltpu.VMEM((8, 128, 128), F32),
            pltpu.VMEM((6, 128, 128), F32),
            pltpu.VMEM((12, 144, 128), F32),
        ],
        "way_up",
    )(me, meta, *map(near, (lift, *blocks, m2, pairs, p2, low, own, high)))


def read_kernel(dest_ref, pay_ref, pos_ref, out_ref, stage_ref, count_ref):
    slots = pay_ref.shape[0]

    def widen(t, carry):
        count_ref[t] = 0
        stage_ref[t] = pay_ref[t].astype(F32)
        return carry

    lax.fori_loop(0, slots, widen, 0, unroll=4)
    lane = iota((8, 128), 1)

    group = together(pos_ref.shape[1], 4)

    def one(block, target, order):
        weight_x, weight_y, weight_z = box_weights(pos_ref, block)
        lower, upper = [], []
        for c in range(3):
            row = pl.multiple_of(order * ROWS + 8 * c, 8)
            packed = stage_ref[target, pl.ds(row, 8), :]
            swapped = pltpu.roll(packed, 64, 1)
            lower.append(jnp.where(lane < 64, packed, swapped))
            upper.append(jnp.where(lane < 64, swapped, packed))
        left = jnp.concatenate(
            [half for pair in zip(lower, upper) for half in pair], axis=0
        ).astype(BF16)
        right = jnp.concatenate(by_levels(weight_y, weight_z), axis=0)
        spread = lax.dot_general(
            left, right, (((1,), (0,)), ((), ())), preferred_element_type=F32
        )
        for c in range(3):
            value = spread[BOX * c : BOX * c + BOX] * weight_x
            out_ref[c, pl.ds(block, 1), :] = jnp.sum(value, axis=0, keepdims=True)

    def several(step, carry):
        places = []
        for n in range(group):
            target = dest_ref[0, step * group + n]
            order = count_ref[target]
            count_ref[target] = order + 1
            places.append((target, order))
        for n in range(group):
            one(step * group + n, *places[n])
        return carry

    lax.fori_loop(0, pos_ref.shape[1] // group, several, 0)


def read(dest, payload, positions):
    slots = payload.shape[0]
    return call(
        read_kernel,
        shaped(positions.shape, F32, False),
        [SMEM, VMEM, VMEM],
        [pltpu.VMEM((slots, 2 * ROWS, 128), F32), pltpu.SMEM((slots,), jnp.int32)],
        "read",
    )(dest, near(payload), positions)


def moved(value, step):
    size = lax.axis_size(AX)
    return lax.ppermute(value, AX, [(i, (i + step) % size) for i in range(size)])


def exchanged(value, axes=AX):
    return lax.all_to_all(value, axes, split_axis=0, concat_axis=0, tiled=True)


def shards(marker_positions, marker_forces, dest_slab, base_cells, fluid_source):
    slots = lax.axis_size(AX)
    positions = marker_positions.transpose(1, 0, 2)
    forces = marker_forces.transpose(1, 0, 2)
    dest = dest_slab.T
    me = lax.axis_index(AX).astype(jnp.int32).reshape(1)
    payload = exchanged(build(dest, base_cells.T, positions, forces, fluid_source, slots))
    heads = payload[:, 0 : ROWS + 1 : ROWS, 0 : BOX + 1 : BOX]
    meta = heads.astype(jnp.int32).reshape(4 * slots)
    source, bottom, top, up, down, up2, down2, lift = place(meta, payload, fluid_source)
    m1, p1 = moved(up, 1), moved(down, -1)
    m2, p2 = moved(up2, 2), moved(down2, -2)
    m1, p1, m2, p2, bottom, top = lax.optimization_barrier((m1, p1, m2, p2, bottom, top))
    low, high = moved(top, 1), moved(bottom, -1)
    pairs, tile, share = middle_down(up, down, m1, p1, m2, p2)
    middle = exchanged(share, AX[1])
    blocks = [middle if n == 0 else moved(middle, -LOCAL * n) for n in range(-2, 3)]
    velocity, picked = way_up(
        me, meta, lift, blocks, moved(tile, 2), pairs, moved(tile, -2), low, source, high, slots
    )
    out = read(dest, exchanged(picked), positions)
    return velocity, out.transpose(1, 0, 2)


def solution(mesh):
    torus = Mesh(mesh.devices.reshape(-1, LOCAL), AX)
    return jax.shard_map(
        shards,
        mesh=torus,
        in_specs=(P(AX), P(AX), P(AX), P(AX), P(AX)),
        out_specs=(P(AX), P(AX)),
        check_vma=False,
    )
```

```python
import math

import jax
import jax.numpy as jnp
from jax import lax
from jax.experimental import pallas as pl
from jax.experimental.pallas import tpu as pltpu
from jax.sharding import Mesh
from jax.sharding import PartitionSpec as P

AX = ("hi", "lo")
LOCAL = 8
BOX = 16
CZ = 4
ROWS = 24
SCREEN = 1.0 / 64.0
RELAX = 2.0 / 3.0
INTERPRET = False
F32 = jnp.float32
BF16 = jnp.bfloat16
HIGH = lax.Precision.HIGHEST


def level(index):
    q = 0.25**index
    return q, SCREEN + 6.0 * q, RELAX / (SCREEN + 6.0 * q)


def call(body, out_shape, in_specs=None, scratch=(), megabytes=24):
    options = {} if in_specs is None else {"in_specs": in_specs}
    return pl.pallas_call(
        body,
        out_shape=out_shape,
        scratch_shapes=list(scratch),
        interpret=INTERPRET,
        compiler_params=pltpu.CompilerParams(vmem_limit_bytes=megabytes << 20),
        **options,
    )


def shaped(shape, dtype, near=True):
    if near and not INTERPRET:
        return pltpu.VMEM(shape, dtype)
    return jax.ShapeDtypeStruct(shape, dtype)


def near(value):
    return value if INTERPRET else pltpu.with_memory_space_constraint(value, pltpu.VMEM)


VMEM = pl.BlockSpec(memory_space=pltpu.VMEM)
SMEM = pl.BlockSpec(memory_space=pltpu.SMEM)


def far(value):
    return value if INTERPRET else pltpu.with_memory_space_constraint(value, pltpu.HBM)


def iota(shape, dim):
    return lax.broadcasted_iota(jnp.int32, shape, dim)


COS = (
    0.13884009367929634,
    0.008677498753340366,
    0.0001925760632832398,
    2.2059131886721028e-06,
    1.644977822379996e-08,
)


def phi(offset):
    inside = jnp.maximum(4.0 - offset * offset, 0.0)
    value = inside * COS[-1] + COS[-2]
    for coefficient in COS[-3::-1]:
        value = value * inside + coefficient
    value = value * inside
    return value * value


def split(value):
    high = value.astype(BF16)
    return high, (value - high.astype(F32)).astype(BF16)


def box_weights(pos_ref, block):
    cells = iota((BOX, 256), 0).astype(F32)
    levels = iota((8, 256), 0).astype(F32)
    row = pl.ds(block, 1)
    along_x = 2.0 + (BOX - 5) * pos_ref[0, row, :]
    along_y = 2.0 + (BOX - 5) * pos_ref[1, row, :]
    height = (CZ - 1) * pos_ref[2, row, :]
    return phi(along_x - cells), phi(along_y - cells), phi(height - levels)


def by_levels(weight_y, weight_z):
    return split(jnp.concatenate([weight_z[k : k + 1] * weight_y for k in range(CZ)], axis=0))


PIECES = (2 * BOX, 3 * BOX, 4 * BOX)


def together(count, most):
    return math.gcd(count, most)


def build_kernel(
    dest_ref, base_ref, pos_ref, frc_ref, fluid_ref, out_ref, stage_ref, count_ref
):
    slots = out_ref.shape[0]
    blocks = pos_ref.shape[1]
    group = together(blocks, 8)

    def clear(t, carry):
        count_ref[t] = 0
        for order in range(2):
            stage_ref[t, order * ROWS : order * ROWS + 8, :] = jnp.zeros((8, 128), F32)
        return carry

    lax.fori_loop(0, slots, clear, 0, unroll=4)
    lane = iota((8, 128), 1)
    top = iota((8, 128), 0) == 0

    def one(block):
        weight_x, weight_y, weight_z = box_weights(pos_ref, block)
        loaded = [frc_ref[c, pl.ds(block, 1), :] * weight_x for c in range(3)]
        high, low = split(jnp.concatenate(loaded, axis=0))
        right = jnp.concatenate(by_levels(weight_y, weight_z), axis=0)
        dims = (((1,), (1,)), ((), ()))
        box = lax.dot_general(high, right, dims, preferred_element_type=F32)
        box = box + lax.dot_general(low, right, dims, preferred_element_type=F32)
        box = box + pltpu.roll(box, 64, 1)
        base_x = base_ref[0, block].astype(F32) + 1.0
        base_y = base_ref[1, block].astype(F32)
        tiles, sums = [], []
        for c in range(3):
            tile = jnp.where(
                lane < 64, box[BOX * c : BOX * c + 8], box[BOX * c + 8 : BOX * c + 16]
            )
            sums.append(tile.astype(BF16).astype(F32))
            if c == 0:
                tile = jnp.where(top & (lane == 0), base_x, tile)
                tile = jnp.where(top & (lane == BOX), base_y, tile)
            tiles.append(tile)
        return tiles, sums

    def several(step, carry):
        results = []
        for n in range(group):
            tiles, sums = one(step * group + n)
            results.append(tiles)
            carry = tuple(a + b for a, b in zip(carry, sums))
        for n in range(group):
            target = dest_ref[0, step * group + n]
            order = count_ref[target]
            count_ref[target] = order + 1
            for c in range(3):
                row = pl.multiple_of(order * ROWS + 8 * c, 8)
                stage_ref[target, pl.ds(row, 8), :] = results[n][c]
        return carry

    fluid = []
    for c in range(3):
        column = fluid_ref[0, c] + fluid_ref[1, c] + (fluid_ref[2, c] + fluid_ref[3, c])
        fluid.append(jnp.sum(column.reshape(16, 8, 128), axis=0))
    fluid = lax.fori_loop(0, blocks // group, several, tuple(fluid))
    pieces = []
    for c in range(3):
        rest = jnp.broadcast_to(jnp.sum(fluid[c], axis=(0, 1), keepdims=True), (8, 128))
        marked = jnp.zeros((8, 128), F32)
        for place_of in PIECES:
            part = rest.astype(BF16).astype(F32)
            marked = jnp.where(lane == place_of, part, marked)
            rest = rest - part
        pieces.append(marked)
    held = top & ((lane == PIECES[0]) | (lane == PIECES[1]) | (lane == PIECES[2]))

    def finish(t, carry):
        tiles = [
            jnp.where(held, pieces[c], stage_ref[t, 8 * c : 8 * c + 8, :]) for c in range(3)
        ]
        tiles.append(stage_ref[t, ROWS : 2 * ROWS, :])
        out_ref[t] = jnp.concatenate(tiles, axis=0).astype(BF16)
        return carry

    lax.fori_loop(0, slots, finish, 0, unroll=4)


def build(dest, base, positions, forces, fluid, slots):
    return call(
        build_kernel,
        shaped((slots, 2 * ROWS, 128), BF16),
        [SMEM, SMEM, VMEM, VMEM, VMEM],
        [pltpu.VMEM((slots, 2 * ROWS, 128), F32), pltpu.SMEM((slots,), jnp.int32)],
    )(*map(far, (dest, base, positions, forces, fluid)))


def flat_ring(x):
    rows = x.shape[-2]
    ax = x.ndim - 2
    return (
        pltpu.roll(x, 1, ax)
        + pltpu.roll(x, rows - 1, ax)
        + (pltpu.roll(x, 1, ax + 1) + pltpu.roll(x, 127, ax + 1))
    )


def group_ring(x):
    rows = x.shape[-2]
    ax = x.ndim - 2
    lane = iota(x.shape, ax + 1) & 31
    before = jnp.where(lane == 0, pltpu.roll(x, 97, ax + 1), pltpu.roll(x, 1, ax + 1))
    after = jnp.where(lane == 31, pltpu.roll(x, 31, ax + 1), pltpu.roll(x, 127, ax + 1))
    return pltpu.roll(x, 1, ax) + pltpu.roll(x, rows - 1, ax) + (before + after)


def start_of(b, below, above, ring, index):
    q, _, w = level(index)
    return w * ((4.0 / 3.0) * b + (w * q) * (ring(b) + (below + above)))


def left_of(b, u, below, above, ring, index):
    q, diag, _ = level(index)
    return b - diag * u + q * (ring(u) + (below + above))


def sweep_of(b, u, below, above, ring, index):
    q, _, w = level(index)
    return (1.0 - RELAX) * u + (w * b + (w * q) * (ring(u) + (below + above)))


def dot(left, right):
    return lax.dot_general(
        left, right, (((1,), (0,)), ((), ())), precision=HIGH, preferred_element_type=F32
    )


def lanes(test):
    return test(iota((128, 128), 0), iota((128, 128), 1))


def place_kernel(
    meta_ref, pay_ref, fluid_ref,
    src_ref, up_ref, down_ref, up2_ref, down2_ref, lift_ref,
    grid_ref, u_ref, sum_ref,
):
    slots = pay_ref.shape[0]
    lane = iota((8, 128), 1)
    sub = iota((8, 128), 0)
    for z in range(CZ):
        for c in range(3):
            grid_ref[3 * z + c, 0:128, :] = fluid_ref[z, c]
            grid_ref[3 * z + c, 128:144, :] = jnp.zeros((16, 128), F32)

    def turned(tile, head, base_y):
        base_x = jnp.maximum(head - 1, 0)
        shift = base_x & 7
        row = pl.multiple_of(base_x - shift, 8)
        window = (lane - base_y) & 127
        inside = (window >= 1) & (window <= BOX - 2) & (head > 0)
        late = inside & (sub >= shift)
        early = inside & (sub < shift)
        values = []
        for c in range(3):
            piece = pltpu.roll(tile[8 * c : 8 * c + 8], shift, 0)
            for g in range(8):
                values.append(pltpu.roll(piece, (base_y - BOX * g) & 127, 1))
        return row, late, early, values

    def add(row, late, early, values):
        for k in range(CZ):
            for c in range(3):
                first = values[8 * c + k]
                second = values[8 * c + 4 + k]
                kc = 3 * k + c
                grid_ref[kc, pl.ds(row, 8), :] += jnp.where(late, first, 0.0)
                grid_ref[kc, pl.ds(row + 8, 8), :] += jnp.where(
                    early, first, jnp.where(late, second, 0.0)
                )
                grid_ref[kc, pl.ds(row + 16, 8), :] += jnp.where(early, second, 0.0)

    group = together(slots, 4)

    def several(step, carry):
        found = []
        for n in range(group):
            d = step * group + n
            tile = pay_ref[d].astype(F32)
            carry = tuple(
                carry[c] + jnp.where(held, tile[8 * c : 8 * c + 8], 0.0) for c in range(3)
            )
            for order in range(2):
                found.append(
                    turned(
                        tile[order * ROWS : (order + 1) * ROWS],
                        meta_ref[4 * d + 2 * order],
                        meta_ref[4 * d + 2 * order + 1],
                    )
                )
        for one in found:
            add(*one)
        return carry

    held = (sub == 0) & ((lane == PIECES[0]) | (lane == PIECES[1]) | (lane == PIECES[2]))
    zero = jnp.zeros((8, 128), F32)
    totals = lax.fori_loop(0, slots // group, several, (zero, zero, zero))
    factor = (1.0 - level(3)[2] * SCREEN) ** 6 / SCREEN
    for index in range(3):
        factor = factor * (1.0 - level(index)[2] * SCREEN) ** 2
    scale = factor / (slots * CZ * 128.0 * 128.0)
    lift_ref[...] = zero
    for c in range(3):
        total = jnp.sum(totals[c], axis=(0, 1), keepdims=True)
        lift_ref[c : c + 1, :] = jnp.broadcast_to(total * scale, (1, 128))
    pool = [
        jnp.where(lanes(lambda r, l: (r // 2 == (l & 63)) & (l // 64 == half)), 0.125, 0.0)
        for half in range(2)
    ]
    q, _, w = level(0)
    spill_up, spill_down = [], []
    for c in range(3):
        for z in range(CZ):
            kc = 3 * z + c
            grid_ref[kc, 0:16, :] += grid_ref[kc, 128:144, :]
            src_ref[z, c] = grid_ref[kc, 0:128, :]

        def b_at(z):
            return src_ref[z, c] if 0 <= z < CZ else 0.0

        for z in range(CZ):
            u_ref[z + 1] = start_of(src_ref[z, c], b_at(z - 1), b_at(z + 1), flat_ring, 0)
        u_ref[0] = (w * w * q) * src_ref[0, c]
        u_ref[CZ + 1] = (w * w * q) * src_ref[CZ - 1, c]

        def left(z):
            if z == -2:
                return q * u_ref[0]
            if z == CZ + 1:
                return q * u_ref[CZ + 1]
            below = u_ref[z] if z > -1 else 0.0
            above = u_ref[z + 2] if z < CZ else 0.0
            return left_of(b_at(z), u_ref[z + 1], below, above, flat_ring, 0)

        rows = []
        for pair in range(-1, 3):
            sum_ref[...] = left(2 * pair) + left(2 * pair + 1)
            rows.append(sum_ref[pl.ds(0, 64, 2), :] + sum_ref[pl.ds(1, 64, 2), :])
        own = dot(rows[1], pool[0]) + dot(rows[2], pool[1])
        up_ref[c] = own
        down_ref[c] = own
        spill_down.append(dot(rows[0], pool[c % 2]))
        spill_up.append(dot(rows[3], pool[c % 2]))
    for ref, far_ref, spill in ((up_ref, up2_ref, spill_up), (down_ref, down2_ref, spill_down)):
        both = spill[0] + spill[1]
        ref[3] = both
        ref[4] = spill[2]
        far_ref[0] = both
        far_ref[1] = spill[2]


def place(meta, payload, fluid):
    return call(
        place_kernel,
        (
            shaped(fluid.shape, F32),
            shaped((5, 64, 128), F32),
            shaped((5, 64, 128), F32),
            shaped((2, 64, 128), F32),
            shaped((2, 64, 128), F32),
            shaped((8, 128), F32),
        ),
        [SMEM, VMEM, VMEM],
        [
            pltpu.VMEM((12, 144, 128), F32),
            pltpu.VMEM((CZ + 2, 128, 128), F32),
            pltpu.VMEM((128, 128), F32),
        ],
    )(meta, near(payload), far(fluid))


def both_layers(tile):
    lane = iota(tile.shape, tile.ndim - 1)
    turned = pltpu.roll(tile, 64, tile.ndim - 1)
    return jnp.where(lane < 64, tile, turned), jnp.where(lane < 64, turned, tile)


def pack_coarse(value):
    last = value[24:32]
    lane = iota((8, 128), 1)
    return [
        jnp.where(lane < 96, value[8 * c : 8 * c + 8], pltpu.roll(last, 96 - 32 * c, 1))
        for c in range(3)
    ]


def unpack_coarse(tile):
    lane = iota((8, 128), 1)
    last = jnp.zeros((8, 128), F32)
    rows = []
    for c in range(3):
        piece = tile[8 * c : 8 * c + 8]
        turned = pltpu.roll(piece, (32 * c - 96) % 128, 1)
        last = jnp.where(lane // 32 == c, turned, last)
        rows.append(jnp.where(lane < 96, piece, 0.0))
    return jnp.concatenate(rows + [last], axis=0)


def spilled(ref, c, first=0):
    return both_layers(ref[first + c // 2])[c % 2]


U_ROW = 9 * 128


def middle_kernel(
    src_ref, up_ref, down_ref, m1_ref, p1_ref, m2_ref, p2_ref,
    pairs_ref, out_ref, rise_ref, sink_ref, sum_ref,
):
    total = None
    for z in range(3):
        for c in range(3):
            rows = slice(128 * (3 * z + c), 128 * (3 * z + c + 1))
            rise_ref[rows, :] = src_ref[z + 1, c]
            sink_ref[rows, :] = src_ref[z, c]
    lane = iota((64, 128), 1)
    for c in range(3):
        m1, own, p1 = both_layers(m1_ref[c]), both_layers(up_ref[c]), both_layers(p1_ref[c])
        b = [
            m1[0] + spilled(m2_ref, c),
            m1[1] + spilled(down_ref, c, 3),
            own[0] + spilled(m1_ref, c, 3),
            own[1] + spilled(p1_ref, c, 3),
            p1[0] + spilled(up_ref, c, 3),
            p1[1] + spilled(p2_ref, c),
        ]
        for j in range(3):
            pairs_ref[j, c] = jnp.where(lane < 64, b[2 * j], b[2 * j + 1])
        u = [start_of(b[i], b[i - 1], b[i + 1], flat_ring, 1) for i in range(1, 5)]
        rows = slice(U_ROW + 64 * c, U_ROW + 64 * c + 64)
        rise_ref[rows, :] = jnp.where(lane < 64, u[0], u[1])
        sink_ref[rows, :] = jnp.where(lane < 64, u[2], u[3])
        left = [left_of(b[i + 1], u[i], u[i - 1], u[i + 1], flat_ring, 1) for i in (1, 2)]
        sum_ref[...] = left[0] + left[1]
        rows = sum_ref[pl.ds(0, 32, 2), :] + sum_ref[pl.ds(1, 32, 2), :]
        pool = jnp.where(
            lanes(lambda r, l: (r // 2 == (l & 31)) & (l // 32 == c) & (r < 64)), 0.125, 0.0
        )
        part = dot(rows, pool)
        total = part if total is None else total + part
    packed = jnp.concatenate(pack_coarse(total), axis=0)
    for d in range(out_ref.shape[0]):
        out_ref[d] = packed


def middle_down(source, up, down, m1, p1, m2, p2):
    return call(
        middle_kernel,
        (
            shaped((3, 3, 64, 128), F32),
            shaped((LOCAL, 24, 128), F32),
            shaped((U_ROW + 192, 128), F32),
            shaped((U_ROW + 192, 128), F32),
        ),
        None,
        [pltpu.VMEM((64, 128), F32)],
    )(*map(near, (source, up, down, m1, p1, m2, p2)))


def inner(x):
    return x[1:-1]


def coarse_part(me, blocks, lift_ref, window_ref, pool_ref, final_ref):
    parity = me % 2
    first = me % LOCAL - parity
    for n, ref in enumerate(blocks):
        window_ref[LOCAL * n : LOCAL * n + LOCAL] = ref[...]
    b2 = jnp.stack([unpack_coarse(window_ref[first + t]) for t in range(34)])
    group = iota((1, 128), 1) // 32
    lift = jnp.zeros((1, 128), F32)
    for c in range(3):
        lift = jnp.where(group == c, lift_ref[c : c + 1, :], lift)
    _, _, w3 = level(3)
    u2 = start_of(inner(b2), b2[:-2], b2[2:], group_ring, 2)
    r2 = left_of(b2[2:-2], inner(u2), u2[:-2], u2[2:], group_ring, 2)
    pairs = r2.reshape(15, 2, 32, 128)
    pool_ref[...] = (pairs[:, 0] + pairs[:, 1]).reshape(480, 128)
    rows = pool_ref[pl.ds(0, 240, 2), :] + pool_ref[pl.ds(1, 240, 2), :]
    pool = jnp.where(
        lanes(lambda r, l: ((r & 31) // 2 == (l & 15)) & (r // 32 == l // 32)), 0.125, 0.0
    )
    b3 = dot(rows, pool).reshape(15, 16, 128)
    u3 = w3 * b3
    for _ in range(5):
        b3 = inner(b3)
        u3 = sweep_of(b3, inner(u3), u3[:-2], u3[2:], group_ring, 3)
    u3 = (u3 + lift[None]).reshape(80, 128)
    spread = jnp.where(
        lanes(lambda r, l: ((l & 31) // 2 == (r & 31)) & (r // 32 == l // 32)), 1.0, 0.0
    )
    wide = dot(u3, spread)
    pool_ref[pl.ds(0, 80, 2), :] = wide
    pool_ref[pl.ds(1, 80, 2), :] = wide
    lifted = pool_ref[0:160, :].reshape(5, 1, 32, 128)
    u = (u2[11:21].reshape(5, 2, 32, 128) + lifted).reshape(10, 32, 128)
    u = sweep_of(b2[13:21], inner(u), u[:-2], u[2:], group_ring, 2)
    u = sweep_of(b2[14:20], inner(u), u[:-2], u[2:], group_ring, 2)
    final_ref[...] = u
    return jnp.concatenate([final_ref[parity + h] for h in range(5)], axis=0)


def up_kernel(
    me_ref, meta_ref, lift_ref, g0_ref, g1_ref, g2_ref, g3_ref, g4_ref,
    pairs_ref, low_ref, own_ref, high_ref, vel_ref, pay_ref,
    window_ref, pool_ref, final_ref, lift1_ref, b1_ref, u1_ref, v1_ref, lift0_ref, u0_ref,
    v0_ref, ext_ref,
):
    blocks = (g0_ref, g1_ref, g2_ref, g3_ref, g4_ref)
    coarse = coarse_part(me_ref[0], blocks, lift_ref, window_ref, pool_ref, final_ref)
    for c in range(3):
        spread = jnp.where(lanes(lambda r, l: r == 32 * c + (l & 63) // 2), 1.0, 0.0)
        wide = dot(coarse, spread)
        lift1_ref[c, pl.ds(0, 160, 2), :] = wide
        lift1_ref[c, pl.ds(1, 160, 2), :] = wide
    spread0 = jnp.where(lanes(lambda r, l: r == l // 2), 1.0, 0.0)

    def b_at(z, c):
        if 0 <= z < CZ:
            return own_ref[z, c]
        ref, first = (low_ref, z + 3) if z < 0 else (high_ref, z - CZ)
        return ref[pl.ds(pl.multiple_of(128 * (3 * first + c), 128), 128), :]

    def component(c, carry):
        for j in range(3):
            b1_ref[2 * j], b1_ref[2 * j + 1] = both_layers(pairs_ref[j, c])
        rows = pl.ds(pl.multiple_of(U_ROW + 64 * c, 64), 64)
        u1 = list(both_layers(low_ref[rows, :]))
        for i in range(1, 5):
            u1.append(start_of(b1_ref[i], b1_ref[i - 1], b1_ref[i + 1], flat_ring, 1))
        u1.extend(both_layers(high_ref[rows, :]))
        for z in range(-3, 5):
            h = z // 2 + 2
            u1_ref[z + 3] = u1[z + 3] + lift1_ref[c, 64 * h : 64 * h + 64, :]
        for z in range(-2, 4):
            i = z + 3
            v1_ref[z + 2] = sweep_of(
                b1_ref[z + 2], u1_ref[i], u1_ref[i - 1], u1_ref[i + 1], flat_ring, 1
            )
        for z in range(-1, 3):
            i = z + 2
            value = sweep_of(
                b1_ref[z + 2], v1_ref[i], v1_ref[i - 1], v1_ref[i + 1], flat_ring, 1
            )
            wide = dot(value, spread0)
            lift0_ref[z + 1, pl.ds(0, 64, 2), :] = wide
            lift0_ref[z + 1, pl.ds(1, 64, 2), :] = wide
        for z in range(-2, 6):
            u0_ref[z + 2] = (
                start_of(b_at(z, c), b_at(z - 1, c), b_at(z + 1, c), flat_ring, 0)
                + lift0_ref[z // 2 + 1]
            )
        for z in range(-1, 5):
            i = z + 2
            v0_ref[z + 1] = sweep_of(
                b_at(z, c), u0_ref[i], u0_ref[i - 1], u0_ref[i + 1], flat_ring, 0
            )
        for z in range(CZ):
            i = z + 1
            value = sweep_of(
                own_ref[z, c], v0_ref[i], v0_ref[i - 1], v0_ref[i + 1], flat_ring, 0
            )
            vel_ref[z, c] = value
            rounded = value.astype(BF16).astype(F32)
            ext_ref[3 * z + c, 0:128, :] = rounded
            ext_ref[3 * z + c, 128:144, :] = rounded[0:16]
        return carry

    lax.fori_loop(0, 3, component, 0)
    lane = iota((8, 128), 1)
    sub = iota((8, 128), 0)

    half = [lane // BOX == g for g in range(8)]

    def gather(head, base_y):
        base_x = jnp.maximum(head - 1, 0)
        shift = base_x & 7
        row = pl.multiple_of(base_x - shift, 8)
        late = sub >= shift
        values = []
        for k in range(CZ):
            for c in range(3):
                tiles = [ext_ref[3 * k + c, pl.ds(row + 8 * n, 8), :] for n in range(3)]
                for upper in range(2):
                    value = jnp.where(late, tiles[upper], tiles[upper + 1])
                    g = 4 * upper + k
                    values.append((c, g, pltpu.roll(value, (BOX * g - base_y) & 127, 1)))
        return (8 - shift) & 7, values

    group = together(pay_ref.shape[0], 4)

    def several(step, carry):
        found = []
        for n in range(group):
            d = step * group + n
            for order in range(2):
                found.append(
                    gather(meta_ref[4 * d + 2 * order], meta_ref[4 * d + 2 * order + 1])
                )
        for n in range(group):
            pieces = []
            for order in range(2):
                back, values = found[2 * n + order]
                for c in range(3):
                    packed = jnp.zeros((8, 128), F32)
                    for own_c, g, value in values:
                        if own_c == c:
                            packed = jnp.where(half[g], value, packed)
                    pieces.append(pltpu.roll(packed, back, 0))
            pay_ref[step * group + n] = jnp.concatenate(pieces, axis=0).astype(BF16)
        return carry

    lax.fori_loop(0, pay_ref.shape[0] // group, several, 0)


def way_up(me, meta, lift, blocks, pairs, low, own, high, slots):
    return call(
        up_kernel,
        (
            shaped(own.shape, F32, False),
            shaped((slots, 2 * ROWS, 128), BF16),
        ),
        [SMEM, SMEM] + [VMEM] * 10,
        [
            pltpu.VMEM((5 * LOCAL, 24, 128), F32),
            pltpu.VMEM((480, 128), F32),
            pltpu.VMEM((6, 32, 128), F32),
            pltpu.VMEM((3, 320, 128), F32),
            pltpu.VMEM((6, 64, 128), F32),
            pltpu.VMEM((8, 64, 128), F32),
            pltpu.VMEM((6, 64, 128), F32),
            pltpu.VMEM((4, 128, 128), F32),
            pltpu.VMEM((8, 128, 128), F32),
            pltpu.VMEM((6, 128, 128), F32),
            pltpu.VMEM((12, 144, 128), F32),
        ],
    )(me, meta, *map(near, (lift, *blocks, pairs, low, own, high)))


def read_kernel(dest_ref, pay_ref, pos_ref, out_ref, stage_ref, count_ref):
    slots = pay_ref.shape[0]

    def widen(t, carry):
        count_ref[t] = 0
        stage_ref[t] = pay_ref[t].astype(F32)
        return carry

    lax.fori_loop(0, slots, widen, 0, unroll=4)
    lane = iota((8, 128), 1)

    group = together(pos_ref.shape[1], 8)

    def one(block, target, order):
        weight_x, weight_y, weight_z = box_weights(pos_ref, block)
        lower, upper = [], []
        for c in range(3):
            row = pl.multiple_of(order * ROWS + 8 * c, 8)
            packed = stage_ref[target, pl.ds(row, 8), :]
            swapped = pltpu.roll(packed, 64, 1)
            lower.append(jnp.where(lane < 64, packed, swapped))
            upper.append(jnp.where(lane < 64, swapped, packed))
        left = jnp.concatenate(
            [half for pair in zip(lower, upper) for half in pair], axis=0
        ).astype(BF16)
        right = jnp.concatenate(by_levels(weight_y, weight_z), axis=0)
        spread = lax.dot_general(
            left, right, (((1,), (0,)), ((), ())), preferred_element_type=F32
        )
        for c in range(3):
            value = spread[BOX * c : BOX * c + BOX] * weight_x
            out_ref[c, pl.ds(block, 1), :] = jnp.sum(value, axis=0, keepdims=True)

    def several(step, carry):
        places = []
        for n in range(group):
            target = dest_ref[0, step * group + n]
            order = count_ref[target]
            count_ref[target] = order + 1
            places.append((target, order))
        for n in range(group):
            one(step * group + n, *places[n])
        return carry

    lax.fori_loop(0, pos_ref.shape[1] // group, several, 0)


def read(dest, payload, positions):
    slots = payload.shape[0]
    return call(
        read_kernel,
        shaped(positions.shape, F32, False),
        [SMEM, VMEM, VMEM],
        [pltpu.VMEM((slots, 2 * ROWS, 128), F32), pltpu.SMEM((slots,), jnp.int32)],
    )(far(dest), near(payload), far(positions))


def moved(value, step):
    size = lax.axis_size(AX)
    return lax.ppermute(value, AX, [(i, (i + step) % size) for i in range(size)])


def exchanged(value, axes=AX):
    return lax.all_to_all(value, axes, split_axis=0, concat_axis=0, tiled=True)


def shards(marker_positions, marker_forces, dest_slab, base_cells, fluid_source):
    slots = lax.axis_size(AX)
    positions = marker_positions.transpose(1, 0, 2)
    forces = marker_forces.transpose(1, 0, 2)
    dest = dest_slab.T
    me = lax.axis_index(AX).astype(jnp.int32).reshape(1)
    payload = exchanged(build(dest, base_cells.T, positions, forces, fluid_source, slots))
    heads = payload[:, 0 : ROWS + 1 : ROWS, 0 : BOX + 1 : BOX]
    meta = heads.astype(jnp.int32).reshape(4 * slots)
    source, up, down, up2, down2, lift = place(meta, payload, fluid_source)
    m1, p1 = moved(up, 1), moved(down, -1)
    m2, p2 = moved(up2, 2), moved(down2, -2)
    pairs, share, rise, sink = middle_down(source, up, down, m1, p1, m2, p2)
    middle = exchanged(share, AX[1])
    middle, rise, sink = lax.optimization_barrier((middle, rise, sink))
    low, high = moved(rise, 1), moved(sink, -1)
    blocks = [middle if n == 0 else moved(middle, -LOCAL * n) for n in range(-2, 3)]
    velocity, picked = way_up(me, meta, lift, blocks, pairs, low, source, high, slots)
    out = read(dest, exchanged(picked), positions)
    return velocity, out.transpose(1, 0, 2)


def solution(mesh):
    torus = Mesh(mesh.devices.reshape(-1, LOCAL), AX)
    return jax.shard_map(
        shards,
        mesh=torus,
        in_specs=(P(AX), P(AX), P(AX), P(AX), P(AX)),
        out_specs=(P(AX), P(AX)),
        check_vma=False,
    )
```

```python
import math

import jax
import jax.numpy as jnp
from jax import lax
from jax.experimental import pallas as pl
from jax.experimental.pallas import tpu as pltpu
from jax.sharding import Mesh
from jax.sharding import PartitionSpec as P

AX = ("hi", "lo")
LOCAL = 8
BOX = 16
CZ = 4
HALF = CZ * BOX
ROWS = 3 * BOX
SCREEN = 1.0 / 64.0
RELAX = 2.0 / 3.0
INTERPRET = False
F32 = jnp.float32
BF16 = jnp.bfloat16
HIGH = lax.Precision.HIGHEST


def level(index):
    q = 0.25**index
    return q, SCREEN + 6.0 * q, RELAX / (SCREEN + 6.0 * q)


def call(body, out_shape, in_specs=None, scratch=(), name=None, megabytes=24):
    options = {} if in_specs is None else {"in_specs": in_specs}
    return pl.pallas_call(
        body,
        out_shape=out_shape,
        scratch_shapes=list(scratch),
        name=name,
        interpret=INTERPRET,
        compiler_params=pltpu.CompilerParams(vmem_limit_bytes=megabytes << 20),
        **options,
    )


def shaped(shape, dtype, near=True):
    if near and not INTERPRET:
        return pltpu.VMEM(shape, dtype)
    return jax.ShapeDtypeStruct(shape, dtype)


def near(value):
    return value if INTERPRET else pltpu.with_memory_space_constraint(value, pltpu.VMEM)


VMEM = pl.BlockSpec(memory_space=pltpu.VMEM)
SMEM = pl.BlockSpec(memory_space=pltpu.SMEM)


def far(value):
    return value if INTERPRET else pltpu.with_memory_space_constraint(value, pltpu.HBM)


def iota(shape, dim):
    return lax.broadcasted_iota(jnp.int32, shape, dim)


COS = (
    0.13884009367929634,
    0.008677498753340366,
    0.0001925760632832398,
    2.2059131886721028e-06,
    1.644977822379996e-08,
)


def phi(offset):
    inside = jnp.maximum(4.0 - offset * offset, 0.0)
    value = inside * COS[-1] + COS[-2]
    for coefficient in COS[-3::-1]:
        value = value * inside + coefficient
    value = value * inside
    return value * value


def split(value):
    high = value.astype(BF16)
    return high, (value - high.astype(F32)).astype(BF16)


def box_weights(pos_ref, block):
    cells = iota((BOX, 256), 0).astype(F32)
    levels = iota((8, 256), 0).astype(F32)
    row = pl.ds(block, 1)
    along_x = 2.0 + (BOX - 5) * pos_ref[0, row, :]
    along_y = 2.0 + (BOX - 5) * pos_ref[1, row, :]
    height = (CZ - 1) * pos_ref[2, row, :]
    return phi(along_x - cells), phi(along_y - cells), phi(height - levels)


def by_levels(weight_y, weight_z):
    return split(jnp.concatenate([weight_z[k : k + 1] * weight_y for k in range(CZ)], axis=0))


PIECES = (2 * BOX, 3 * BOX, 3 * BOX - 1)


def together(count, most):
    return math.gcd(count, most)


def build_kernel(
    dest_ref, base_ref, pos_ref, frc_ref, fluid_ref, out_ref, stage_ref, count_ref
):
    slots = out_ref.shape[0]
    blocks = pos_ref.shape[1]
    group = together(blocks, 16)

    def clear(t, carry):
        count_ref[t] = 0
        stage_ref[t, 0:8, :] = jnp.zeros((8, 128), F32)
        return carry

    lax.fori_loop(0, slots, clear, 0, unroll=4)
    lane = iota((8, 128), 1)
    top = iota((8, 128), 0) == 0

    def one(block):
        weight_x, weight_y, weight_z = box_weights(pos_ref, block)
        loaded = [frc_ref[c, pl.ds(block, 1), :] * weight_x for c in range(3)]
        high, low = split(jnp.concatenate(loaded, axis=0))
        right = jnp.concatenate(by_levels(weight_y, weight_z), axis=0)
        dims = (((1,), (1,)), ((), ()))
        box = lax.dot_general(high, right, dims, preferred_element_type=F32)
        box = box + lax.dot_general(low, right, dims, preferred_element_type=F32)
        box = box + pltpu.roll(box, HALF, 1)
        base_x = base_ref[0, block].astype(F32) + 1.0
        base_y = base_ref[1, block].astype(F32)
        tiles = [box[8 * n : 8 * n + 8] for n in range(6)]
        rounded = [tile.astype(BF16).astype(F32) for tile in tiles]
        sums = [rounded[2 * c] + rounded[2 * c + 1] for c in range(3)]
        tiles[0] = jnp.where(top & (lane % HALF == 0), base_x, tiles[0])
        tiles[0] = jnp.where(top & (lane % HALF == BOX), base_y, tiles[0])
        return tiles, sums

    def several(step, carry):
        results = []
        for n in range(group):
            tiles, sums = one(step * group + n)
            results.append(tiles)
            carry = tuple(a + b for a, b in zip(carry, sums))
        for n in range(group):
            target = dest_ref[0, step * group + n]
            order = count_ref[target]
            count_ref[target] = order + 1
            mine = lane // HALF == order
            for m in range(6):
                rows = slice(8 * m, 8 * m + 8)
                stage_ref[target, rows, :] = jnp.where(
                    mine, results[n][m], stage_ref[target, rows, :]
                )
        return carry

    fluid = []
    for c in range(3):
        column = fluid_ref[0, c] + fluid_ref[1, c] + (fluid_ref[2, c] + fluid_ref[3, c])
        fluid.append(jnp.sum(column.reshape(16, 8, 128), axis=0))
    zero = jnp.zeros((8, 128), F32)
    boxes = lax.fori_loop(0, blocks // group, several, (zero, zero, zero))
    fluid = [a + 0.5 * b for a, b in zip(fluid, boxes)]
    pieces = []
    for c in range(3):
        rest = jnp.broadcast_to(jnp.sum(fluid[c], axis=(0, 1), keepdims=True), (8, 128))
        marked = jnp.zeros((8, 128), F32)
        for place_of in PIECES:
            part = rest.astype(BF16).astype(F32)
            marked = jnp.where(lane == place_of, part, marked)
            rest = rest - part
        pieces.append(marked)
    held = top & ((lane == PIECES[0]) | (lane == PIECES[1]) | (lane == PIECES[2]))

    def finish(t, carry):
        tiles = []
        for c in range(3):
            row = BOX * c
            tiles.append(jnp.where(held, pieces[c], stage_ref[t, row : row + 8, :]))
            tiles.append(stage_ref[t, row + 8 : row + BOX, :])
        out_ref[t] = jnp.concatenate(tiles, axis=0).astype(BF16)
        return carry

    lax.fori_loop(0, slots, finish, 0, unroll=4)


def build(dest, base, positions, forces, fluid, slots):
    return call(
        build_kernel,
        shaped((slots, ROWS, 128), BF16),
        [SMEM, SMEM, VMEM, VMEM, VMEM],
        [pltpu.VMEM((slots, ROWS, 128), F32), pltpu.SMEM((slots,), jnp.int32)],
        "build",
    )(*map(far, (dest, base, positions, forces, fluid)))


def flat_ring(x):
    rows = x.shape[-2]
    ax = x.ndim - 2
    return (
        pltpu.roll(x, 1, ax)
        + pltpu.roll(x, rows - 1, ax)
        + (pltpu.roll(x, 1, ax + 1) + pltpu.roll(x, 127, ax + 1))
    )


def group_ring(x):
    rows = x.shape[-2]
    ax = x.ndim - 2
    lane = iota(x.shape, ax + 1) & 31
    before = jnp.where(lane == 0, pltpu.roll(x, 97, ax + 1), pltpu.roll(x, 1, ax + 1))
    after = jnp.where(lane == 31, pltpu.roll(x, 31, ax + 1), pltpu.roll(x, 127, ax + 1))
    return pltpu.roll(x, 1, ax) + pltpu.roll(x, rows - 1, ax) + (before + after)


def start_of(b, below, above, ring, index):
    q, _, w = level(index)
    return w * ((4.0 / 3.0) * b + (w * q) * (ring(b) + (below + above)))


def left_of(b, u, below, above, ring, index):
    q, diag, _ = level(index)
    return b - diag * u + q * (ring(u) + (below + above))


def sweep_of(b, u, below, above, ring, index):
    q, _, w = level(index)
    return (1.0 - RELAX) * u + (w * b + (w * q) * (ring(u) + (below + above)))


def dot(left, right):
    return lax.dot_general(
        left, right, (((1,), (0,)), ((), ())), precision=HIGH, preferred_element_type=F32
    )


def lanes(test):
    return test(iota((128, 128), 0), iota((128, 128), 1))


def place_kernel(
    meta_ref, pay_ref, fluid_ref,
    src_ref, up_ref, down_ref, up2_ref, down2_ref, lift_ref,
    grid_ref, u_ref, sum_ref,
):
    slots = pay_ref.shape[0]
    lane = iota((8, 128), 1)
    sub = iota((8, 128), 0)
    for z in range(CZ):
        for c in range(3):
            grid_ref[3 * z + c, 0:128, :] = fluid_ref[z, c]
            grid_ref[3 * z + c, 128:144, :] = jnp.zeros((16, 128), F32)

    def turned(tile, order, head, base_y):
        base_x = jnp.maximum(head - 1, 0)
        shift = base_x & 7
        row = pl.multiple_of(base_x - shift, 8)
        window = (lane - base_y) & 127
        inside = (window >= 1) & (window <= BOX - 2) & (head > 0)
        late = inside & (sub >= shift)
        early = inside & (sub < shift)
        pieces = [pltpu.roll(tile[8 * n : 8 * n + 8], shift, 0) for n in range(6)]
        values = []
        for k in range(CZ):
            step = (base_y - HALF * order - BOX * k) & 127
            values.append([pltpu.roll(piece, step, 1) for piece in pieces])
        return row, late, early, values

    def add(row, late, early, values):
        for k in range(CZ):
            for c in range(3):
                first, second = values[k][2 * c], values[k][2 * c + 1]
                kc = 3 * k + c
                grid_ref[kc, pl.ds(row, 8), :] += jnp.where(late, first, 0.0)
                grid_ref[kc, pl.ds(row + 8, 8), :] += jnp.where(
                    early, first, jnp.where(late, second, 0.0)
                )
                grid_ref[kc, pl.ds(row + 16, 8), :] += jnp.where(early, second, 0.0)

    group = together(slots, 8)

    def several(step, carry):
        found = []
        for n in range(group):
            d = step * group + n
            tile = pay_ref[d].astype(F32)
            carry = tuple(
                carry[c] + jnp.where(held, tile[BOX * c : BOX * c + 8], 0.0) for c in range(3)
            )
            for order in range(2):
                at = 8 * d + 4 * order
                found.append(turned(tile, order, meta_ref[at], meta_ref[at + 1]))
        for one in found:
            add(*one)
        return carry

    held = (sub == 0) & ((lane == PIECES[0]) | (lane == PIECES[1]) | (lane == PIECES[2]))
    zero = jnp.zeros((8, 128), F32)
    totals = lax.fori_loop(0, slots // group, several, (zero, zero, zero))
    factor = (1.0 - level(3)[2] * SCREEN) ** 6 / SCREEN
    for index in range(3):
        factor = factor * (1.0 - level(index)[2] * SCREEN) ** 2
    scale = factor / (slots * CZ * 128.0 * 128.0)
    lift_ref[...] = zero
    for c in range(3):
        total = jnp.sum(totals[c], axis=(0, 1), keepdims=True)
        lift_ref[c : c + 1, :] = jnp.broadcast_to(total * scale, (1, 128))
    pool = [
        jnp.where(lanes(lambda r, l: (r // 2 == (l & 63)) & (l // 64 == half)), 0.125, 0.0)
        for half in range(2)
    ]
    q, diag, w = level(0)
    spill_up, spill_down = [], []
    for c in range(3):
        for z in range(CZ):
            kc = 3 * z + c
            grid_ref[kc, 0:16, :] += grid_ref[kc, 128:144, :]
            src_ref[z, c] = grid_ref[kc, 0:128, :]

        def b_at(z):
            return src_ref[z, c] if 0 <= z < CZ else 0.0

        for z in range(CZ):
            u_ref[z + 1] = start_of(src_ref[z, c], b_at(z - 1), b_at(z + 1), flat_ring, 0)
        u_ref[0] = (w * w * q) * src_ref[0, c]
        u_ref[CZ + 1] = (w * w * q) * src_ref[CZ - 1, c]

        def left(z):
            if z == -2:
                return q * u_ref[0]
            if z == CZ + 1:
                return q * u_ref[CZ + 1]
            below = u_ref[z] if z > -1 else 0.0
            above = u_ref[z + 2] if z < CZ else 0.0
            return left_of(b_at(z), u_ref[z + 1], below, above, flat_ring, 0)

        rows = []
        for pair in range(-1, 3):
            sum_ref[...] = left(2 * pair) + left(2 * pair + 1)
            rows.append(sum_ref[pl.ds(0, 64, 2), :] + sum_ref[pl.ds(1, 64, 2), :])
        own = dot(rows[1], pool[0]) + dot(rows[2], pool[1])
        up_ref[c] = own
        down_ref[c] = own
        spill_down.append(dot(rows[0], pool[c % 2]))
        spill_up.append(dot(rows[3], pool[c % 2]))
    for ref, far_ref, spill in ((up_ref, up2_ref, spill_up), (down_ref, down2_ref, spill_down)):
        both = spill[0] + spill[1]
        ref[3] = both
        ref[4] = spill[2]
        far_ref[0] = both
        far_ref[1] = spill[2]


def place(meta, payload, fluid):
    return call(
        place_kernel,
        (
            shaped(fluid.shape, F32),
            shaped((5, 64, 128), F32),
            shaped((5, 64, 128), F32),
            shaped((2, 64, 128), F32),
            shaped((2, 64, 128), F32),
            shaped((8, 128), F32),
        ),
        [SMEM, VMEM, VMEM],
        [
            pltpu.VMEM((12, 144, 128), F32),
            pltpu.VMEM((CZ + 2, 128, 128), F32),
            pltpu.VMEM((128, 128), F32),
        ],
        "place",
    )(meta, near(payload), near(fluid))


def both_layers(tile):
    lane = iota(tile.shape, tile.ndim - 1)
    turned = pltpu.roll(tile, 64, tile.ndim - 1)
    return jnp.where(lane < 64, tile, turned), jnp.where(lane < 64, turned, tile)


def pack_coarse(value):
    last = value[24:32]
    lane = iota((8, 128), 1)
    return [
        jnp.where(lane < 96, value[8 * c : 8 * c + 8], pltpu.roll(last, 96 - 32 * c, 1))
        for c in range(3)
    ]


def unpack_coarse(tile):
    lane = iota((8, 128), 1)
    last = jnp.zeros((8, 128), F32)
    rows = []
    for c in range(3):
        piece = tile[8 * c : 8 * c + 8]
        turned = pltpu.roll(piece, (32 * c - 96) % 128, 1)
        last = jnp.where(lane // 32 == c, turned, last)
        rows.append(jnp.where(lane < 96, piece, 0.0))
    return jnp.concatenate(rows + [last], axis=0)


def spilled(ref, c, first=0):
    return both_layers(ref[first + c // 2])[c % 2]


U_ROW = 9 * 128


def middle_kernel(
    src_ref, up_ref, down_ref, m1_ref, p1_ref, m2_ref, p2_ref,
    pairs_ref, out_ref, rise_ref, sink_ref, sum_ref,
):
    total = None
    for z in range(3):
        for c in range(3):
            rows = slice(128 * (3 * z + c), 128 * (3 * z + c + 1))
            rise_ref[rows, :] = src_ref[z + 1, c]
            sink_ref[rows, :] = src_ref[z, c]
    lane = iota((64, 128), 1)
    for c in range(3):
        m1, own, p1 = both_layers(m1_ref[c]), both_layers(up_ref[c]), both_layers(p1_ref[c])
        b = [
            m1[0] + spilled(m2_ref, c),
            m1[1] + spilled(down_ref, c, 3),
            own[0] + spilled(m1_ref, c, 3),
            own[1] + spilled(p1_ref, c, 3),
            p1[0] + spilled(up_ref, c, 3),
            p1[1] + spilled(p2_ref, c),
        ]
        for j in range(3):
            pairs_ref[j, c] = jnp.where(lane < 64, b[2 * j], b[2 * j + 1])
        u = [start_of(b[i], b[i - 1], b[i + 1], flat_ring, 1) for i in range(1, 5)]
        rows = slice(U_ROW + 64 * c, U_ROW + 64 * c + 64)
        rise_ref[rows, :] = jnp.where(lane < 64, u[0], u[1])
        sink_ref[rows, :] = jnp.where(lane < 64, u[2], u[3])
        left = [left_of(b[i + 1], u[i], u[i - 1], u[i + 1], flat_ring, 1) for i in (1, 2)]
        sum_ref[...] = left[0] + left[1]
        rows = sum_ref[pl.ds(0, 32, 2), :] + sum_ref[pl.ds(1, 32, 2), :]
        pool = jnp.where(
            lanes(lambda r, l: (r // 2 == (l & 31)) & (l // 32 == c) & (r < 64)), 0.125, 0.0
        )
        part = dot(rows, pool)
        total = part if total is None else total + part
    packed = jnp.concatenate(pack_coarse(total), axis=0)
    for d in range(out_ref.shape[0]):
        out_ref[d] = packed


def middle_down(source, up, down, m1, p1, m2, p2):
    return call(
        middle_kernel,
        (
            shaped((3, 3, 64, 128), F32),
            shaped((LOCAL, 24, 128), F32),
            shaped((U_ROW + 192, 128), F32),
            shaped((U_ROW + 192, 128), F32),
        ),
        None,
        [pltpu.VMEM((64, 128), F32)],
        "middle_down",
    )(*map(near, (source, up, down, m1, p1, m2, p2)))


def inner(x):
    return x[1:-1]


def coarse_part(me, blocks, lift_ref, window_ref, pool_ref, final_ref):
    parity = me % 2
    first = me % LOCAL - parity
    for n, ref in enumerate(blocks):
        window_ref[LOCAL * n : LOCAL * n + LOCAL] = ref[...]
    b2 = jnp.stack([unpack_coarse(window_ref[first + t]) for t in range(34)])
    group = iota((1, 128), 1) // 32
    lift = jnp.zeros((1, 128), F32)
    for c in range(3):
        lift = jnp.where(group == c, lift_ref[c : c + 1, :], lift)
    _, _, w3 = level(3)
    u2 = start_of(inner(b2), b2[:-2], b2[2:], group_ring, 2)
    r2 = left_of(b2[2:-2], inner(u2), u2[:-2], u2[2:], group_ring, 2)
    pairs = r2.reshape(15, 2, 32, 128)
    pool_ref[...] = (pairs[:, 0] + pairs[:, 1]).reshape(480, 128)
    rows = pool_ref[pl.ds(0, 240, 2), :] + pool_ref[pl.ds(1, 240, 2), :]
    pool = jnp.where(
        lanes(lambda r, l: ((r & 31) // 2 == (l & 15)) & (r // 32 == l // 32)), 0.125, 0.0
    )
    b3 = dot(rows, pool).reshape(15, 16, 128)
    u3 = w3 * b3
    for _ in range(5):
        b3 = inner(b3)
        u3 = sweep_of(b3, inner(u3), u3[:-2], u3[2:], group_ring, 3)
    u3 = (u3 + lift[None]).reshape(80, 128)
    spread = jnp.where(
        lanes(lambda r, l: ((l & 31) // 2 == (r & 31)) & (r // 32 == l // 32)), 1.0, 0.0
    )
    wide = dot(u3, spread)
    pool_ref[pl.ds(0, 80, 2), :] = wide
    pool_ref[pl.ds(1, 80, 2), :] = wide
    lifted = pool_ref[0:160, :].reshape(5, 1, 32, 128)
    u = (u2[11:21].reshape(5, 2, 32, 128) + lifted).reshape(10, 32, 128)
    u = sweep_of(b2[13:21], inner(u), u[:-2], u[2:], group_ring, 2)
    u = sweep_of(b2[14:20], inner(u), u[:-2], u[2:], group_ring, 2)
    final_ref[...] = u
    return jnp.concatenate([final_ref[parity + h] for h in range(5)], axis=0)


def up_kernel(
    me_ref, meta_ref, lift_ref, g0_ref, g1_ref, g2_ref, g3_ref, g4_ref,
    pairs_ref, low_ref, own_ref, high_ref, vel_ref, pay_ref,
    window_ref, pool_ref, final_ref, lift1_ref, b1_ref, u1_ref, v1_ref, lift0_ref, u0_ref,
    v0_ref, ext_ref,
):
    blocks = (g0_ref, g1_ref, g2_ref, g3_ref, g4_ref)
    coarse = coarse_part(me_ref[0], blocks, lift_ref, window_ref, pool_ref, final_ref)
    for c in range(3):
        spread = jnp.where(lanes(lambda r, l: r == 32 * c + (l & 63) // 2), 1.0, 0.0)
        wide = dot(coarse, spread)
        lift1_ref[c, pl.ds(0, 160, 2), :] = wide
        lift1_ref[c, pl.ds(1, 160, 2), :] = wide
    spread0 = jnp.where(lanes(lambda r, l: r == l // 2), 1.0, 0.0)

    def b_at(z, c):
        if 0 <= z < CZ:
            return own_ref[z, c]
        ref, first = (low_ref, z + 3) if z < 0 else (high_ref, z - CZ)
        return ref[pl.ds(pl.multiple_of(128 * (3 * first + c), 128), 128), :]

    def component(c, carry):
        for j in range(3):
            b1_ref[2 * j], b1_ref[2 * j + 1] = both_layers(pairs_ref[j, c])
        rows = pl.ds(pl.multiple_of(U_ROW + 64 * c, 64), 64)
        u1 = list(both_layers(low_ref[rows, :]))
        for i in range(1, 5):
            u1.append(start_of(b1_ref[i], b1_ref[i - 1], b1_ref[i + 1], flat_ring, 1))
        u1.extend(both_layers(high_ref[rows, :]))
        for z in range(-3, 5):
            h = z // 2 + 2
            u1_ref[z + 3] = u1[z + 3] + lift1_ref[c, 64 * h : 64 * h + 64, :]
        for z in range(-2, 4):
            i = z + 3
            v1_ref[z + 2] = sweep_of(
                b1_ref[z + 2], u1_ref[i], u1_ref[i - 1], u1_ref[i + 1], flat_ring, 1
            )
        for z in range(-1, 3):
            i = z + 2
            value = sweep_of(
                b1_ref[z + 2], v1_ref[i], v1_ref[i - 1], v1_ref[i + 1], flat_ring, 1
            )
            wide = dot(value, spread0)
            lift0_ref[z + 1, pl.ds(0, 64, 2), :] = wide
            lift0_ref[z + 1, pl.ds(1, 64, 2), :] = wide
        for z in range(-2, 6):
            u0_ref[z + 2] = (
                start_of(b_at(z, c), b_at(z - 1, c), b_at(z + 1, c), flat_ring, 0)
                + lift0_ref[z // 2 + 1]
            )
        for z in range(-1, 5):
            i = z + 2
            v0_ref[z + 1] = sweep_of(
                b_at(z, c), u0_ref[i], u0_ref[i - 1], u0_ref[i + 1], flat_ring, 0
            )
        for z in range(CZ):
            i = z + 1
            value = sweep_of(
                own_ref[z, c], v0_ref[i], v0_ref[i - 1], v0_ref[i + 1], flat_ring, 0
            )
            vel_ref[z, c] = value
            rounded = value.astype(BF16).astype(F32)
            ext_ref[3 * z + c, 0:128, :] = rounded
            ext_ref[3 * z + c, 128:144, :] = rounded[0:16]
        return carry

    lax.fori_loop(0, 3, component, 0)
    lane = iota((8, 128), 1)
    sub = iota((8, 128), 0)

    part = [(lane // BOX) % CZ == k for k in range(CZ)]

    def gather(order, head, base_y):
        base_x = jnp.maximum(head - 1, 0)
        shift = base_x & 7
        row = pl.multiple_of(base_x - shift, 8)
        late = sub >= shift
        values = []
        for k in range(CZ):
            step = (HALF * order + BOX * k - base_y) & 127
            line = []
            for c in range(3):
                tiles = [ext_ref[3 * k + c, pl.ds(row + 8 * n, 8), :] for n in range(3)]
                for n in range(2):
                    value = jnp.where(late, tiles[n], tiles[n + 1])
                    line.append(pltpu.roll(value, step, 1))
            values.append(line)
        return (8 - shift) & 7, values

    group = together(pay_ref.shape[0], 8)

    def several(step, carry):
        found = []
        for n in range(group):
            for order in range(2):
                at = 8 * (step * group + n) + 4 * order
                found.append(gather(order, meta_ref[at], meta_ref[at + 1]))
        for n in range(group):
            pieces = []
            for m in range(6):
                both = []
                for order in range(2):
                    back, values = found[2 * n + order]
                    packed = values[0][m]
                    for k in range(1, CZ):
                        packed = jnp.where(part[k], values[k][m], packed)
                    both.append(pltpu.roll(packed, back, 0))
                pieces.append(jnp.where(lane < HALF, both[0], both[1]))
            pay_ref[step * group + n] = jnp.concatenate(pieces, axis=0).astype(BF16)
        return carry

    lax.fori_loop(0, pay_ref.shape[0] // group, several, 0)


def way_up(me, meta, lift, blocks, pairs, low, own, high, slots):
    return call(
        up_kernel,
        (
            shaped(own.shape, F32, False),
            shaped((slots, ROWS, 128), BF16),
        ),
        [SMEM, SMEM] + [VMEM] * 10,
        [
            pltpu.VMEM((5 * LOCAL, 24, 128), F32),
            pltpu.VMEM((480, 128), F32),
            pltpu.VMEM((6, 32, 128), F32),
            pltpu.VMEM((3, 320, 128), F32),
            pltpu.VMEM((6, 64, 128), F32),
            pltpu.VMEM((8, 64, 128), F32),
            pltpu.VMEM((6, 64, 128), F32),
            pltpu.VMEM((4, 128, 128), F32),
            pltpu.VMEM((8, 128, 128), F32),
            pltpu.VMEM((6, 128, 128), F32),
            pltpu.VMEM((12, 144, 128), F32),
        ],
        "way_up",
    )(me, meta, *map(near, (lift, *blocks, pairs, low, own, high)))


def read_kernel(dest_ref, pay_ref, pos_ref, out_ref, stage_ref, count_ref):
    slots = pay_ref.shape[0]

    def widen(t, carry):
        count_ref[t] = 0
        stage_ref[t] = pay_ref[t].astype(F32)
        return carry

    lax.fori_loop(0, slots, widen, 0, unroll=4)
    lane = iota((8, 128), 1)

    group = together(pos_ref.shape[1], 16)

    def one(block, target, order):
        weight_x, weight_y, weight_z = box_weights(pos_ref, block)
        mine = lane // HALF == order
        left = []
        for n in range(6):
            packed = stage_ref[target, 8 * n : 8 * n + 8, :]
            left.append(jnp.where(mine, packed, pltpu.roll(packed, HALF, 1)))
        left = jnp.concatenate(left, axis=0).astype(BF16)
        right = jnp.concatenate(by_levels(weight_y, weight_z), axis=0)
        spread = lax.dot_general(
            left, right, (((1,), (0,)), ((), ())), preferred_element_type=F32
        )
        for c in range(3):
            value = spread[BOX * c : BOX * c + BOX] * weight_x
            out_ref[c, pl.ds(block, 1), :] = jnp.sum(value, axis=0, keepdims=True)

    def several(step, carry):
        places = []
        for n in range(group):
            target = dest_ref[0, step * group + n]
            order = count_ref[target]
            count_ref[target] = order + 1
            places.append((target, order))
        for n in range(group):
            one(step * group + n, *places[n])
        return carry

    lax.fori_loop(0, pos_ref.shape[1] // group, several, 0)


def read(dest, payload, positions):
    slots = payload.shape[0]
    return call(
        read_kernel,
        shaped(positions.shape, F32, False),
        [SMEM, VMEM, VMEM],
        [pltpu.VMEM((slots, ROWS, 128), F32), pltpu.SMEM((slots,), jnp.int32)],
        "read",
    )(far(dest), near(payload), near(positions))


def moved(value, step):
    size = lax.axis_size(AX)
    return lax.ppermute(value, AX, [(i, (i + step) % size) for i in range(size)])


def exchanged(value, axes=AX):
    return lax.all_to_all(value, axes, split_axis=0, concat_axis=0, tiled=True)


def shards(marker_positions, marker_forces, dest_slab, base_cells, fluid_source):
    slots = lax.axis_size(AX)
    positions = marker_positions.transpose(1, 0, 2)
    forces = marker_forces.transpose(1, 0, 2)
    dest = dest_slab.T
    me = lax.axis_index(AX).astype(jnp.int32).reshape(1)
    payload = exchanged(build(dest, base_cells.T, positions, forces, fluid_source, slots))
    meta = payload[:, 0:1, ::BOX].astype(jnp.int32).reshape(8 * slots)
    source, up, down, up2, down2, lift = place(meta, payload, fluid_source)
    m1, p1 = moved(up, 1), moved(down, -1)
    m2, p2 = moved(up2, 2), moved(down2, -2)
    pairs, share, rise, sink = middle_down(source, up, down, m1, p1, m2, p2)
    middle = exchanged(share, AX[1])
    low, high = moved(rise, 1), moved(sink, -1)
    blocks = [middle if n == 0 else moved(middle, -LOCAL * n) for n in range(-2, 3)]
    velocity, picked = way_up(me, meta, lift, blocks, pairs, low, source, high, slots)
    out = read(dest, exchanged(picked), positions)
    return velocity, out.transpose(1, 0, 2)


def solution(mesh):
    torus = Mesh(mesh.devices.reshape(-1, LOCAL), AX)
    return jax.shard_map(
        shards,
        mesh=torus,
        in_specs=(P(AX), P(AX), P(AX), P(AX), P(AX)),
        out_specs=(P(AX), P(AX)),
        check_vma=False,
    )
```

```python
import math

import jax
import jax.numpy as jnp
from jax import lax
from jax.experimental import pallas as pl
from jax.experimental.pallas import tpu as pltpu
from jax.sharding import Mesh
from jax.sharding import PartitionSpec as P

AX = ("hi", "lo")
LOCAL = 8
BOX = 16
CZ = 4
HALF = CZ * BOX
ROWS = 3 * BOX
SCREEN = 1.0 / 64.0
RELAX = 2.0 / 3.0
INTERPRET = False
F32 = jnp.float32
BF16 = jnp.bfloat16
HIGH = lax.Precision.HIGHEST


def level(index):
    q = 0.25**index
    return q, SCREEN + 6.0 * q, RELAX / (SCREEN + 6.0 * q)


def call(body, out_shape, in_specs=None, scratch=(), megabytes=24):
    options = {} if in_specs is None else {"in_specs": in_specs}
    return pl.pallas_call(
        body,
        out_shape=out_shape,
        scratch_shapes=list(scratch),
        interpret=INTERPRET,
        compiler_params=pltpu.CompilerParams(vmem_limit_bytes=megabytes << 20),
        **options,
    )


def shaped(shape, dtype, near=True):
    if near and not INTERPRET:
        return pltpu.VMEM(shape, dtype)
    return jax.ShapeDtypeStruct(shape, dtype)


def near(value):
    return value if INTERPRET else pltpu.with_memory_space_constraint(value, pltpu.VMEM)


VMEM = pl.BlockSpec(memory_space=pltpu.VMEM)
SMEM = pl.BlockSpec(memory_space=pltpu.SMEM)


def far(value):
    return value if INTERPRET else pltpu.with_memory_space_constraint(value, pltpu.HBM)


def iota(shape, dim):
    return lax.broadcasted_iota(jnp.int32, shape, dim)


COS = (
    0.13884009367929634,
    0.008677498753340366,
    0.0001925760632832398,
    2.2059131886721028e-06,
    1.644977822379996e-08,
)


def phi(offset):
    inside = jnp.maximum(4.0 - offset * offset, 0.0)
    value = inside * COS[-1] + COS[-2]
    for coefficient in COS[-3::-1]:
        value = value * inside + coefficient
    value = value * inside
    return value * value


def split(value):
    high = value.astype(BF16)
    return high, (value - high.astype(F32)).astype(BF16)


def box_weights(pos_ref, block):
    cells = iota((BOX, 256), 0).astype(F32)
    levels = iota((8, 256), 0).astype(F32)
    row = pl.ds(block, 1)
    along_x = 2.0 + (BOX - 5) * pos_ref[0, row, :]
    along_y = 2.0 + (BOX - 5) * pos_ref[1, row, :]
    height = (CZ - 1) * pos_ref[2, row, :]
    return phi(along_x - cells), phi(along_y - cells), phi(height - levels)


def by_levels(weight_y, weight_z):
    return split(jnp.concatenate([weight_z[k : k + 1] * weight_y for k in range(CZ)], axis=0))


PIECES = (2 * BOX, 3 * BOX, 3 * BOX - 1)


def together(count, most):
    return math.gcd(count, most)


def build_kernel(
    dest_ref, base_ref, pos_ref, frc_ref, fluid_ref, out_ref, stage_ref, count_ref
):
    slots = out_ref.shape[0]
    blocks = pos_ref.shape[1]
    group = together(blocks, 16)

    def clear(t, carry):
        count_ref[t] = 0
        stage_ref[t, 0:8, :] = jnp.zeros((8, 128), F32)
        return carry

    lax.fori_loop(0, slots, clear, 0, unroll=4)
    lane = iota((8, 128), 1)
    top = iota((8, 128), 0) == 0

    def one(block):
        weight_x, weight_y, weight_z = box_weights(pos_ref, block)
        loaded = [frc_ref[c, pl.ds(block, 1), :] * weight_x for c in range(3)]
        high, low = split(jnp.concatenate(loaded, axis=0))
        right = jnp.concatenate(by_levels(weight_y, weight_z), axis=0)
        dims = (((1,), (1,)), ((), ()))
        box = lax.dot_general(high, right, dims, preferred_element_type=F32)
        box = box + lax.dot_general(low, right, dims, preferred_element_type=F32)
        box = box + pltpu.roll(box, HALF, 1)
        base_x = base_ref[0, block].astype(F32) + 1.0
        base_y = base_ref[1, block].astype(F32)
        tiles = [box[8 * n : 8 * n + 8] for n in range(6)]
        rounded = [tile.astype(BF16).astype(F32) for tile in tiles]
        sums = [rounded[2 * c] + rounded[2 * c + 1] for c in range(3)]
        tiles[0] = jnp.where(top & (lane % HALF == 0), base_x, tiles[0])
        tiles[0] = jnp.where(top & (lane % HALF == BOX), base_y, tiles[0])
        return tiles, sums

    def several(step, carry):
        results = []
        for n in range(group):
            tiles, sums = one(step * group + n)
            results.append(tiles)
            carry = tuple(a + b for a, b in zip(carry, sums))
        for n in range(group):
            target = dest_ref[0, step * group + n]
            order = count_ref[target]
            count_ref[target] = order + 1
            mine = lane // HALF == order
            for m in range(6):
                rows = slice(8 * m, 8 * m + 8)
                stage_ref[target, rows, :] = jnp.where(
                    mine, results[n][m], stage_ref[target, rows, :]
                )
        return carry

    fluid = []
    for c in range(3):
        column = fluid_ref[0, c] + fluid_ref[1, c] + (fluid_ref[2, c] + fluid_ref[3, c])
        fluid.append(jnp.sum(column.reshape(16, 8, 128), axis=0))
    zero = jnp.zeros((8, 128), F32)
    boxes = lax.fori_loop(0, blocks // group, several, (zero, zero, zero))
    fluid = [a + 0.5 * b for a, b in zip(fluid, boxes)]
    pieces = []
    for c in range(3):
        rest = jnp.broadcast_to(jnp.sum(fluid[c], axis=(0, 1), keepdims=True), (8, 128))
        marked = jnp.zeros((8, 128), F32)
        for place_of in PIECES:
            part = rest.astype(BF16).astype(F32)
            marked = jnp.where(lane == place_of, part, marked)
            rest = rest - part
        pieces.append(marked)
    held = top & ((lane == PIECES[0]) | (lane == PIECES[1]) | (lane == PIECES[2]))

    def finish(t, carry):
        tiles = []
        for c in range(3):
            row = BOX * c
            tiles.append(jnp.where(held, pieces[c], stage_ref[t, row : row + 8, :]))
            tiles.append(stage_ref[t, row + 8 : row + BOX, :])
        out_ref[t] = jnp.concatenate(tiles, axis=0).astype(BF16)
        return carry

    lax.fori_loop(0, slots, finish, 0, unroll=4)


def build(dest, base, positions, forces, fluid, slots):
    return call(
        build_kernel,
        shaped((slots, ROWS, 128), BF16),
        [SMEM, SMEM, VMEM, VMEM, VMEM],
        [pltpu.VMEM((slots, ROWS, 128), F32), pltpu.SMEM((slots,), jnp.int32)],
    )(*map(far, (dest, base, positions, forces, fluid)))


def flat_ring(x):
    rows = x.shape[-2]
    ax = x.ndim - 2
    return (
        pltpu.roll(x, 1, ax)
        + pltpu.roll(x, rows - 1, ax)
        + (pltpu.roll(x, 1, ax + 1) + pltpu.roll(x, 127, ax + 1))
    )


def group_ring(x):
    rows = x.shape[-2]
    ax = x.ndim - 2
    lane = iota(x.shape, ax + 1) & 31
    before = jnp.where(lane == 0, pltpu.roll(x, 97, ax + 1), pltpu.roll(x, 1, ax + 1))
    after = jnp.where(lane == 31, pltpu.roll(x, 31, ax + 1), pltpu.roll(x, 127, ax + 1))
    return pltpu.roll(x, 1, ax) + pltpu.roll(x, rows - 1, ax) + (before + after)


def start_of(b, below, above, ring, index):
    q, _, w = level(index)
    return w * ((4.0 / 3.0) * b + (w * q) * (ring(b) + (below + above)))


def left_of(b, u, below, above, ring, index):
    q, diag, _ = level(index)
    return b - diag * u + q * (ring(u) + (below + above))


def sweep_of(b, u, below, above, ring, index):
    q, _, w = level(index)
    return (1.0 - RELAX) * u + (w * b + (w * q) * (ring(u) + (below + above)))


def dot(left, right):
    return lax.dot_general(
        left, right, (((1,), (0,)), ((), ())), precision=HIGH, preferred_element_type=F32
    )


def lanes(test):
    return test(iota((128, 128), 0), iota((128, 128), 1))


def place_kernel(
    meta_ref, pay_ref, fluid_ref,
    src_ref, up_ref, down_ref, up2_ref, down2_ref, lift_ref,
    grid_ref, u_ref, sum_ref,
):
    slots = pay_ref.shape[0]
    lane = iota((8, 128), 1)
    sub = iota((8, 128), 0)
    for z in range(CZ):
        for c in range(3):
            grid_ref[3 * z + c, 0:128, :] = fluid_ref[z, c]
            grid_ref[3 * z + c, 128:144, :] = jnp.zeros((16, 128), F32)

    def turned(tile, order, head, base_y):
        base_x = jnp.maximum(head - 1, 0)
        shift = base_x & 7
        row = pl.multiple_of(base_x - shift, 8)
        window = (lane - base_y) & 127
        inside = (window >= 1) & (window <= BOX - 2) & (head > 0)
        late = inside & (sub >= shift)
        early = inside & (sub < shift)
        pieces = [pltpu.roll(tile[8 * n : 8 * n + 8], shift, 0) for n in range(6)]
        values = []
        for k in range(CZ):
            step = (base_y - HALF * order - BOX * k) & 127
            values.append([pltpu.roll(piece, step, 1) for piece in pieces])
        return row, late, early, values

    def add(row, late, early, values):
        for k in range(CZ):
            for c in range(3):
                first, second = values[k][2 * c], values[k][2 * c + 1]
                kc = 3 * k + c
                grid_ref[kc, pl.ds(row, 8), :] += jnp.where(late, first, 0.0)
                grid_ref[kc, pl.ds(row + 8, 8), :] += jnp.where(
                    early, first, jnp.where(late, second, 0.0)
                )
                grid_ref[kc, pl.ds(row + 16, 8), :] += jnp.where(early, second, 0.0)

    group = together(slots, 8)

    def several(step, carry):
        found = []
        for n in range(group):
            d = step * group + n
            tile = pay_ref[d].astype(F32)
            carry = tuple(
                carry[c] + jnp.where(held, tile[BOX * c : BOX * c + 8], 0.0) for c in range(3)
            )
            for order in range(2):
                at = 8 * d + 4 * order
                found.append(turned(tile, order, meta_ref[at], meta_ref[at + 1]))
        for one in found:
            add(*one)
        return carry

    held = (sub == 0) & ((lane == PIECES[0]) | (lane == PIECES[1]) | (lane == PIECES[2]))
    zero = jnp.zeros((8, 128), F32)
    totals = lax.fori_loop(0, slots // group, several, (zero, zero, zero))
    factor = (1.0 - level(3)[2] * SCREEN) ** 6 / SCREEN
    for index in range(3):
        factor = factor * (1.0 - level(index)[2] * SCREEN) ** 2
    scale = factor / (slots * CZ * 128.0 * 128.0)
    lift_ref[...] = zero
    for c in range(3):
        total = jnp.sum(totals[c], axis=(0, 1), keepdims=True)
        lift_ref[c : c + 1, :] = jnp.broadcast_to(total * scale, (1, 128))
    pool = [
        jnp.where(lanes(lambda r, l: (r // 2 == (l & 63)) & (l // 64 == half)), 0.125, 0.0)
        for half in range(2)
    ]
    q, _, w = level(0)
    spill_up, spill_down = [], []
    for c in range(3):
        for z in range(CZ):
            kc = 3 * z + c
            grid_ref[kc, 0:16, :] += grid_ref[kc, 128:144, :]
            src_ref[z, c] = grid_ref[kc, 0:128, :]

        def b_at(z):
            return src_ref[z, c] if 0 <= z < CZ else 0.0

        for z in range(CZ):
            u_ref[z + 1] = start_of(src_ref[z, c], b_at(z - 1), b_at(z + 1), flat_ring, 0)
        u_ref[0] = (w * w * q) * src_ref[0, c]
        u_ref[CZ + 1] = (w * w * q) * src_ref[CZ - 1, c]

        def left(z):
            if z == -2:
                return q * u_ref[0]
            if z == CZ + 1:
                return q * u_ref[CZ + 1]
            below = u_ref[z] if z > -1 else 0.0
            above = u_ref[z + 2] if z < CZ else 0.0
            return left_of(b_at(z), u_ref[z + 1], below, above, flat_ring, 0)

        rows = []
        for pair in range(-1, 3):
            sum_ref[...] = left(2 * pair) + left(2 * pair + 1)
            rows.append(sum_ref[pl.ds(0, 64, 2), :] + sum_ref[pl.ds(1, 64, 2), :])
        own = dot(rows[1], pool[0]) + dot(rows[2], pool[1])
        up_ref[c] = own
        down_ref[c] = own
        spill_down.append(dot(rows[0], pool[c % 2]))
        spill_up.append(dot(rows[3], pool[c % 2]))
    for ref, far_ref, spill in ((up_ref, up2_ref, spill_up), (down_ref, down2_ref, spill_down)):
        both = spill[0] + spill[1]
        ref[3] = both
        ref[4] = spill[2]
        far_ref[0] = both
        far_ref[1] = spill[2]


def place(meta, payload, fluid):
    return call(
        place_kernel,
        (
            shaped(fluid.shape, F32),
            shaped((5, 64, 128), F32),
            shaped((5, 64, 128), F32),
            shaped((2, 64, 128), F32),
            shaped((2, 64, 128), F32),
            shaped((8, 128), F32),
        ),
        [SMEM, VMEM, VMEM],
        [
            pltpu.VMEM((12, 144, 128), F32),
            pltpu.VMEM((CZ + 2, 128, 128), F32),
            pltpu.VMEM((128, 128), F32),
        ],
    )(meta, near(payload), near(fluid))


def both_layers(tile):
    lane = iota(tile.shape, tile.ndim - 1)
    turned = pltpu.roll(tile, 64, tile.ndim - 1)
    return jnp.where(lane < 64, tile, turned), jnp.where(lane < 64, turned, tile)


def pack_coarse(value):
    last = value[24:32]
    lane = iota((8, 128), 1)
    return [
        jnp.where(lane < 96, value[8 * c : 8 * c + 8], pltpu.roll(last, 96 - 32 * c, 1))
        for c in range(3)
    ]


def unpack_coarse(tile):
    lane = iota((8, 128), 1)
    last = jnp.zeros((8, 128), F32)
    rows = []
    for c in range(3):
        piece = tile[8 * c : 8 * c + 8]
        turned = pltpu.roll(piece, (32 * c - 96) % 128, 1)
        last = jnp.where(lane // 32 == c, turned, last)
        rows.append(jnp.where(lane < 96, piece, 0.0))
    return jnp.concatenate(rows + [last], axis=0)


def spilled(ref, c, first=0):
    return both_layers(ref[first + c // 2])[c % 2]


U_ROW = 9 * 128


def middle_kernel(
    src_ref, up_ref, down_ref, m1_ref, p1_ref, m2_ref, p2_ref,
    pairs_ref, out_ref, rise_ref, sink_ref, sum_ref,
):
    total = None
    for z in range(3):
        for c in range(3):
            rows = slice(128 * (3 * z + c), 128 * (3 * z + c + 1))
            rise_ref[rows, :] = src_ref[z + 1, c]
            sink_ref[rows, :] = src_ref[z, c]
    lane = iota((64, 128), 1)
    for c in range(3):
        m1, own, p1 = both_layers(m1_ref[c]), both_layers(up_ref[c]), both_layers(p1_ref[c])
        b = [
            m1[0] + spilled(m2_ref, c),
            m1[1] + spilled(down_ref, c, 3),
            own[0] + spilled(m1_ref, c, 3),
            own[1] + spilled(p1_ref, c, 3),
            p1[0] + spilled(up_ref, c, 3),
            p1[1] + spilled(p2_ref, c),
        ]
        for j in range(3):
            pairs_ref[j, c] = jnp.where(lane < 64, b[2 * j], b[2 * j + 1])
        u = [start_of(b[i], b[i - 1], b[i + 1], flat_ring, 1) for i in range(1, 5)]
        rows = slice(U_ROW + 64 * c, U_ROW + 64 * c + 64)
        rise_ref[rows, :] = jnp.where(lane < 64, u[0], u[1])
        sink_ref[rows, :] = jnp.where(lane < 64, u[2], u[3])
        left = [left_of(b[i + 1], u[i], u[i - 1], u[i + 1], flat_ring, 1) for i in (1, 2)]
        sum_ref[...] = left[0] + left[1]
        rows = sum_ref[pl.ds(0, 32, 2), :] + sum_ref[pl.ds(1, 32, 2), :]
        pool = jnp.where(
            lanes(lambda r, l: (r // 2 == (l & 31)) & (l // 32 == c) & (r < 64)), 0.125, 0.0
        )
        part = dot(rows, pool)
        total = part if total is None else total + part
    packed = jnp.concatenate(pack_coarse(total), axis=0)
    for d in range(out_ref.shape[0]):
        out_ref[d] = packed


def middle_down(source, up, down, m1, p1, m2, p2):
    return call(
        middle_kernel,
        (
            shaped((3, 3, 64, 128), F32),
            shaped((LOCAL, 24, 128), F32),
            shaped((U_ROW + 192, 128), F32),
            shaped((U_ROW + 192, 128), F32),
        ),
        None,
        [pltpu.VMEM((64, 128), F32)],
    )(*map(near, (source, up, down, m1, p1, m2, p2)))


def inner(x):
    return x[1:-1]


def coarse_part(me, blocks, lift_ref, window_ref, pool_ref, final_ref):
    parity = me % 2
    first = me % LOCAL - parity
    for n, ref in enumerate(blocks):
        window_ref[LOCAL * n : LOCAL * n + LOCAL] = ref[...]
    b2 = jnp.stack([unpack_coarse(window_ref[first + t]) for t in range(34)])
    group = iota((1, 128), 1) // 32
    lift = jnp.zeros((1, 128), F32)
    for c in range(3):
        lift = jnp.where(group == c, lift_ref[c : c + 1, :], lift)
    _, _, w3 = level(3)
    u2 = start_of(inner(b2), b2[:-2], b2[2:], group_ring, 2)
    r2 = left_of(b2[2:-2], inner(u2), u2[:-2], u2[2:], group_ring, 2)
    pairs = r2.reshape(15, 2, 32, 128)
    pool_ref[...] = (pairs[:, 0] + pairs[:, 1]).reshape(480, 128)
    rows = pool_ref[pl.ds(0, 240, 2), :] + pool_ref[pl.ds(1, 240, 2), :]
    pool = jnp.where(
        lanes(lambda r, l: ((r & 31) // 2 == (l & 15)) & (r // 32 == l // 32)), 0.125, 0.0
    )
    b3 = dot(rows, pool).reshape(15, 16, 128)
    u3 = w3 * b3
    for _ in range(5):
        b3 = inner(b3)
        u3 = sweep_of(b3, inner(u3), u3[:-2], u3[2:], group_ring, 3)
    u3 = (u3 + lift[None]).reshape(80, 128)
    spread = jnp.where(
        lanes(lambda r, l: ((l & 31) // 2 == (r & 31)) & (r // 32 == l // 32)), 1.0, 0.0
    )
    wide = dot(u3, spread)
    pool_ref[pl.ds(0, 80, 2), :] = wide
    pool_ref[pl.ds(1, 80, 2), :] = wide
    lifted = pool_ref[0:160, :].reshape(5, 1, 32, 128)
    u = (u2[11:21].reshape(5, 2, 32, 128) + lifted).reshape(10, 32, 128)
    u = sweep_of(b2[13:21], inner(u), u[:-2], u[2:], group_ring, 2)
    u = sweep_of(b2[14:20], inner(u), u[:-2], u[2:], group_ring, 2)
    final_ref[...] = u
    return jnp.concatenate([final_ref[parity + h] for h in range(5)], axis=0)


def up_kernel(
    me_ref, meta_ref, lift_ref, g0_ref, g1_ref, g2_ref, g3_ref, g4_ref,
    pairs_ref, low_ref, own_ref, high_ref, vel_ref, pay_ref,
    window_ref, pool_ref, final_ref, lift1_ref, b1_ref, u1_ref, v1_ref, lift0_ref, u0_ref,
    v0_ref, ext_ref,
):
    blocks = (g0_ref, g1_ref, g2_ref, g3_ref, g4_ref)
    coarse = coarse_part(me_ref[0], blocks, lift_ref, window_ref, pool_ref, final_ref)
    for c in range(3):
        spread = jnp.where(lanes(lambda r, l: r == 32 * c + (l & 63) // 2), 1.0, 0.0)
        wide = dot(coarse, spread)
        lift1_ref[c, pl.ds(0, 160, 2), :] = wide
        lift1_ref[c, pl.ds(1, 160, 2), :] = wide
    spread0 = jnp.where(lanes(lambda r, l: r == l // 2), 1.0, 0.0)

    def b_at(z, c):
        if 0 <= z < CZ:
            return own_ref[z, c]
        ref, first = (low_ref, z + 3) if z < 0 else (high_ref, z - CZ)
        return ref[pl.ds(pl.multiple_of(128 * (3 * first + c), 128), 128), :]

    def component(c, carry):
        for j in range(3):
            b1_ref[2 * j], b1_ref[2 * j + 1] = both_layers(pairs_ref[j, c])
        rows = pl.ds(pl.multiple_of(U_ROW + 64 * c, 64), 64)
        u1 = list(both_layers(low_ref[rows, :]))
        for i in range(1, 5):
            u1.append(start_of(b1_ref[i], b1_ref[i - 1], b1_ref[i + 1], flat_ring, 1))
        u1.extend(both_layers(high_ref[rows, :]))
        for z in range(-3, 5):
            h = z // 2 + 2
            u1_ref[z + 3] = u1[z + 3] + lift1_ref[c, 64 * h : 64 * h + 64, :]
        for z in range(-2, 4):
            i = z + 3
            v1_ref[z + 2] = sweep_of(
                b1_ref[z + 2], u1_ref[i], u1_ref[i - 1], u1_ref[i + 1], flat_ring, 1
            )
        for z in range(-1, 3):
            i = z + 2
            value = sweep_of(
                b1_ref[z + 2], v1_ref[i], v1_ref[i - 1], v1_ref[i + 1], flat_ring, 1
            )
            wide = dot(value, spread0)
            lift0_ref[z + 1, pl.ds(0, 64, 2), :] = wide
            lift0_ref[z + 1, pl.ds(1, 64, 2), :] = wide
        for z in range(-2, 6):
            u0_ref[z + 2] = (
                start_of(b_at(z, c), b_at(z - 1, c), b_at(z + 1, c), flat_ring, 0)
                + lift0_ref[z // 2 + 1]
            )
        for z in range(-1, 5):
            i = z + 2
            v0_ref[z + 1] = sweep_of(
                b_at(z, c), u0_ref[i], u0_ref[i - 1], u0_ref[i + 1], flat_ring, 0
            )
        for z in range(CZ):
            i = z + 1
            value = sweep_of(
                own_ref[z, c], v0_ref[i], v0_ref[i - 1], v0_ref[i + 1], flat_ring, 0
            )
            vel_ref[z, c] = value
            rounded = value.astype(BF16).astype(F32)
            ext_ref[3 * z + c, 0:128, :] = rounded
            ext_ref[3 * z + c, 128:144, :] = rounded[0:16]
        return carry

    lax.fori_loop(0, 3, component, 0)
    lane = iota((8, 128), 1)
    sub = iota((8, 128), 0)

    part = [(lane // BOX) % CZ == k for k in range(CZ)]

    def gather(order, head, base_y):
        base_x = jnp.maximum(head - 1, 0)
        shift = base_x & 7
        row = pl.multiple_of(base_x - shift, 8)
        late = sub >= shift
        values = []
        for k in range(CZ):
            step = (HALF * order + BOX * k - base_y) & 127
            line = []
            for c in range(3):
                tiles = [ext_ref[3 * k + c, pl.ds(row + 8 * n, 8), :] for n in range(3)]
                for n in range(2):
                    value = jnp.where(late, tiles[n], tiles[n + 1])
                    line.append(pltpu.roll(value, step, 1))
            values.append(line)
        return (8 - shift) & 7, values

    group = together(pay_ref.shape[0], 8)

    def several(step, carry):
        found = []
        for n in range(group):
            for order in range(2):
                at = 8 * (step * group + n) + 4 * order
                found.append(gather(order, meta_ref[at], meta_ref[at + 1]))
        for n in range(group):
            pieces = []
            for m in range(6):
                both = []
                for order in range(2):
                    back, values = found[2 * n + order]
                    packed = values[0][m]
                    for k in range(1, CZ):
                        packed = jnp.where(part[k], values[k][m], packed)
                    both.append(pltpu.roll(packed, back, 0))
                pieces.append(jnp.where(lane < HALF, both[0], both[1]))
            pay_ref[step * group + n] = jnp.concatenate(pieces, axis=0).astype(BF16)
        return carry

    lax.fori_loop(0, pay_ref.shape[0] // group, several, 0)


def way_up(me, meta, lift, blocks, pairs, low, own, high, slots):
    return call(
        up_kernel,
        (
            shaped(own.shape, F32, False),
            shaped((slots, ROWS, 128), BF16),
        ),
        [SMEM, SMEM] + [VMEM] * 10,
        [
            pltpu.VMEM((5 * LOCAL, 24, 128), F32),
            pltpu.VMEM((480, 128), F32),
            pltpu.VMEM((6, 32, 128), F32),
            pltpu.VMEM((3, 320, 128), F32),
            pltpu.VMEM((6, 64, 128), F32),
            pltpu.VMEM((8, 64, 128), F32),
            pltpu.VMEM((6, 64, 128), F32),
            pltpu.VMEM((4, 128, 128), F32),
            pltpu.VMEM((8, 128, 128), F32),
            pltpu.VMEM((6, 128, 128), F32),
            pltpu.VMEM((12, 144, 128), F32),
        ],
    )(me, meta, *map(near, (lift, *blocks, pairs, low, own, high)))


def read_kernel(dest_ref, pay_ref, pos_ref, out_ref, stage_ref, count_ref):
    slots = pay_ref.shape[0]

    def widen(t, carry):
        count_ref[t] = 0
        stage_ref[t] = pay_ref[t].astype(F32)
        return carry

    lax.fori_loop(0, slots, widen, 0, unroll=4)
    lane = iota((8, 128), 1)

    group = together(pos_ref.shape[1], 16)

    def one(block, target, order):
        weight_x, weight_y, weight_z = box_weights(pos_ref, block)
        mine = lane // HALF == order
        left = []
        for n in range(6):
            packed = stage_ref[target, 8 * n : 8 * n + 8, :]
            left.append(jnp.where(mine, packed, pltpu.roll(packed, HALF, 1)))
        left = jnp.concatenate(left, axis=0).astype(BF16)
        right = jnp.concatenate(by_levels(weight_y, weight_z), axis=0)
        spread = lax.dot_general(
            left, right, (((1,), (0,)), ((), ())), preferred_element_type=F32
        )
        for c in range(3):
            value = spread[BOX * c : BOX * c + BOX] * weight_x
            out_ref[c, pl.ds(block, 1), :] = jnp.sum(value, axis=0, keepdims=True)

    def several(step, carry):
        places = []
        for n in range(group):
            target = dest_ref[0, step * group + n]
            order = count_ref[target]
            count_ref[target] = order + 1
            places.append((target, order))
        for n in range(group):
            one(step * group + n, *places[n])
        return carry

    lax.fori_loop(0, pos_ref.shape[1] // group, several, 0)


def read(dest, payload, positions):
    slots = payload.shape[0]
    return call(
        read_kernel,
        shaped(positions.shape, F32, False),
        [SMEM, VMEM, VMEM],
        [pltpu.VMEM((slots, ROWS, 128), F32), pltpu.SMEM((slots,), jnp.int32)],
    )(far(dest), near(payload), near(positions))


def moved(value, step):
    size = lax.axis_size(AX)
    return lax.ppermute(value, AX, [(i, (i + step) % size) for i in range(size)])


def exchanged(value, axes=AX):
    return lax.all_to_all(value, axes, split_axis=0, concat_axis=0, tiled=True)


def shards(marker_positions, marker_forces, dest_slab, base_cells, fluid_source):
    slots = lax.axis_size(AX)
    positions = marker_positions.transpose(1, 0, 2)
    forces = marker_forces.transpose(1, 0, 2)
    dest = dest_slab.T
    me = lax.axis_index(AX).astype(jnp.int32).reshape(1)
    payload = exchanged(build(dest, base_cells.T, positions, forces, fluid_source, slots))
    meta = payload[:, 0:1, ::BOX].astype(jnp.int32).reshape(8 * slots)
    source, up, down, up2, down2, lift = place(meta, payload, fluid_source)
    m1, m2 = moved(up, 1), moved(up2, 2)
    p1, p2 = moved(down, -1), moved(down2, -2)
    pairs, share, rise, sink = middle_down(source, up, down, m1, p1, m2, p2)
    middle = exchanged(share, AX[1])
    low, high = moved(rise, 1), moved(sink, -1)
    blocks = [middle if n == 0 else moved(middle, -LOCAL * n) for n in range(-2, 3)]
    velocity, picked = way_up(me, meta, lift, blocks, pairs, low, source, high, slots)
    out = read(dest, exchanged(picked), positions)
    return velocity, out.transpose(1, 0, 2)


def solution(mesh):
    torus = Mesh(mesh.devices.reshape(-1, LOCAL), AX)
    return jax.shard_map(
        shards,
        mesh=torus,
        in_specs=(P(AX), P(AX), P(AX), P(AX), P(AX)),
        out_specs=(P(AX), P(AX)),
        check_vma=False,
    )
```

```python
import math

import jax
import jax.numpy as jnp
from jax import lax
from jax.experimental import pallas as pl
from jax.experimental.pallas import tpu as pltpu
from jax.sharding import Mesh
from jax.sharding import PartitionSpec as P

AX = ("hi", "lo")
LOCAL = 8
BOX = 16
CZ = 4
HALF = CZ * BOX
ROWS = 3 * BOX
SCREEN = 1.0 / 64.0
RELAX = 2.0 / 3.0
INTERPRET = False
F32 = jnp.float32
BF16 = jnp.bfloat16
HIGH = lax.Precision.HIGHEST


def level(index):
    q = 0.25**index
    return q, SCREEN + 6.0 * q, RELAX / (SCREEN + 6.0 * q)


def call(body, out_shape, in_specs=None, scratch=(), megabytes=24):
    options = {} if in_specs is None else {"in_specs": in_specs}
    return pl.pallas_call(
        body,
        out_shape=out_shape,
        scratch_shapes=list(scratch),
        interpret=INTERPRET,
        compiler_params=pltpu.CompilerParams(vmem_limit_bytes=megabytes << 20),
        **options,
    )


def shaped(shape, dtype, near=True):
    if near and not INTERPRET:
        return pltpu.VMEM(shape, dtype)
    return jax.ShapeDtypeStruct(shape, dtype)


def near(value):
    return value if INTERPRET else pltpu.with_memory_space_constraint(value, pltpu.VMEM)


VMEM = pl.BlockSpec(memory_space=pltpu.VMEM)
SMEM = pl.BlockSpec(memory_space=pltpu.SMEM)


def far(value):
    return value if INTERPRET else pltpu.with_memory_space_constraint(value, pltpu.HBM)


def iota(shape, dim):
    return lax.broadcasted_iota(jnp.int32, shape, dim)


COS = (
    0.9999999999524891,
    -1.2337005406331254,
    0.2536692036544627,
    -0.02086006949632079,
    0.0009036280586426939,
)
SIN = (
    1.5707963267880989,
    -0.6459640961467292,
    0.07969258272440714,
    -0.004681266248964948,
    0.00015820628792786513,
)


def polynomial(coefficients, x):
    value = x * coefficients[-1] + coefficients[-2]
    for coefficient in coefficients[-3::-1]:
        value = value * x + coefficient
    return value


def split(value):
    high = value.astype(BF16)
    return high, (value - high.astype(F32)).astype(BF16)


def waves(pos_ref, first, group, wave_ref):
    rows = pl.ds(pl.multiple_of(first, group), group)
    for axis in range(3):
        point = pos_ref[axis, rows, :]
        point = 2.0 + (BOX - 5) * point if axis < 2 else (CZ - 1) * point
        nearest = jnp.floor(point + 0.5)
        rest = point - nearest
        square = rest * rest
        even = polynomial(COS, square)
        odd = polynomial(SIN, square) * rest
        quarter = nearest.astype(jnp.int32) & 3
        swap = (quarter & 1) == 1
        cosine = jnp.where(swap, odd, even)
        sine = jnp.where(swap, even, odd)
        wave_ref[3 * axis] = point
        wave_ref[3 * axis + 1] = jnp.where((quarter == 1) | (quarter == 2), -cosine, cosine)
        wave_ref[3 * axis + 2] = jnp.where(quarter >= 2, -sine, sine)


def box_weights(wave_ref, block):
    row = slice(block, block + 1)
    cell = iota((8, 256), 0)
    sign = jnp.where(cell % 4 < 2, 0.25, -0.25)
    weights = []
    for axis in range(3):
        point, cosine, sine = (wave_ref[3 * axis + n, row, :] for n in range(3))
        pattern = jnp.where(cell % 2 == 0, cosine, sine) * sign + 0.25
        parts = []
        for first in range(0, BOX if axis < 2 else 8, 8):
            offset = point - (cell + first).astype(F32)
            parts.append(jnp.where(jnp.abs(offset) < 2.0, pattern, 0.0))
        weights.append(jnp.concatenate(parts, axis=0) if axis < 2 else parts[0])
    return weights


def by_levels(weight_y, weight_z):
    return split(jnp.concatenate([weight_z[k : k + 1] * weight_y for k in range(CZ)], axis=0))


PIECES = (2 * BOX, 3 * BOX, 3 * BOX - 1)


def together(count, most):
    return math.gcd(count, most)


def build_kernel(
    dest_ref, base_ref, pos_ref, frc_ref, fluid_ref, out_ref, stage_ref, count_ref, wave_ref
):
    slots = out_ref.shape[0]
    blocks = pos_ref.shape[1]
    group = together(blocks, 16)

    def clear(t, carry):
        count_ref[t] = 0
        stage_ref[t, 0:8, :] = jnp.zeros((8, 128), F32)
        return carry

    lax.fori_loop(0, slots, clear, 0, unroll=4)
    lane = iota((8, 128), 1)
    top = iota((8, 128), 0) == 0

    def one(first, n):
        block = first + n
        weight_x, weight_y, weight_z = box_weights(wave_ref, n)
        loaded = [frc_ref[c, pl.ds(block, 1), :] * weight_x for c in range(3)]
        high, low = split(jnp.concatenate(loaded, axis=0))
        right = jnp.concatenate(by_levels(weight_y, weight_z), axis=0)
        dims = (((1,), (1,)), ((), ()))
        box = lax.dot_general(high, right, dims, preferred_element_type=F32)
        box = box + lax.dot_general(low, right, dims, preferred_element_type=F32)
        box = box + pltpu.roll(box, HALF, 1)
        base_x = base_ref[0, block].astype(F32) + 1.0
        base_y = base_ref[1, block].astype(F32)
        tiles = [box[8 * n : 8 * n + 8] for n in range(6)]
        rounded = [tile.astype(BF16).astype(F32) for tile in tiles]
        sums = [rounded[2 * c] + rounded[2 * c + 1] for c in range(3)]
        tiles[0] = jnp.where(top & (lane % HALF == 0), base_x, tiles[0])
        tiles[0] = jnp.where(top & (lane % HALF == BOX), base_y, tiles[0])
        return tiles, sums

    def several(step, carry):
        results = []
        waves(pos_ref, step * group, group, wave_ref)
        for n in range(group):
            tiles, sums = one(step * group, n)
            results.append(tiles)
            carry = tuple(a + b for a, b in zip(carry, sums))
        for n in range(group):
            target = dest_ref[0, step * group + n]
            order = count_ref[target]
            count_ref[target] = order + 1
            mine = lane // HALF == order
            for m in range(6):
                rows = slice(8 * m, 8 * m + 8)
                stage_ref[target, rows, :] = jnp.where(
                    mine, results[n][m], stage_ref[target, rows, :]
                )
        return carry

    fluid = []
    for c in range(3):
        column = fluid_ref[0, c] + fluid_ref[1, c] + (fluid_ref[2, c] + fluid_ref[3, c])
        fluid.append(jnp.sum(column.reshape(16, 8, 128), axis=0))
    zero = jnp.zeros((8, 128), F32)
    boxes = lax.fori_loop(0, blocks // group, several, (zero, zero, zero))
    fluid = [a + 0.5 * b for a, b in zip(fluid, boxes)]
    pieces = []
    for c in range(3):
        rest = jnp.broadcast_to(jnp.sum(fluid[c], axis=(0, 1), keepdims=True), (8, 128))
        marked = jnp.zeros((8, 128), F32)
        for place_of in PIECES:
            part = rest.astype(BF16).astype(F32)
            marked = jnp.where(lane == place_of, part, marked)
            rest = rest - part
        pieces.append(marked)
    held = top & ((lane == PIECES[0]) | (lane == PIECES[1]) | (lane == PIECES[2]))

    def finish(t, carry):
        tiles = []
        for c in range(3):
            row = BOX * c
            tiles.append(jnp.where(held, pieces[c], stage_ref[t, row : row + 8, :]))
            tiles.append(stage_ref[t, row + 8 : row + BOX, :])
        out_ref[t] = jnp.concatenate(tiles, axis=0).astype(BF16)
        return carry

    lax.fori_loop(0, slots, finish, 0, unroll=4)


def build(dest, base, positions, forces, fluid, slots):
    return call(
        build_kernel,
        shaped((slots, ROWS, 128), BF16),
        [SMEM, SMEM, VMEM, VMEM, VMEM],
        [
            pltpu.VMEM((slots, ROWS, 128), F32),
            pltpu.SMEM((slots,), jnp.int32),
            pltpu.VMEM((9, together(positions.shape[1], 16), 256), F32),
        ],
    )(*map(far, (dest, base, positions, forces, fluid)))


def flat_ring(x):
    rows = x.shape[-2]
    ax = x.ndim - 2
    return (
        pltpu.roll(x, 1, ax)
        + pltpu.roll(x, rows - 1, ax)
        + (pltpu.roll(x, 1, ax + 1) + pltpu.roll(x, 127, ax + 1))
    )


def group_ring(x):
    rows = x.shape[-2]
    ax = x.ndim - 2
    lane = iota(x.shape, ax + 1) & 31
    before = jnp.where(lane == 0, pltpu.roll(x, 97, ax + 1), pltpu.roll(x, 1, ax + 1))
    after = jnp.where(lane == 31, pltpu.roll(x, 31, ax + 1), pltpu.roll(x, 127, ax + 1))
    return pltpu.roll(x, 1, ax) + pltpu.roll(x, rows - 1, ax) + (before + after)


def start_of(b, below, above, ring, index):
    q, _, w = level(index)
    return w * ((4.0 / 3.0) * b + (w * q) * (ring(b) + (below + above)))


def left_of(b, u, below, above, ring, index):
    q, diag, _ = level(index)
    return b - diag * u + q * (ring(u) + (below + above))


def sweep_of(b, u, below, above, ring, index):
    q, _, w = level(index)
    return (1.0 - RELAX) * u + (w * b + (w * q) * (ring(u) + (below + above)))


def dot(left, right):
    return lax.dot_general(
        left, right, (((1,), (0,)), ((), ())), precision=HIGH, preferred_element_type=F32
    )


def lanes(test):
    return test(iota((128, 128), 0), iota((128, 128), 1))


def place_kernel(
    meta_ref, pay_ref, fluid_ref,
    src_ref, up_ref, down_ref, up2_ref, down2_ref, lift_ref,
    grid_ref, u_ref, sum_ref,
):
    slots = pay_ref.shape[0]
    lane = iota((8, 128), 1)
    sub = iota((8, 128), 0)
    for z in range(CZ):
        for c in range(3):
            grid_ref[3 * z + c, 0:128, :] = fluid_ref[z, c]
            grid_ref[3 * z + c, 128:144, :] = jnp.zeros((16, 128), F32)

    def turned(tile, order, head, base_y):
        base_x = jnp.maximum(head - 1, 0)
        shift = base_x & 7
        row = pl.multiple_of(base_x - shift, 8)
        window = (lane - base_y) & 127
        inside = (window >= 1) & (window <= BOX - 2) & (head > 0)
        late = inside & (sub >= shift)
        early = inside & (sub < shift)
        pieces = [pltpu.roll(tile[8 * n : 8 * n + 8], shift, 0) for n in range(6)]
        values = []
        for k in range(CZ):
            step = (base_y - HALF * order - BOX * k) & 127
            values.append([pltpu.roll(piece, step, 1) for piece in pieces])
        return row, late, early, values

    def add(row, late, early, values):
        for k in range(CZ):
            for c in range(3):
                first, second = values[k][2 * c], values[k][2 * c + 1]
                kc = 3 * k + c
                grid_ref[kc, pl.ds(row, 8), :] += jnp.where(late, first, 0.0)
                grid_ref[kc, pl.ds(row + 8, 8), :] += jnp.where(
                    early, first, jnp.where(late, second, 0.0)
                )
                grid_ref[kc, pl.ds(row + 16, 8), :] += jnp.where(early, second, 0.0)

    group = together(slots, 8)

    def several(step, carry):
        found = []
        for n in range(group):
            d = step * group + n
            tile = pay_ref[d].astype(F32)
            carry = tuple(
                carry[c] + jnp.where(held, tile[BOX * c : BOX * c + 8], 0.0) for c in range(3)
            )
            for order in range(2):
                at = 8 * d + 4 * order
                found.append(turned(tile, order, meta_ref[at], meta_ref[at + 1]))
        for one in found:
            add(*one)
        return carry

    held = (sub == 0) & ((lane == PIECES[0]) | (lane == PIECES[1]) | (lane == PIECES[2]))
    zero = jnp.zeros((8, 128), F32)
    totals = lax.fori_loop(0, slots // group, several, (zero, zero, zero))
    factor = (1.0 - level(3)[2] * SCREEN) ** 6 / SCREEN
    for index in range(3):
        factor = factor * (1.0 - level(index)[2] * SCREEN) ** 2
    scale = factor / (slots * CZ * 128.0 * 128.0)
    lift_ref[...] = zero
    for c in range(3):
        total = jnp.sum(totals[c], axis=(0, 1), keepdims=True)
        lift_ref[c : c + 1, :] = jnp.broadcast_to(total * scale, (1, 128))
    pool = [
        jnp.where(lanes(lambda r, l: (r // 2 == (l & 63)) & (l // 64 == half)), 0.125, 0.0)
        for half in range(2)
    ]
    q, _, w = level(0)
    spill_up, spill_down = [], []
    for c in range(3):
        for z in range(CZ):
            kc = 3 * z + c
            grid_ref[kc, 0:16, :] += grid_ref[kc, 128:144, :]
            src_ref[z, c] = grid_ref[kc, 0:128, :]

        def b_at(z):
            return src_ref[z, c] if 0 <= z < CZ else 0.0

        for z in range(CZ):
            u_ref[z + 1] = start_of(src_ref[z, c], b_at(z - 1), b_at(z + 1), flat_ring, 0)
        u_ref[0] = (w * w * q) * src_ref[0, c]
        u_ref[CZ + 1] = (w * w * q) * src_ref[CZ - 1, c]

        def left(z):
            if z == -2:
                return q * u_ref[0]
            if z == CZ + 1:
                return q * u_ref[CZ + 1]
            below = u_ref[z] if z > -1 else 0.0
            above = u_ref[z + 2] if z < CZ else 0.0
            return left_of(b_at(z), u_ref[z + 1], below, above, flat_ring, 0)

        rows = []
        for pair in range(-1, 3):
            sum_ref[...] = left(2 * pair) + left(2 * pair + 1)
            rows.append(sum_ref[pl.ds(0, 64, 2), :] + sum_ref[pl.ds(1, 64, 2), :])
        own = dot(rows[1], pool[0]) + dot(rows[2], pool[1])
        up_ref[c] = own
        down_ref[c] = own
        spill_down.append(dot(rows[0], pool[c % 2]))
        spill_up.append(dot(rows[3], pool[c % 2]))
    for ref, far_ref, spill in ((up_ref, up2_ref, spill_up), (down_ref, down2_ref, spill_down)):
        both = spill[0] + spill[1]
        ref[3] = both
        ref[4] = spill[2]
        far_ref[0] = both
        far_ref[1] = spill[2]


def place(meta, payload, fluid):
    return call(
        place_kernel,
        (
            shaped(fluid.shape, F32),
            shaped((5, 64, 128), F32),
            shaped((5, 64, 128), F32),
            shaped((2, 64, 128), F32),
            shaped((2, 64, 128), F32),
            shaped((8, 128), F32),
        ),
        [SMEM, VMEM, VMEM],
        [
            pltpu.VMEM((12, 144, 128), F32),
            pltpu.VMEM((CZ + 2, 128, 128), F32),
            pltpu.VMEM((128, 128), F32),
        ],
    )(meta, near(payload), near(fluid))


def both_layers(tile):
    lane = iota(tile.shape, tile.ndim - 1)
    turned = pltpu.roll(tile, 64, tile.ndim - 1)
    return jnp.where(lane < 64, tile, turned), jnp.where(lane < 64, turned, tile)


def pack_coarse(value):
    last = value[24:32]
    lane = iota((8, 128), 1)
    return [
        jnp.where(lane < 96, value[8 * c : 8 * c + 8], pltpu.roll(last, 96 - 32 * c, 1))
        for c in range(3)
    ]


def unpack_coarse(tile):
    lane = iota((8, 128), 1)
    last = jnp.zeros((8, 128), F32)
    rows = []
    for c in range(3):
        piece = tile[8 * c : 8 * c + 8]
        turned = pltpu.roll(piece, (32 * c - 96) % 128, 1)
        last = jnp.where(lane // 32 == c, turned, last)
        rows.append(jnp.where(lane < 96, piece, 0.0))
    return jnp.concatenate(rows + [last], axis=0)


def spilled(ref, c, first=0):
    return both_layers(ref[first + c // 2])[c % 2]


U_ROW = 12 * 128


def middle_kernel(
    src_ref, up_ref, down_ref, m1_ref, p1_ref, m2_ref, p2_ref,
    pairs_ref, out_ref, rise_ref, sink_ref, sum_ref,
):
    total = None
    for ref, order in ((rise_ref, (3, 2, 1)), (sink_ref, (0, 1, 2))):
        for c in range(3):
            parts = split(src_ref[order[0], c])
            parts += tuple(src_ref[z, c].astype(BF16) for z in order[1:])
            for n in range(4):
                ref[128 * (3 * n + c) : 128 * (3 * n + c + 1), :] = parts[n]
    lane = iota((64, 128), 1)
    for c in range(3):
        m1, own, p1 = both_layers(m1_ref[c]), both_layers(up_ref[c]), both_layers(p1_ref[c])
        b = [
            m1[0] + spilled(m2_ref, c),
            m1[1] + spilled(down_ref, c, 3),
            own[0] + spilled(m1_ref, c, 3),
            own[1] + spilled(p1_ref, c, 3),
            p1[0] + spilled(up_ref, c, 3),
            p1[1] + spilled(p2_ref, c),
        ]
        for j in range(3):
            pairs_ref[j, c] = jnp.where(lane < 64, b[2 * j], b[2 * j + 1])
        u = [start_of(b[i], b[i - 1], b[i + 1], flat_ring, 1) for i in range(1, 5)]
        rows = slice(U_ROW + 64 * c, U_ROW + 64 * c + 64)
        rise_ref[rows, :] = jnp.where(lane < 64, u[0], u[1]).astype(BF16)
        sink_ref[rows, :] = jnp.where(lane < 64, u[2], u[3]).astype(BF16)
        left = [left_of(b[i + 1], u[i], u[i - 1], u[i + 1], flat_ring, 1) for i in (1, 2)]
        sum_ref[...] = left[0] + left[1]
        rows = sum_ref[pl.ds(0, 32, 2), :] + sum_ref[pl.ds(1, 32, 2), :]
        pool = jnp.where(
            lanes(lambda r, l: (r // 2 == (l & 31)) & (l // 32 == c) & (r < 64)), 0.125, 0.0
        )
        part = dot(rows, pool)
        total = part if total is None else total + part
    packed = jnp.concatenate(pack_coarse(total), axis=0)
    for d in range(out_ref.shape[0]):
        out_ref[d] = packed


def middle_down(source, up, down, m1, p1, m2, p2):
    return call(
        middle_kernel,
        (
            shaped((3, 3, 64, 128), F32),
            shaped((LOCAL, 24, 128), F32),
            shaped((U_ROW + 192, 128), BF16),
            shaped((U_ROW + 192, 128), BF16),
        ),
        None,
        [pltpu.VMEM((64, 128), F32)],
    )(*map(near, (source, up, down, m1, p1, m2, p2)))


def inner(x):
    return x[1:-1]


def coarse_part(me, blocks, lift_ref, window_ref, pool_ref, final_ref):
    parity = me % 2
    first = me % LOCAL - parity
    for n, ref in enumerate(blocks):
        window_ref[LOCAL * n : LOCAL * n + LOCAL] = ref[...]
    b2 = jnp.stack([unpack_coarse(window_ref[first + t]) for t in range(34)])
    group = iota((1, 128), 1) // 32
    lift = jnp.zeros((1, 128), F32)
    for c in range(3):
        lift = jnp.where(group == c, lift_ref[c : c + 1, :], lift)
    _, _, w3 = level(3)
    u2 = start_of(inner(b2), b2[:-2], b2[2:], group_ring, 2)
    r2 = left_of(b2[2:-2], inner(u2), u2[:-2], u2[2:], group_ring, 2)
    pairs = r2.reshape(15, 2, 32, 128)
    pool_ref[...] = (pairs[:, 0] + pairs[:, 1]).reshape(480, 128)
    rows = pool_ref[pl.ds(0, 240, 2), :] + pool_ref[pl.ds(1, 240, 2), :]
    pool = jnp.where(
        lanes(lambda r, l: ((r & 31) // 2 == (l & 15)) & (r // 32 == l // 32)), 0.125, 0.0
    )
    b3 = dot(rows, pool).reshape(15, 16, 128)
    u3 = w3 * b3
    for _ in range(5):
        b3 = inner(b3)
        u3 = sweep_of(b3, inner(u3), u3[:-2], u3[2:], group_ring, 3)
    u3 = (u3 + lift[None]).reshape(80, 128)
    spread = jnp.where(
        lanes(lambda r, l: ((l & 31) // 2 == (r & 31)) & (r // 32 == l // 32)), 1.0, 0.0
    )
    wide = dot(u3, spread)
    pool_ref[pl.ds(0, 80, 2), :] = wide
    pool_ref[pl.ds(1, 80, 2), :] = wide
    lifted = pool_ref[0:160, :].reshape(5, 1, 32, 128)
    u = (u2[11:21].reshape(5, 2, 32, 128) + lifted).reshape(10, 32, 128)
    u = sweep_of(b2[13:21], inner(u), u[:-2], u[2:], group_ring, 2)
    u = sweep_of(b2[14:20], inner(u), u[:-2], u[2:], group_ring, 2)
    final_ref[...] = u
    return jnp.concatenate([final_ref[parity + h] for h in range(5)], axis=0)


def up_kernel(
    me_ref, meta_ref, lift_ref, g0_ref, g1_ref, g2_ref, g3_ref, g4_ref,
    pairs_ref, low_ref, own_ref, high_ref, vel_ref, pay_ref,
    window_ref, pool_ref, final_ref, lift1_ref, b1_ref, u1_ref, v1_ref, lift0_ref, u0_ref,
    v0_ref, ext_ref, halo_ref,
):
    blocks = (g0_ref, g1_ref, g2_ref, g3_ref, g4_ref)
    coarse = coarse_part(me_ref[0], blocks, lift_ref, window_ref, pool_ref, final_ref)
    for c in range(3):
        spread = jnp.where(lanes(lambda r, l: r == 32 * c + (l & 63) // 2), 1.0, 0.0)
        wide = dot(coarse, spread)
        lift1_ref[c, pl.ds(0, 160, 2), :] = wide
        lift1_ref[c, pl.ds(1, 160, 2), :] = wide
    spread0 = jnp.where(lanes(lambda r, l: r == l // 2), 1.0, 0.0)

    def b_at(z, c):
        if 0 <= z < CZ:
            return own_ref[z, c]
        return halo_ref[z + 3 if z < 0 else z - 1]

    def component(c, carry):
        for ref, order in ((low_ref, (2, 1, 0)), (high_ref, (3, 4, 5))):
            planes = [
                ref[pl.ds(pl.multiple_of(128 * (3 * n + c), 128), 128), :].astype(F32)
                for n in range(4)
            ]
            halo_ref[order[0]] = planes[0] + planes[1]
            halo_ref[order[1]] = planes[2]
            halo_ref[order[2]] = planes[3]
        for j in range(3):
            b1_ref[2 * j], b1_ref[2 * j + 1] = both_layers(pairs_ref[j, c])
        rows = pl.ds(pl.multiple_of(U_ROW + 64 * c, 64), 64)
        u1 = list(both_layers(low_ref[rows, :].astype(F32)))
        for i in range(1, 5):
            u1.append(start_of(b1_ref[i], b1_ref[i - 1], b1_ref[i + 1], flat_ring, 1))
        u1.extend(both_layers(high_ref[rows, :].astype(F32)))
        for z in range(-3, 5):
            h = z // 2 + 2
            u1_ref[z + 3] = u1[z + 3] + lift1_ref[c, 64 * h : 64 * h + 64, :]
        for z in range(-2, 4):
            i = z + 3
            v1_ref[z + 2] = sweep_of(
                b1_ref[z + 2], u1_ref[i], u1_ref[i - 1], u1_ref[i + 1], flat_ring, 1
            )
        for z in range(-1, 3):
            i = z + 2
            value = sweep_of(
                b1_ref[z + 2], v1_ref[i], v1_ref[i - 1], v1_ref[i + 1], flat_ring, 1
            )
            wide = dot(value, spread0)
            lift0_ref[z + 1, pl.ds(0, 64, 2), :] = wide
            lift0_ref[z + 1, pl.ds(1, 64, 2), :] = wide
        for z in range(-2, 6):
            u0_ref[z + 2] = (
                start_of(b_at(z, c), b_at(z - 1, c), b_at(z + 1, c), flat_ring, 0)
                + lift0_ref[z // 2 + 1]
            )
        for z in range(-1, 5):
            i = z + 2
            v0_ref[z + 1] = sweep_of(
                b_at(z, c), u0_ref[i], u0_ref[i - 1], u0_ref[i + 1], flat_ring, 0
            )
        for z in range(CZ):
            i = z + 1
            value = sweep_of(
                own_ref[z, c], v0_ref[i], v0_ref[i - 1], v0_ref[i + 1], flat_ring, 0
            )
            vel_ref[z, c] = value
            rounded = value.astype(BF16).astype(F32)
            ext_ref[3 * z + c, 0:128, :] = rounded
            ext_ref[3 * z + c, 128:144, :] = rounded[0:16]
        return carry

    lax.fori_loop(0, 3, component, 0)
    lane = iota((8, 128), 1)
    sub = iota((8, 128), 0)

    part = [(lane // BOX) % CZ == k for k in range(CZ)]

    def gather(order, head, base_y):
        base_x = jnp.maximum(head - 1, 0)
        shift = base_x & 7
        row = pl.multiple_of(base_x - shift, 8)
        late = sub >= shift
        values = []
        for k in range(CZ):
            step = (HALF * order + BOX * k - base_y) & 127
            line = []
            for c in range(3):
                tiles = [ext_ref[3 * k + c, pl.ds(row + 8 * n, 8), :] for n in range(3)]
                for n in range(2):
                    value = jnp.where(late, tiles[n], tiles[n + 1])
                    line.append(pltpu.roll(value, step, 1))
            values.append(line)
        return (8 - shift) & 7, values

    group = together(pay_ref.shape[0], 8)

    def several(step, carry):
        found = []
        for n in range(group):
            for order in range(2):
                at = 8 * (step * group + n) + 4 * order
                found.append(gather(order, meta_ref[at], meta_ref[at + 1]))
        for n in range(group):
            pieces = []
            for m in range(6):
                both = []
                for order in range(2):
                    back, values = found[2 * n + order]
                    packed = values[0][m]
                    for k in range(1, CZ):
                        packed = jnp.where(part[k], values[k][m], packed)
                    both.append(pltpu.roll(packed, back, 0))
                pieces.append(jnp.where(lane < HALF, both[0], both[1]))
            pay_ref[step * group + n] = jnp.concatenate(pieces, axis=0).astype(BF16)
        return carry

    lax.fori_loop(0, pay_ref.shape[0] // group, several, 0)


def way_up(me, meta, lift, blocks, pairs, low, own, high, slots):
    return call(
        up_kernel,
        (
            shaped(own.shape, F32, False),
            shaped((slots, ROWS, 128), BF16),
        ),
        [SMEM, SMEM] + [VMEM] * 10,
        [
            pltpu.VMEM((5 * LOCAL, 24, 128), F32),
            pltpu.VMEM((480, 128), F32),
            pltpu.VMEM((6, 32, 128), F32),
            pltpu.VMEM((3, 320, 128), F32),
            pltpu.VMEM((6, 64, 128), F32),
            pltpu.VMEM((8, 64, 128), F32),
            pltpu.VMEM((6, 64, 128), F32),
            pltpu.VMEM((4, 128, 128), F32),
            pltpu.VMEM((8, 128, 128), F32),
            pltpu.VMEM((6, 128, 128), F32),
            pltpu.VMEM((12, 144, 128), F32),
            pltpu.VMEM((6, 128, 128), F32),
        ],
    )(me, meta, *map(near, (lift, *blocks, pairs, low, own, high)))


def read_kernel(dest_ref, pay_ref, pos_ref, out_ref, stage_ref, count_ref, wave_ref):
    slots = pay_ref.shape[0]

    def widen(t, carry):
        count_ref[t] = 0
        stage_ref[t] = pay_ref[t].astype(F32)
        return carry

    lax.fori_loop(0, slots, widen, 0, unroll=4)
    lane = iota((8, 128), 1)

    group = together(pos_ref.shape[1], 16)

    def one(first, n, target, order):
        block = first + n
        weight_x, weight_y, weight_z = box_weights(wave_ref, n)
        mine = lane // HALF == order
        left = []
        for m in range(6):
            packed = stage_ref[target, 8 * m : 8 * m + 8, :]
            left.append(jnp.where(mine, packed, pltpu.roll(packed, HALF, 1)))
        left = jnp.concatenate(left, axis=0).astype(BF16)
        right = jnp.concatenate(by_levels(weight_y, weight_z), axis=0)
        spread = lax.dot_general(
            left, right, (((1,), (0,)), ((), ())), preferred_element_type=F32
        )
        for c in range(3):
            value = spread[BOX * c : BOX * c + BOX] * weight_x
            out_ref[c, pl.ds(block, 1), :] = jnp.sum(value, axis=0, keepdims=True)

    def several(step, carry):
        places = []
        for n in range(group):
            target = dest_ref[0, step * group + n]
            order = count_ref[target]
            count_ref[target] = order + 1
            places.append((target, order))
        waves(pos_ref, step * group, group, wave_ref)
        for n in range(group):
            one(step * group, n, *places[n])
        return carry

    lax.fori_loop(0, pos_ref.shape[1] // group, several, 0)


def read(dest, payload, positions):
    slots = payload.shape[0]
    return call(
        read_kernel,
        shaped(positions.shape, F32, False),
        [SMEM, VMEM, VMEM],
        [
            pltpu.VMEM((slots, ROWS, 128), F32),
            pltpu.SMEM((slots,), jnp.int32),
            pltpu.VMEM((9, together(positions.shape[1], 16), 256), F32),
        ],
    )(far(dest), near(payload), near(positions))


def moved(value, step):
    size = lax.axis_size(AX)
    return lax.ppermute(value, AX, [(i, (i + step) % size) for i in range(size)])


def exchanged(value, axes=AX):
    return lax.all_to_all(value, axes, split_axis=0, concat_axis=0, tiled=True)


def shards(marker_positions, marker_forces, dest_slab, base_cells, fluid_source):
    slots = lax.axis_size(AX)
    positions = marker_positions.transpose(1, 0, 2)
    forces = marker_forces.transpose(1, 0, 2)
    dest = dest_slab.T
    me = lax.axis_index(AX).astype(jnp.int32).reshape(1)
    payload = exchanged(build(dest, base_cells.T, positions, forces, fluid_source, slots))
    meta = payload[:, 0:1, ::BOX].astype(jnp.int32).reshape(8 * slots)
    source, up, down, up2, down2, lift = place(meta, payload, fluid_source)
    m1, m2 = moved(up, 1), moved(up2, 2)
    p1, p2 = moved(down, -1), moved(down2, -2)
    pairs, share, rise, sink = middle_down(source, up, down, m1, p1, m2, p2)
    middle = exchanged(share, AX[1])
    low, high = moved(rise, 1), moved(sink, -1)
    blocks = [middle if n == 0 else moved(middle, -LOCAL * n) for n in range(-2, 3)]
    velocity, picked = way_up(me, meta, lift, blocks, pairs, low, source, high, slots)
    out = read(dest, exchanged(picked), positions)
    return velocity, out.transpose(1, 0, 2)


def solution(mesh):
    torus = Mesh(mesh.devices.reshape(-1, LOCAL), AX)
    return jax.shard_map(
        shards,
        mesh=torus,
        in_specs=(P(AX), P(AX), P(AX), P(AX), P(AX)),
        out_specs=(P(AX), P(AX)),
        check_vma=False,
    )
```

```python
import math

import jax
import jax.numpy as jnp
from jax import lax
from jax.experimental import pallas as pl
from jax.experimental.pallas import tpu as pltpu
from jax.sharding import Mesh
from jax.sharding import PartitionSpec as P

AX = ("hi", "lo")
LOCAL = 16
BOX = 16
CZ = 4
HALF = CZ * BOX
ROWS = 3 * BOX
SCREEN = 1.0 / 64.0
RELAX = 2.0 / 3.0
INTERPRET = False
F32 = jnp.float32
BF16 = jnp.bfloat16
HIGH = lax.Precision.HIGHEST


def level(index):
    q = 0.25**index
    return q, SCREEN + 6.0 * q, RELAX / (SCREEN + 6.0 * q)


def call(body, out_shape, in_specs=None, scratch=(), megabytes=24):
    options = {} if in_specs is None else {"in_specs": in_specs}
    return pl.pallas_call(
        body,
        out_shape=out_shape,
        scratch_shapes=list(scratch),
        interpret=INTERPRET,
        compiler_params=pltpu.CompilerParams(vmem_limit_bytes=megabytes << 20),
        **options,
    )


def shaped(shape, dtype, near=True):
    if near and not INTERPRET:
        return pltpu.VMEM(shape, dtype)
    return jax.ShapeDtypeStruct(shape, dtype)


def near(value):
    return value if INTERPRET else pltpu.with_memory_space_constraint(value, pltpu.VMEM)


VMEM = pl.BlockSpec(memory_space=pltpu.VMEM)
SMEM = pl.BlockSpec(memory_space=pltpu.SMEM)


def far(value):
    return value if INTERPRET else pltpu.with_memory_space_constraint(value, pltpu.HBM)


def iota(shape, dim):
    return lax.broadcasted_iota(jnp.int32, shape, dim)


COS = (
    0.9999999999524891,
    -1.2337005406331254,
    0.2536692036544627,
    -0.02086006949632079,
    0.0009036280586426939,
)
SIN = (
    1.5707963267880989,
    -0.6459640961467292,
    0.07969258272440714,
    -0.004681266248964948,
    0.00015820628792786513,
)


def polynomial(coefficients, x):
    value = x * coefficients[-1] + coefficients[-2]
    for coefficient in coefficients[-3::-1]:
        value = value * x + coefficient
    return value


def split(value):
    high = value.astype(BF16)
    return high, (value - high.astype(F32)).astype(BF16)


def waves(pos_ref, first, group, wave_ref):
    rows = pl.ds(pl.multiple_of(first, group), group)
    for axis in range(3):
        point = pos_ref[axis, rows, :]
        point = 2.0 + (BOX - 5) * point if axis < 2 else (CZ - 1) * point
        nearest = jnp.floor(point + 0.5)
        rest = point - nearest
        square = rest * rest
        even = polynomial(COS, square)
        odd = polynomial(SIN, square) * rest
        quarter = nearest.astype(jnp.int32) & 3
        swap = (quarter & 1) == 1
        cosine = jnp.where(swap, odd, even)
        sine = jnp.where(swap, even, odd)
        wave_ref[3 * axis] = point
        wave_ref[3 * axis + 1] = jnp.where((quarter == 1) | (quarter == 2), -cosine, cosine)
        wave_ref[3 * axis + 2] = jnp.where(quarter >= 2, -sine, sine)


def box_weights(wave_ref, block):
    row = slice(block, block + 1)
    cell = iota((8, 256), 0)
    sign = jnp.where(cell % 4 < 2, 0.25, -0.25)
    weights = []
    for axis in range(3):
        point, cosine, sine = (wave_ref[3 * axis + n, row, :] for n in range(3))
        pattern = jnp.where(cell % 2 == 0, cosine, sine) * sign + 0.25
        parts = []
        for first in range(0, BOX if axis < 2 else 8, 8):
            offset = point - (cell + first).astype(F32)
            parts.append(jnp.where(jnp.abs(offset) < 2.0, pattern, 0.0))
        weights.append(jnp.concatenate(parts, axis=0) if axis < 2 else parts[0])
    return weights


def by_levels(weight_y, weight_z):
    return split(jnp.concatenate([weight_z[k : k + 1] * weight_y for k in range(CZ)], axis=0))


PIECES = (2 * BOX, 3 * BOX, 3 * BOX - 1)


def together(count, most):
    return math.gcd(count, most)


def build_kernel(
    dest_ref, base_ref, pos_ref, frc_ref, fluid_ref, out_ref, stage_ref, count_ref, wave_ref
):
    slots = out_ref.shape[0]
    blocks = pos_ref.shape[1]
    group = together(blocks, 16)

    def clear(t, carry):
        count_ref[t] = 0
        stage_ref[t, 0:8, :] = jnp.zeros((8, 128), F32)
        return carry

    lax.fori_loop(0, slots, clear, 0, unroll=4)
    lane = iota((8, 128), 1)
    top = iota((8, 128), 0) == 0

    def one(first, n):
        block = first + n
        weight_x, weight_y, weight_z = box_weights(wave_ref, n)
        loaded = [frc_ref[c, pl.ds(block, 1), :] * weight_x for c in range(3)]
        high, low = split(jnp.concatenate(loaded, axis=0))
        right = jnp.concatenate(by_levels(weight_y, weight_z), axis=0)
        dims = (((1,), (1,)), ((), ()))
        box = lax.dot_general(high, right, dims, preferred_element_type=F32)
        box = box + lax.dot_general(low, right, dims, preferred_element_type=F32)
        box = box + pltpu.roll(box, HALF, 1)
        base_x = base_ref[0, block].astype(F32) + 1.0
        base_y = base_ref[1, block].astype(F32)
        tiles = [box[8 * n : 8 * n + 8] for n in range(6)]
        rounded = [tile.astype(BF16).astype(F32) for tile in tiles]
        sums = [rounded[2 * c] + rounded[2 * c + 1] for c in range(3)]
        tiles[0] = jnp.where(top & (lane % HALF == 0), base_x, tiles[0])
        tiles[0] = jnp.where(top & (lane % HALF == BOX), base_y, tiles[0])
        return tiles, sums

    def several(step, carry):
        results = []
        waves(pos_ref, step * group, group, wave_ref)
        for n in range(group):
            tiles, sums = one(step * group, n)
            results.append(tiles)
            carry = tuple(a + b for a, b in zip(carry, sums))
        for n in range(group):
            target = dest_ref[0, step * group + n]
            order = count_ref[target]
            count_ref[target] = order + 1
            mine = lane // HALF == order
            for m in range(6):
                rows = slice(8 * m, 8 * m + 8)
                stage_ref[target, rows, :] = jnp.where(
                    mine, results[n][m], stage_ref[target, rows, :]
                )
        return carry

    fluid = []
    for c in range(3):
        column = fluid_ref[0, c] + fluid_ref[1, c] + (fluid_ref[2, c] + fluid_ref[3, c])
        fluid.append(jnp.sum(column.reshape(16, 8, 128), axis=0))
    zero = jnp.zeros((8, 128), F32)
    boxes = lax.fori_loop(0, blocks // group, several, (zero, zero, zero))
    fluid = [a + 0.5 * b for a, b in zip(fluid, boxes)]
    pieces = []
    for c in range(3):
        rest = jnp.broadcast_to(jnp.sum(fluid[c], axis=(0, 1), keepdims=True), (8, 128))
        marked = jnp.zeros((8, 128), F32)
        for place_of in PIECES:
            part = rest.astype(BF16).astype(F32)
            marked = jnp.where(lane == place_of, part, marked)
            rest = rest - part
        pieces.append(marked)
    held = top & ((lane == PIECES[0]) | (lane == PIECES[1]) | (lane == PIECES[2]))

    def finish(t, carry):
        tiles = []
        for c in range(3):
            row = BOX * c
            tiles.append(jnp.where(held, pieces[c], stage_ref[t, row : row + 8, :]))
            tiles.append(stage_ref[t, row + 8 : row + BOX, :])
        out_ref[t] = jnp.concatenate(tiles, axis=0).astype(BF16)
        return carry

    lax.fori_loop(0, slots, finish, 0, unroll=4)


def build(dest, base, positions, forces, fluid, slots):
    return call(
        build_kernel,
        shaped((slots, ROWS, 128), BF16),
        [SMEM, SMEM, VMEM, VMEM, VMEM],
        [
            pltpu.VMEM((slots, ROWS, 128), F32),
            pltpu.SMEM((slots,), jnp.int32),
            pltpu.VMEM((9, together(positions.shape[1], 16), 256), F32),
        ],
    )(*map(far, (dest, base, positions, forces, fluid)))


def flat_ring(x):
    rows = x.shape[-2]
    ax = x.ndim - 2
    return (
        pltpu.roll(x, 1, ax)
        + pltpu.roll(x, rows - 1, ax)
        + (pltpu.roll(x, 1, ax + 1) + pltpu.roll(x, 127, ax + 1))
    )


def group_ring(x):
    rows = x.shape[-2]
    ax = x.ndim - 2
    lane = iota(x.shape, ax + 1) & 31
    before = jnp.where(lane == 0, pltpu.roll(x, 97, ax + 1), pltpu.roll(x, 1, ax + 1))
    after = jnp.where(lane == 31, pltpu.roll(x, 31, ax + 1), pltpu.roll(x, 127, ax + 1))
    return pltpu.roll(x, 1, ax) + pltpu.roll(x, rows - 1, ax) + (before + after)


def start_of(b, below, above, ring, index):
    q, _, w = level(index)
    return w * ((4.0 / 3.0) * b + (w * q) * (ring(b) + (below + above)))


def left_of(b, u, below, above, ring, index):
    q, diag, _ = level(index)
    return b - diag * u + q * (ring(u) + (below + above))


def sweep_of(b, u, below, above, ring, index):
    q, _, w = level(index)
    return (1.0 - RELAX) * u + (w * b + (w * q) * (ring(u) + (below + above)))


def dot(left, right):
    return lax.dot_general(
        left, right, (((1,), (0,)), ((), ())), precision=HIGH, preferred_element_type=F32
    )


def lanes(test):
    return test(iota((128, 128), 0), iota((128, 128), 1))


def place_kernel(
    meta_ref, pay_ref, fluid_ref,
    src_ref, up_ref, down_ref, up2_ref, down2_ref, lift_ref,
    grid_ref, u_ref, sum_ref,
):
    slots = pay_ref.shape[0]
    lane = iota((8, 128), 1)
    sub = iota((8, 128), 0)
    for z in range(CZ):
        for c in range(3):
            grid_ref[3 * z + c, 0:128, :] = fluid_ref[z, c]
            grid_ref[3 * z + c, 128:144, :] = jnp.zeros((16, 128), F32)

    def turned(tile, order, head, base_y):
        base_x = jnp.maximum(head - 1, 0)
        shift = base_x & 7
        row = pl.multiple_of(base_x - shift, 8)
        window = (lane - base_y) & 127
        inside = (window >= 1) & (window <= BOX - 2) & (head > 0)
        late = inside & (sub >= shift)
        early = inside & (sub < shift)
        pieces = [pltpu.roll(tile[8 * n : 8 * n + 8], shift, 0) for n in range(6)]
        values = []
        for k in range(CZ):
            step = (base_y - HALF * order - BOX * k) & 127
            values.append([pltpu.roll(piece, step, 1) for piece in pieces])
        return row, late, early, values

    def add(row, late, early, values):
        for k in range(CZ):
            for c in range(3):
                first, second = values[k][2 * c], values[k][2 * c + 1]
                kc = 3 * k + c
                grid_ref[kc, pl.ds(row, 8), :] += jnp.where(late, first, 0.0)
                grid_ref[kc, pl.ds(row + 8, 8), :] += jnp.where(
                    early, first, jnp.where(late, second, 0.0)
                )
                grid_ref[kc, pl.ds(row + 16, 8), :] += jnp.where(early, second, 0.0)

    group = together(slots, 8)

    def several(step, carry):
        found = []
        for n in range(group):
            d = step * group + n
            tile = pay_ref[d].astype(F32)
            carry = tuple(
                carry[c] + jnp.where(held, tile[BOX * c : BOX * c + 8], 0.0) for c in range(3)
            )
            for order in range(2):
                at = 8 * d + 4 * order
                found.append(turned(tile, order, meta_ref[at], meta_ref[at + 1]))
        for one in found:
            add(*one)
        return carry

    held = (sub == 0) & ((lane == PIECES[0]) | (lane == PIECES[1]) | (lane == PIECES[2]))
    zero = jnp.zeros((8, 128), F32)
    totals = lax.fori_loop(0, slots // group, several, (zero, zero, zero))
    factor = (1.0 - level(3)[2] * SCREEN) ** 6 / SCREEN
    for index in range(3):
        factor = factor * (1.0 - level(index)[2] * SCREEN) ** 2
    scale = factor / (slots * CZ * 128.0 * 128.0)
    lift_ref[...] = zero
    for c in range(3):
        total = jnp.sum(totals[c], axis=(0, 1), keepdims=True)
        lift_ref[c : c + 1, :] = jnp.broadcast_to(total * scale, (1, 128))
    pool = [
        jnp.where(lanes(lambda r, l: (r // 2 == (l & 63)) & (l // 64 == half)), 0.125, 0.0)
        for half in range(2)
    ]
    q, _, w = level(0)
    spill_up, spill_down = [], []
    for c in range(3):
        for z in range(CZ):
            kc = 3 * z + c
            grid_ref[kc, 0:16, :] += grid_ref[kc, 128:144, :]
            src_ref[z, c] = grid_ref[kc, 0:128, :]

        def b_at(z):
            return src_ref[z, c] if 0 <= z < CZ else 0.0

        for z in range(CZ):
            u_ref[z + 1] = start_of(src_ref[z, c], b_at(z - 1), b_at(z + 1), flat_ring, 0)
        u_ref[0] = (w * w * q) * src_ref[0, c]
        u_ref[CZ + 1] = (w * w * q) * src_ref[CZ - 1, c]

        def left(z):
            if z == -2:
                return q * u_ref[0]
            if z == CZ + 1:
                return q * u_ref[CZ + 1]
            below = u_ref[z] if z > -1 else 0.0
            above = u_ref[z + 2] if z < CZ else 0.0
            return left_of(b_at(z), u_ref[z + 1], below, above, flat_ring, 0)

        rows = []
        for pair in range(-1, 3):
            sum_ref[...] = left(2 * pair) + left(2 * pair + 1)
            rows.append(sum_ref[pl.ds(0, 64, 2), :] + sum_ref[pl.ds(1, 64, 2), :])
        own = dot(rows[1], pool[0]) + dot(rows[2], pool[1])
        up_ref[c] = own
        down_ref[c] = own
        spill_down.append(dot(rows[0], pool[c % 2]))
        spill_up.append(dot(rows[3], pool[c % 2]))
    for ref, far_ref, spill in ((up_ref, up2_ref, spill_up), (down_ref, down2_ref, spill_down)):
        both = spill[0] + spill[1]
        ref[3] = both
        ref[4] = spill[2]
        far_ref[0] = both
        far_ref[1] = spill[2]


def place(meta, payload, fluid):
    return call(
        place_kernel,
        (
            shaped(fluid.shape, F32),
            shaped((5, 64, 128), F32),
            shaped((5, 64, 128), F32),
            shaped((2, 64, 128), F32),
            shaped((2, 64, 128), F32),
            shaped((8, 128), F32),
        ),
        [SMEM, VMEM, VMEM],
        [
            pltpu.VMEM((12, 144, 128), F32),
            pltpu.VMEM((CZ + 2, 128, 128), F32),
            pltpu.VMEM((128, 128), F32),
        ],
    )(meta, near(payload), near(fluid))


def both_layers(tile):
    lane = iota(tile.shape, tile.ndim - 1)
    turned = pltpu.roll(tile, 64, tile.ndim - 1)
    return jnp.where(lane < 64, tile, turned), jnp.where(lane < 64, turned, tile)


def pack_coarse(value):
    last = value[24:32]
    lane = iota((8, 128), 1)
    return [
        jnp.where(lane < 96, value[8 * c : 8 * c + 8], pltpu.roll(last, 96 - 32 * c, 1))
        for c in range(3)
    ]


def unpack_coarse(tile):
    lane = iota((8, 128), 1)
    last = jnp.zeros((8, 128), F32)
    rows = []
    for c in range(3):
        piece = tile[8 * c : 8 * c + 8]
        turned = pltpu.roll(piece, (32 * c - 96) % 128, 1)
        last = jnp.where(lane // 32 == c, turned, last)
        rows.append(jnp.where(lane < 96, piece, 0.0))
    return jnp.concatenate(rows + [last], axis=0)


def spilled(ref, c, first=0):
    return both_layers(ref[first + c // 2])[c % 2]


U_ROW = 12 * 128


def middle_kernel(
    src_ref, up_ref, down_ref, m1_ref, p1_ref, m2_ref, p2_ref,
    pairs_ref, out_ref, rise_ref, sink_ref, sum_ref,
):
    total = None
    for ref, order in ((rise_ref, (3, 2, 1)), (sink_ref, (0, 1, 2))):
        for c in range(3):
            parts = split(src_ref[order[0], c])
            parts += tuple(src_ref[z, c].astype(BF16) for z in order[1:])
            for n in range(4):
                ref[128 * (3 * n + c) : 128 * (3 * n + c + 1), :] = parts[n]
    lane = iota((64, 128), 1)
    for c in range(3):
        m1, own, p1 = both_layers(m1_ref[c]), both_layers(up_ref[c]), both_layers(p1_ref[c])
        b = [
            m1[0] + spilled(m2_ref, c),
            m1[1] + spilled(down_ref, c, 3),
            own[0] + spilled(m1_ref, c, 3),
            own[1] + spilled(p1_ref, c, 3),
            p1[0] + spilled(up_ref, c, 3),
            p1[1] + spilled(p2_ref, c),
        ]
        for j in range(3):
            pairs_ref[j, c] = jnp.where(lane < 64, b[2 * j], b[2 * j + 1])
        u = [start_of(b[i], b[i - 1], b[i + 1], flat_ring, 1) for i in range(1, 5)]
        rows = slice(U_ROW + 64 * c, U_ROW + 64 * c + 64)
        rise_ref[rows, :] = jnp.where(lane < 64, u[0], u[1]).astype(BF16)
        sink_ref[rows, :] = jnp.where(lane < 64, u[2], u[3]).astype(BF16)
        left = [left_of(b[i + 1], u[i], u[i - 1], u[i + 1], flat_ring, 1) for i in (1, 2)]
        sum_ref[...] = left[0] + left[1]
        rows = sum_ref[pl.ds(0, 32, 2), :] + sum_ref[pl.ds(1, 32, 2), :]
        pool = jnp.where(
            lanes(lambda r, l: (r // 2 == (l & 31)) & (l // 32 == c) & (r < 64)), 0.125, 0.0
        )
        part = dot(rows, pool)
        total = part if total is None else total + part
    packed = jnp.concatenate(pack_coarse(total), axis=0)
    for d in range(out_ref.shape[0]):
        out_ref[d] = packed


def middle_down(source, up, down, m1, p1, m2, p2):
    return call(
        middle_kernel,
        (
            shaped((3, 3, 64, 128), F32),
            shaped((LOCAL, 24, 128), F32),
            shaped((U_ROW + 192, 128), BF16),
            shaped((U_ROW + 192, 128), BF16),
        ),
        None,
        [pltpu.VMEM((64, 128), F32)],
    )(*map(near, (source, up, down, m1, p1, m2, p2)))


def inner(x):
    return x[1:-1]


def coarse_part(me, blocks, lift_ref, window_ref, pool_ref, final_ref):
    parity = me % 2
    first = me % LOCAL - parity
    for n, ref in enumerate(blocks):
        window_ref[LOCAL * n : LOCAL * n + LOCAL] = ref[...]
    b2 = jnp.stack([unpack_coarse(window_ref[first + t]) for t in range(34)])
    group = iota((1, 128), 1) // 32
    lift = jnp.zeros((1, 128), F32)
    for c in range(3):
        lift = jnp.where(group == c, lift_ref[c : c + 1, :], lift)
    _, _, w3 = level(3)
    u2 = start_of(inner(b2), b2[:-2], b2[2:], group_ring, 2)
    r2 = left_of(b2[2:-2], inner(u2), u2[:-2], u2[2:], group_ring, 2)
    pairs = r2.reshape(15, 2, 32, 128)
    pool_ref[...] = (pairs[:, 0] + pairs[:, 1]).reshape(480, 128)
    rows = pool_ref[pl.ds(0, 240, 2), :] + pool_ref[pl.ds(1, 240, 2), :]
    pool = jnp.where(
        lanes(lambda r, l: ((r & 31) // 2 == (l & 15)) & (r // 32 == l // 32)), 0.125, 0.0
    )
    b3 = dot(rows, pool).reshape(15, 16, 128)
    u3 = w3 * b3
    for _ in range(5):
        b3 = inner(b3)
        u3 = sweep_of(b3, inner(u3), u3[:-2], u3[2:], group_ring, 3)
    u3 = (u3 + lift[None]).reshape(80, 128)
    spread = jnp.where(
        lanes(lambda r, l: ((l & 31) // 2 == (r & 31)) & (r // 32 == l // 32)), 1.0, 0.0
    )
    wide = dot(u3, spread)
    pool_ref[pl.ds(0, 80, 2), :] = wide
    pool_ref[pl.ds(1, 80, 2), :] = wide
    lifted = pool_ref[0:160, :].reshape(5, 1, 32, 128)
    u = (u2[11:21].reshape(5, 2, 32, 128) + lifted).reshape(10, 32, 128)
    u = sweep_of(b2[13:21], inner(u), u[:-2], u[2:], group_ring, 2)
    u = sweep_of(b2[14:20], inner(u), u[:-2], u[2:], group_ring, 2)
    final_ref[...] = u
    return jnp.concatenate([final_ref[parity + h] for h in range(5)], axis=0)


def up_kernel(
    me_ref, meta_ref, lift_ref, g0_ref, g1_ref, g2_ref,
    pairs_ref, low_ref, own_ref, high_ref, vel_ref, pay_ref,
    window_ref, pool_ref, final_ref, lift1_ref, b1_ref, u1_ref, v1_ref, lift0_ref, u0_ref,
    v0_ref, ext_ref, halo_ref,
):
    blocks = (g0_ref, g1_ref, g2_ref)
    coarse = coarse_part(me_ref[0], blocks, lift_ref, window_ref, pool_ref, final_ref)
    for c in range(3):
        spread = jnp.where(lanes(lambda r, l: r == 32 * c + (l & 63) // 2), 1.0, 0.0)
        wide = dot(coarse, spread)
        lift1_ref[c, pl.ds(0, 160, 2), :] = wide
        lift1_ref[c, pl.ds(1, 160, 2), :] = wide
    spread0 = jnp.where(lanes(lambda r, l: r == l // 2), 1.0, 0.0)

    def b_at(z, c):
        if 0 <= z < CZ:
            return own_ref[z, c]
        return halo_ref[z + 3 if z < 0 else z - 1]

    def component(c, carry):
        for ref, order in ((low_ref, (2, 1, 0)), (high_ref, (3, 4, 5))):
            planes = [
                ref[pl.ds(pl.multiple_of(128 * (3 * n + c), 128), 128), :].astype(F32)
                for n in range(4)
            ]
            halo_ref[order[0]] = planes[0] + planes[1]
            halo_ref[order[1]] = planes[2]
            halo_ref[order[2]] = planes[3]
        for j in range(3):
            b1_ref[2 * j], b1_ref[2 * j + 1] = both_layers(pairs_ref[j, c])
        rows = pl.ds(pl.multiple_of(U_ROW + 64 * c, 64), 64)
        u1 = list(both_layers(low_ref[rows, :].astype(F32)))
        for i in range(1, 5):
            u1.append(start_of(b1_ref[i], b1_ref[i - 1], b1_ref[i + 1], flat_ring, 1))
        u1.extend(both_layers(high_ref[rows, :].astype(F32)))
        for z in range(-3, 5):
            h = z // 2 + 2
            u1_ref[z + 3] = u1[z + 3] + lift1_ref[c, 64 * h : 64 * h + 64, :]
        for z in range(-2, 4):
            i = z + 3
            v1_ref[z + 2] = sweep_of(
                b1_ref[z + 2], u1_ref[i], u1_ref[i - 1], u1_ref[i + 1], flat_ring, 1
            )
        for z in range(-1, 3):
            i = z + 2
            value = sweep_of(
                b1_ref[z + 2], v1_ref[i], v1_ref[i - 1], v1_ref[i + 1], flat_ring, 1
            )
            wide = dot(value, spread0)
            lift0_ref[z + 1, pl.ds(0, 64, 2), :] = wide
            lift0_ref[z + 1, pl.ds(1, 64, 2), :] = wide
        for z in range(-2, 6):
            u0_ref[z + 2] = (
                start_of(b_at(z, c), b_at(z - 1, c), b_at(z + 1, c), flat_ring, 0)
                + lift0_ref[z // 2 + 1]
            )
        for z in range(-1, 5):
            i = z + 2
            v0_ref[z + 1] = sweep_of(
                b_at(z, c), u0_ref[i], u0_ref[i - 1], u0_ref[i + 1], flat_ring, 0
            )
        for z in range(CZ):
            i = z + 1
            value = sweep_of(
                own_ref[z, c], v0_ref[i], v0_ref[i - 1], v0_ref[i + 1], flat_ring, 0
            )
            vel_ref[z, c] = value
            rounded = value.astype(BF16).astype(F32)
            ext_ref[3 * z + c, 0:128, :] = rounded
            ext_ref[3 * z + c, 128:144, :] = rounded[0:16]
        return carry

    lax.fori_loop(0, 3, component, 0)
    lane = iota((8, 128), 1)
    sub = iota((8, 128), 0)

    part = [(lane // BOX) % CZ == k for k in range(CZ)]

    def gather(order, head, base_y):
        base_x = jnp.maximum(head - 1, 0)
        shift = base_x & 7
        row = pl.multiple_of(base_x - shift, 8)
        late = sub >= shift
        values = []
        for k in range(CZ):
            step = (HALF * order + BOX * k - base_y) & 127
            line = []
            for c in range(3):
                tiles = [ext_ref[3 * k + c, pl.ds(row + 8 * n, 8), :] for n in range(3)]
                for n in range(2):
                    value = jnp.where(late, tiles[n], tiles[n + 1])
                    line.append(pltpu.roll(value, step, 1))
            values.append(line)
        return (8 - shift) & 7, values

    group = together(pay_ref.shape[0], 8)

    def several(step, carry):
        found = []
        for n in range(group):
            for order in range(2):
                at = 8 * (step * group + n) + 4 * order
                found.append(gather(order, meta_ref[at], meta_ref[at + 1]))
        for n in range(group):
            pieces = []
            for m in range(6):
                both = []
                for order in range(2):
                    back, values = found[2 * n + order]
                    packed = values[0][m]
                    for k in range(1, CZ):
                        packed = jnp.where(part[k], values[k][m], packed)
                    both.append(pltpu.roll(packed, back, 0))
                pieces.append(jnp.where(lane < HALF, both[0], both[1]))
            pay_ref[step * group + n] = jnp.concatenate(pieces, axis=0).astype(BF16)
        return carry

    lax.fori_loop(0, pay_ref.shape[0] // group, several, 0)


def way_up(me, meta, lift, blocks, pairs, low, own, high, slots):
    return call(
        up_kernel,
        (
            shaped(own.shape, F32, False),
            shaped((slots, ROWS, 128), BF16),
        ),
        [SMEM, SMEM] + [VMEM] * 8,
        [
            pltpu.VMEM((3 * LOCAL, 24, 128), F32),
            pltpu.VMEM((480, 128), F32),
            pltpu.VMEM((6, 32, 128), F32),
            pltpu.VMEM((3, 320, 128), F32),
            pltpu.VMEM((6, 64, 128), F32),
            pltpu.VMEM((8, 64, 128), F32),
            pltpu.VMEM((6, 64, 128), F32),
            pltpu.VMEM((4, 128, 128), F32),
            pltpu.VMEM((8, 128, 128), F32),
            pltpu.VMEM((6, 128, 128), F32),
            pltpu.VMEM((12, 144, 128), F32),
            pltpu.VMEM((6, 128, 128), F32),
        ],
    )(me, meta, *map(near, (lift, *blocks, pairs, low, own, high)))


def read_kernel(dest_ref, pay_ref, pos_ref, out_ref, stage_ref, count_ref, wave_ref):
    slots = pay_ref.shape[0]

    def widen(t, carry):
        count_ref[t] = 0
        stage_ref[t] = pay_ref[t].astype(F32)
        return carry

    lax.fori_loop(0, slots, widen, 0, unroll=4)
    lane = iota((8, 128), 1)

    group = together(pos_ref.shape[1], 16)

    def one(first, n, target, order):
        block = first + n
        weight_x, weight_y, weight_z = box_weights(wave_ref, n)
        mine = lane // HALF == order
        left = []
        for m in range(6):
            packed = stage_ref[target, 8 * m : 8 * m + 8, :]
            left.append(jnp.where(mine, packed, pltpu.roll(packed, HALF, 1)))
        left = jnp.concatenate(left, axis=0).astype(BF16)
        right = jnp.concatenate(by_levels(weight_y, weight_z), axis=0)
        spread = lax.dot_general(
            left, right, (((1,), (0,)), ((), ())), preferred_element_type=F32
        )
        for c in range(3):
            value = spread[BOX * c : BOX * c + BOX] * weight_x
            out_ref[c, pl.ds(block, 1), :] = jnp.sum(value, axis=0, keepdims=True)

    def several(step, carry):
        places = []
        for n in range(group):
            target = dest_ref[0, step * group + n]
            order = count_ref[target]
            count_ref[target] = order + 1
            places.append((target, order))
        waves(pos_ref, step * group, group, wave_ref)
        for n in range(group):
            one(step * group, n, *places[n])
        return carry

    lax.fori_loop(0, pos_ref.shape[1] // group, several, 0)


def read(dest, payload, positions):
    slots = payload.shape[0]
    return call(
        read_kernel,
        shaped(positions.shape, F32, False),
        [SMEM, VMEM, VMEM],
        [
            pltpu.VMEM((slots, ROWS, 128), F32),
            pltpu.SMEM((slots,), jnp.int32),
            pltpu.VMEM((9, together(positions.shape[1], 16), 256), F32),
        ],
    )(far(dest), near(payload), near(positions))


def moved(value, step):
    size = lax.axis_size(AX)
    return lax.ppermute(value, AX, [(i, (i + step) % size) for i in range(size)])


def exchanged(value, axes=AX):
    return lax.all_to_all(value, axes, split_axis=0, concat_axis=0, tiled=True)


def shards(marker_positions, marker_forces, dest_slab, base_cells, fluid_source):
    slots = lax.axis_size(AX)
    positions = marker_positions.transpose(1, 0, 2)
    forces = marker_forces.transpose(1, 0, 2)
    dest = dest_slab.T
    me = lax.axis_index(AX).astype(jnp.int32).reshape(1)
    payload = exchanged(build(dest, base_cells.T, positions, forces, fluid_source, slots))
    meta = payload[:, 0:1, ::BOX].astype(jnp.int32).reshape(8 * slots)
    source, up, down, up2, down2, lift = place(meta, payload, fluid_source)
    m1, m2 = moved(up, 1), moved(up2, 2)
    p1, p2 = moved(down, -1), moved(down2, -2)
    pairs, share, rise, sink = middle_down(source, up, down, m1, p1, m2, p2)
    middle = exchanged(share, AX[1])
    low, high = moved(rise, 1), moved(sink, -1)
    blocks = [middle if n == 0 else moved(middle, -LOCAL * n) for n in range(-1, 2)]
    velocity, picked = way_up(me, meta, lift, blocks, pairs, low, source, high, slots)
    out = read(dest, exchanged(picked), positions)
    return velocity, out.transpose(1, 0, 2)


def solution(mesh):
    torus = Mesh(mesh.devices.reshape(-1, LOCAL), AX)
    return jax.shard_map(
        shards,
        mesh=torus,
        in_specs=(P(AX), P(AX), P(AX), P(AX), P(AX)),
        out_specs=(P(AX), P(AX)),
        check_vma=False,
    )
```

```python
import math

import jax
import jax.numpy as jnp
from jax import lax
from jax.experimental import pallas as pl
from jax.experimental.pallas import tpu as pltpu
from jax.sharding import Mesh
from jax.sharding import PartitionSpec as P

AX = ("hi", "lo")
LOCAL = 8
BOX = 16
CZ = 4
HALF = CZ * BOX
ROWS = 3 * BOX
SCREEN = 1.0 / 64.0
RELAX = 2.0 / 3.0
INTERPRET = False
F32 = jnp.float32
BF16 = jnp.bfloat16
HIGH = lax.Precision.HIGHEST


def level(index):
    q = 0.25**index
    return q, SCREEN + 6.0 * q, RELAX / (SCREEN + 6.0 * q)


def call(body, out_shape, in_specs=None, scratch=(), megabytes=24):
    options = {} if in_specs is None else {"in_specs": in_specs}
    return pl.pallas_call(
        body,
        out_shape=out_shape,
        scratch_shapes=list(scratch),
        interpret=INTERPRET,
        compiler_params=pltpu.CompilerParams(vmem_limit_bytes=megabytes << 20),
        **options,
    )


def shaped(shape, dtype, near=True):
    if near and not INTERPRET:
        return pltpu.VMEM(shape, dtype)
    return jax.ShapeDtypeStruct(shape, dtype)


def near(value):
    return value if INTERPRET else pltpu.with_memory_space_constraint(value, pltpu.VMEM)


VMEM = pl.BlockSpec(memory_space=pltpu.VMEM)
SMEM = pl.BlockSpec(memory_space=pltpu.SMEM)


def far(value):
    return value if INTERPRET else pltpu.with_memory_space_constraint(value, pltpu.HBM)


def iota(shape, dim):
    return lax.broadcasted_iota(jnp.int32, shape, dim)


COS = (
    0.9999999999524891,
    -1.2337005406331254,
    0.2536692036544627,
    -0.02086006949632079,
    0.0009036280586426939,
)
SIN = (
    1.5707963267880989,
    -0.6459640961467292,
    0.07969258272440714,
    -0.004681266248964948,
    0.00015820628792786513,
)


def polynomial(coefficients, x):
    value = x * coefficients[-1] + coefficients[-2]
    for coefficient in coefficients[-3::-1]:
        value = value * x + coefficient
    return value


def split(value):
    high = value.astype(BF16)
    return high, (value - high.astype(F32)).astype(BF16)


def waves(pos_ref, first, group, wave_ref):
    rows = pl.ds(pl.multiple_of(first, group), group)
    for axis in range(3):
        point = pos_ref[axis, rows, :]
        point = 2.0 + (BOX - 5) * point if axis < 2 else (CZ - 1) * point
        nearest = jnp.floor(point + 0.5)
        rest = point - nearest
        square = rest * rest
        even = polynomial(COS, square)
        odd = polynomial(SIN, square) * rest
        quarter = nearest.astype(jnp.int32) & 3
        swap = (quarter & 1) == 1
        cosine = jnp.where(swap, odd, even)
        sine = jnp.where(swap, even, odd)
        wave_ref[3 * axis] = point
        wave_ref[3 * axis + 1] = jnp.where((quarter == 1) | (quarter == 2), -cosine, cosine)
        wave_ref[3 * axis + 2] = jnp.where(quarter >= 2, -sine, sine)


def box_weights(wave_ref, block):
    row = slice(block, block + 1)
    cell = iota((8, 256), 0)
    sign = jnp.where(cell % 4 < 2, 0.25, -0.25)
    weights = []
    for axis in range(3):
        point, cosine, sine = (wave_ref[3 * axis + n, row, :] for n in range(3))
        pattern = jnp.where(cell % 2 == 0, cosine, sine) * sign + 0.25
        parts = []
        for first in range(0, BOX if axis < 2 else 8, 8):
            offset = point - (cell + first).astype(F32)
            parts.append(jnp.where(jnp.abs(offset) < 2.0, pattern, 0.0))
        weights.append(jnp.concatenate(parts, axis=0) if axis < 2 else parts[0])
    return weights


def by_levels(weight_y, weight_z):
    return split(jnp.concatenate([weight_z[k : k + 1] * weight_y for k in range(CZ)], axis=0))


PIECES = (2 * BOX, 3 * BOX, 3 * BOX - 1)


def together(count, most):
    return math.gcd(count, most)


def build_kernel(
    dest_ref, base_ref, pos_ref, frc_ref, fluid_ref, out_ref, stage_ref, count_ref, wave_ref
):
    slots = out_ref.shape[0]
    blocks = pos_ref.shape[1]
    group = together(blocks, 16)

    def clear(t, carry):
        count_ref[t] = 0
        stage_ref[t, 0:8, :] = jnp.zeros((8, 128), F32)
        return carry

    lax.fori_loop(0, slots, clear, 0, unroll=4)
    lane = iota((8, 128), 1)
    top = iota((8, 128), 0) == 0

    def one(first, n):
        block = first + n
        weight_x, weight_y, weight_z = box_weights(wave_ref, n)
        loaded = [frc_ref[c, pl.ds(block, 1), :] * weight_x for c in range(3)]
        high, low = split(jnp.concatenate(loaded, axis=0))
        right = jnp.concatenate(by_levels(weight_y, weight_z), axis=0)
        dims = (((1,), (1,)), ((), ()))
        box = lax.dot_general(high, right, dims, preferred_element_type=F32)
        box = box + lax.dot_general(low, right, dims, preferred_element_type=F32)
        box = box + pltpu.roll(box, HALF, 1)
        base_x = base_ref[0, block].astype(F32) + 1.0
        base_y = base_ref[1, block].astype(F32)
        tiles = [box[8 * n : 8 * n + 8] for n in range(6)]
        rounded = [tile.astype(BF16).astype(F32) for tile in tiles]
        sums = [rounded[2 * c] + rounded[2 * c + 1] for c in range(3)]
        tiles[0] = jnp.where(top & (lane % HALF == 0), base_x, tiles[0])
        tiles[0] = jnp.where(top & (lane % HALF == BOX), base_y, tiles[0])
        return tiles, sums

    def several(step, carry):
        results = []
        waves(pos_ref, step * group, group, wave_ref)
        for n in range(group):
            tiles, sums = one(step * group, n)
            results.append(tiles)
            carry = tuple(a + b for a, b in zip(carry, sums))
        for n in range(group):
            target = dest_ref[0, step * group + n]
            order = count_ref[target]
            count_ref[target] = order + 1
            mine = lane // HALF == order
            for m in range(6):
                rows = slice(8 * m, 8 * m + 8)
                stage_ref[target, rows, :] = jnp.where(
                    mine, results[n][m], stage_ref[target, rows, :]
                )
        return carry

    fluid = []
    for c in range(3):
        column = fluid_ref[0, c] + fluid_ref[1, c] + (fluid_ref[2, c] + fluid_ref[3, c])
        fluid.append(jnp.sum(column.reshape(16, 8, 128), axis=0))
    zero = jnp.zeros((8, 128), F32)
    boxes = lax.fori_loop(0, blocks // group, several, (zero, zero, zero))
    fluid = [a + 0.5 * b for a, b in zip(fluid, boxes)]
    pieces = []
    for c in range(3):
        rest = jnp.broadcast_to(jnp.sum(fluid[c], axis=(0, 1), keepdims=True), (8, 128))
        marked = jnp.zeros((8, 128), F32)
        for place_of in PIECES:
            part = rest.astype(BF16).astype(F32)
            marked = jnp.where(lane == place_of, part, marked)
            rest = rest - part
        pieces.append(marked)
    held = top & ((lane == PIECES[0]) | (lane == PIECES[1]) | (lane == PIECES[2]))

    def finish(t, carry):
        tiles = []
        for c in range(3):
            row = BOX * c
            tiles.append(jnp.where(held, pieces[c], stage_ref[t, row : row + 8, :]))
            tiles.append(stage_ref[t, row + 8 : row + BOX, :])
        out_ref[t] = jnp.concatenate(tiles, axis=0).astype(BF16)
        return carry

    lax.fori_loop(0, slots, finish, 0, unroll=4)


def build(dest, base, positions, forces, fluid, slots):
    return call(
        build_kernel,
        shaped((slots, ROWS, 128), BF16),
        [SMEM, SMEM, VMEM, VMEM, VMEM],
        [
            pltpu.VMEM((slots, ROWS, 128), F32),
            pltpu.SMEM((slots,), jnp.int32),
            pltpu.VMEM((9, together(positions.shape[1], 16), 256), F32),
        ],
    )(*map(far, (dest, base, positions, forces, fluid)))


def flat_ring(x):
    rows = x.shape[-2]
    ax = x.ndim - 2
    return (
        pltpu.roll(x, 1, ax)
        + pltpu.roll(x, rows - 1, ax)
        + (pltpu.roll(x, 1, ax + 1) + pltpu.roll(x, 127, ax + 1))
    )


def group_ring(x):
    rows = x.shape[-2]
    ax = x.ndim - 2
    lane = iota(x.shape, ax + 1) & 31
    before = jnp.where(lane == 0, pltpu.roll(x, 97, ax + 1), pltpu.roll(x, 1, ax + 1))
    after = jnp.where(lane == 31, pltpu.roll(x, 31, ax + 1), pltpu.roll(x, 127, ax + 1))
    return pltpu.roll(x, 1, ax) + pltpu.roll(x, rows - 1, ax) + (before + after)


def start_of(b, below, above, ring, index):
    q, _, w = level(index)
    return w * ((4.0 / 3.0) * b + (w * q) * (ring(b) + (below + above)))


def left_of(b, u, below, above, ring, index):
    q, diag, _ = level(index)
    return b - diag * u + q * (ring(u) + (below + above))


def sweep_of(b, u, below, above, ring, index):
    q, _, w = level(index)
    return (1.0 - RELAX) * u + (w * b + (w * q) * (ring(u) + (below + above)))


def dot(left, right):
    return lax.dot_general(
        left, right, (((1,), (0,)), ((), ())), precision=HIGH, preferred_element_type=F32
    )


def lanes(test):
    return test(iota((128, 128), 0), iota((128, 128), 1))


def place_kernel(
    meta_ref, pay_ref, fluid_ref,
    src_ref, up_ref, down_ref, up2_ref, down2_ref, lift_ref,
    grid_ref, u_ref, sum_ref,
):
    slots = pay_ref.shape[0]
    lane = iota((8, 128), 1)
    sub = iota((8, 128), 0)
    for z in range(CZ):
        for c in range(3):
            grid_ref[3 * z + c, 0:128, :] = fluid_ref[z, c]
            grid_ref[3 * z + c, 128:144, :] = jnp.zeros((16, 128), F32)

    def turned(tile, order, head, base_y):
        base_x = jnp.maximum(head - 1, 0)
        shift = base_x & 7
        row = pl.multiple_of(base_x - shift, 8)
        window = (lane - base_y) & 127
        inside = (window >= 1) & (window <= BOX - 2) & (head > 0)
        late = inside & (sub >= shift)
        early = inside & (sub < shift)
        pieces = [pltpu.roll(tile[8 * n : 8 * n + 8], shift, 0) for n in range(6)]
        values = []
        for k in range(CZ):
            step = (base_y - HALF * order - BOX * k) & 127
            values.append([pltpu.roll(piece, step, 1) for piece in pieces])
        return row, late, early, values

    def add(row, late, early, values):
        for k in range(CZ):
            for c in range(3):
                first, second = values[k][2 * c], values[k][2 * c + 1]
                kc = 3 * k + c
                grid_ref[kc, pl.ds(row, 8), :] += jnp.where(late, first, 0.0)
                grid_ref[kc, pl.ds(row + 8, 8), :] += jnp.where(
                    early, first, jnp.where(late, second, 0.0)
                )
                grid_ref[kc, pl.ds(row + 16, 8), :] += jnp.where(early, second, 0.0)

    group = together(slots, 8)

    def several(step, carry):
        found = []
        for n in range(group):
            d = step * group + n
            tile = pay_ref[d].astype(F32)
            carry = tuple(
                carry[c] + jnp.where(held, tile[BOX * c : BOX * c + 8], 0.0) for c in range(3)
            )
            for order in range(2):
                at = 8 * d + 4 * order
                found.append(turned(tile, order, meta_ref[at], meta_ref[at + 1]))
        for one in found:
            add(*one)
        return carry

    held = (sub == 0) & ((lane == PIECES[0]) | (lane == PIECES[1]) | (lane == PIECES[2]))
    zero = jnp.zeros((8, 128), F32)
    totals = lax.fori_loop(0, slots // group, several, (zero, zero, zero))
    factor = (1.0 - level(3)[2] * SCREEN) ** 6 / SCREEN
    for index in range(3):
        factor = factor * (1.0 - level(index)[2] * SCREEN) ** 2
    scale = factor / (slots * CZ * 128.0 * 128.0)
    lift_ref[...] = zero
    for c in range(3):
        total = jnp.sum(totals[c], axis=(0, 1), keepdims=True)
        lift_ref[c : c + 1, :] = jnp.broadcast_to(total * scale, (1, 128))
    pool = [
        jnp.where(lanes(lambda r, l: (r // 2 == (l & 63)) & (l // 64 == half)), 0.125, 0.0)
        for half in range(2)
    ]
    q, _, w = level(0)
    spill_up, spill_down = [], []
    for c in range(3):
        for z in range(CZ):
            kc = 3 * z + c
            grid_ref[kc, 0:16, :] += grid_ref[kc, 128:144, :]
            src_ref[z, c] = grid_ref[kc, 0:128, :]

        def b_at(z):
            return src_ref[z, c] if 0 <= z < CZ else 0.0

        for z in range(CZ):
            u_ref[z + 1] = start_of(src_ref[z, c], b_at(z - 1), b_at(z + 1), flat_ring, 0)
        u_ref[0] = (w * w * q) * src_ref[0, c]
        u_ref[CZ + 1] = (w * w * q) * src_ref[CZ - 1, c]

        def left(z):
            if z == -2:
                return q * u_ref[0]
            if z == CZ + 1:
                return q * u_ref[CZ + 1]
            below = u_ref[z] if z > -1 else 0.0
            above = u_ref[z + 2] if z < CZ else 0.0
            return left_of(b_at(z), u_ref[z + 1], below, above, flat_ring, 0)

        rows = []
        for pair in range(-1, 3):
            sum_ref[...] = left(2 * pair) + left(2 * pair + 1)
            rows.append(sum_ref[pl.ds(0, 64, 2), :] + sum_ref[pl.ds(1, 64, 2), :])
        own = dot(rows[1], pool[0]) + dot(rows[2], pool[1])
        up_ref[c] = own
        down_ref[c] = own
        spill_down.append(dot(rows[0], pool[c % 2]))
        spill_up.append(dot(rows[3], pool[c % 2]))
    for ref, far_ref, spill in ((up_ref, up2_ref, spill_up), (down_ref, down2_ref, spill_down)):
        both = spill[0] + spill[1]
        ref[3] = both
        ref[4] = spill[2]
        far_ref[0] = both.astype(BF16)
        far_ref[1] = spill[2].astype(BF16)


def place(meta, payload, fluid):
    return call(
        place_kernel,
        (
            shaped(fluid.shape, F32),
            shaped((5, 64, 128), F32),
            shaped((5, 64, 128), F32),
            shaped((2, 64, 128), BF16),
            shaped((2, 64, 128), BF16),
            shaped((8, 128), F32),
        ),
        [SMEM, VMEM, VMEM],
        [
            pltpu.VMEM((12, 144, 128), F32),
            pltpu.VMEM((CZ + 2, 128, 128), F32),
            pltpu.VMEM((128, 128), F32),
        ],
    )(meta, near(payload), near(fluid))


def both_layers(tile):
    lane = iota(tile.shape, tile.ndim - 1)
    turned = pltpu.roll(tile, 64, tile.ndim - 1)
    return jnp.where(lane < 64, tile, turned), jnp.where(lane < 64, turned, tile)


def pack_coarse(value):
    last = value[24:32]
    lane = iota((8, 128), 1)
    return [
        jnp.where(lane < 96, value[8 * c : 8 * c + 8], pltpu.roll(last, 96 - 32 * c, 1))
        for c in range(3)
    ]


def unpack_coarse(tile):
    lane = iota((8, 128), 1)
    last = jnp.zeros((8, 128), F32)
    rows = []
    for c in range(3):
        piece = tile[8 * c : 8 * c + 8]
        turned = pltpu.roll(piece, (32 * c - 96) % 128, 1)
        last = jnp.where(lane // 32 == c, turned, last)
        rows.append(jnp.where(lane < 96, piece, 0.0))
    return jnp.concatenate(rows + [last], axis=0)


def spilled(ref, c, first=0):
    return both_layers(ref[first + c // 2].astype(F32))[c % 2]


U_ROW = 12 * 128


def middle_kernel(
    src_ref, up_ref, down_ref, m1_ref, p1_ref, m2_ref, p2_ref,
    pairs_ref, out_ref, rise_ref, sink_ref, sum_ref,
):
    total = None
    for ref, order in ((rise_ref, (3, 2, 1)), (sink_ref, (0, 1, 2))):
        for c in range(3):
            parts = split(src_ref[order[0], c])
            parts += tuple(src_ref[z, c].astype(BF16) for z in order[1:])
            for n in range(4):
                ref[128 * (3 * n + c) : 128 * (3 * n + c + 1), :] = parts[n]
    lane = iota((64, 128), 1)
    for c in range(3):
        m1, own, p1 = both_layers(m1_ref[c]), both_layers(up_ref[c]), both_layers(p1_ref[c])
        b = [
            m1[0] + spilled(m2_ref, c),
            m1[1] + spilled(down_ref, c, 3),
            own[0] + spilled(m1_ref, c, 3),
            own[1] + spilled(p1_ref, c, 3),
            p1[0] + spilled(up_ref, c, 3),
            p1[1] + spilled(p2_ref, c),
        ]
        for j in range(3):
            pairs_ref[j, c] = jnp.where(lane < 64, b[2 * j], b[2 * j + 1])
        u = [start_of(b[i], b[i - 1], b[i + 1], flat_ring, 1) for i in range(1, 5)]
        rows = slice(U_ROW + 64 * c, U_ROW + 64 * c + 64)
        rise_ref[rows, :] = jnp.where(lane < 64, u[0], u[1]).astype(BF16)
        sink_ref[rows, :] = jnp.where(lane < 64, u[2], u[3]).astype(BF16)
        left = [left_of(b[i + 1], u[i], u[i - 1], u[i + 1], flat_ring, 1) for i in (1, 2)]
        sum_ref[...] = left[0] + left[1]
        rows = sum_ref[pl.ds(0, 32, 2), :] + sum_ref[pl.ds(1, 32, 2), :]
        pool = jnp.where(
            lanes(lambda r, l: (r // 2 == (l & 31)) & (l // 32 == c) & (r < 64)), 0.125, 0.0
        )
        part = dot(rows, pool)
        total = part if total is None else total + part
    packed = jnp.concatenate(pack_coarse(total), axis=0)
    for d in range(out_ref.shape[0]):
        out_ref[d] = packed


def middle_down(source, up, down, m1, p1, m2, p2):
    return call(
        middle_kernel,
        (
            shaped((3, 3, 64, 128), F32),
            shaped((LOCAL, 24, 128), F32),
            shaped((U_ROW + 192, 128), BF16),
            shaped((U_ROW + 192, 128), BF16),
        ),
        None,
        [pltpu.VMEM((64, 128), F32)],
    )(*map(near, (source, up, down, m1, p1, m2, p2)))


def inner(x):
    return x[1:-1]


def coarse_part(me, blocks, lift_ref, window_ref, pool_ref, final_ref):
    parity = me % 2
    first = me % LOCAL - parity
    for n, ref in enumerate(blocks):
        window_ref[LOCAL * n : LOCAL * n + LOCAL] = ref[...].astype(F32)
    b2 = jnp.stack([unpack_coarse(window_ref[first + t]) for t in range(34)])
    group = iota((1, 128), 1) // 32
    lift = jnp.zeros((1, 128), F32)
    for c in range(3):
        lift = jnp.where(group == c, lift_ref[c : c + 1, :], lift)
    _, _, w3 = level(3)
    u2 = start_of(inner(b2), b2[:-2], b2[2:], group_ring, 2)
    r2 = left_of(b2[2:-2], inner(u2), u2[:-2], u2[2:], group_ring, 2)
    pairs = r2.reshape(15, 2, 32, 128)
    pool_ref[...] = (pairs[:, 0] + pairs[:, 1]).reshape(480, 128)
    rows = pool_ref[pl.ds(0, 240, 2), :] + pool_ref[pl.ds(1, 240, 2), :]
    pool = jnp.where(
        lanes(lambda r, l: ((r & 31) // 2 == (l & 15)) & (r // 32 == l // 32)), 0.125, 0.0
    )
    b3 = dot(rows, pool).reshape(15, 16, 128)
    u3 = w3 * b3
    for _ in range(5):
        b3 = inner(b3)
        u3 = sweep_of(b3, inner(u3), u3[:-2], u3[2:], group_ring, 3)
    u3 = (u3 + lift[None]).reshape(80, 128)
    spread = jnp.where(
        lanes(lambda r, l: ((l & 31) // 2 == (r & 31)) & (r // 32 == l // 32)), 1.0, 0.0
    )
    wide = dot(u3, spread)
    pool_ref[pl.ds(0, 80, 2), :] = wide
    pool_ref[pl.ds(1, 80, 2), :] = wide
    lifted = pool_ref[0:160, :].reshape(5, 1, 32, 128)
    u = (u2[11:21].reshape(5, 2, 32, 128) + lifted).reshape(10, 32, 128)
    u = sweep_of(b2[13:21], inner(u), u[:-2], u[2:], group_ring, 2)
    u = sweep_of(b2[14:20], inner(u), u[:-2], u[2:], group_ring, 2)
    final_ref[...] = u
    return jnp.concatenate([final_ref[parity + h] for h in range(5)], axis=0)


def up_kernel(
    me_ref, meta_ref, lift_ref, g0_ref, g1_ref, g2_ref, g3_ref, g4_ref,
    pairs_ref, low_ref, own_ref, high_ref, vel_ref, pay_ref,
    window_ref, pool_ref, final_ref, lift1_ref, b1_ref, u1_ref, v1_ref, lift0_ref, u0_ref,
    v0_ref, ext_ref, halo_ref,
):
    blocks = (g0_ref, g1_ref, g2_ref, g3_ref, g4_ref)
    coarse = coarse_part(me_ref[0], blocks, lift_ref, window_ref, pool_ref, final_ref)
    for c in range(3):
        spread = jnp.where(lanes(lambda r, l: r == 32 * c + (l & 63) // 2), 1.0, 0.0)
        wide = dot(coarse, spread)
        lift1_ref[c, pl.ds(0, 160, 2), :] = wide
        lift1_ref[c, pl.ds(1, 160, 2), :] = wide
    spread0 = jnp.where(lanes(lambda r, l: r == l // 2), 1.0, 0.0)

    def b_at(z, c):
        if 0 <= z < CZ:
            return own_ref[z, c]
        return halo_ref[z + 3 if z < 0 else z - 1]

    def component(c, carry):
        for ref, order in ((low_ref, (2, 1, 0)), (high_ref, (3, 4, 5))):
            planes = [
                ref[pl.ds(pl.multiple_of(128 * (3 * n + c), 128), 128), :].astype(F32)
                for n in range(4)
            ]
            halo_ref[order[0]] = planes[0] + planes[1]
            halo_ref[order[1]] = planes[2]
            halo_ref[order[2]] = planes[3]
        for j in range(3):
            b1_ref[2 * j], b1_ref[2 * j + 1] = both_layers(pairs_ref[j, c])
        rows = pl.ds(pl.multiple_of(U_ROW + 64 * c, 64), 64)
        u1 = list(both_layers(low_ref[rows, :].astype(F32)))
        for i in range(1, 5):
            u1.append(start_of(b1_ref[i], b1_ref[i - 1], b1_ref[i + 1], flat_ring, 1))
        u1.extend(both_layers(high_ref[rows, :].astype(F32)))
        for z in range(-3, 5):
            h = z // 2 + 2
            u1_ref[z + 3] = u1[z + 3] + lift1_ref[c, 64 * h : 64 * h + 64, :]
        for z in range(-2, 4):
            i = z + 3
            v1_ref[z + 2] = sweep_of(
                b1_ref[z + 2], u1_ref[i], u1_ref[i - 1], u1_ref[i + 1], flat_ring, 1
            )
        for z in range(-1, 3):
            i = z + 2
            value = sweep_of(
                b1_ref[z + 2], v1_ref[i], v1_ref[i - 1], v1_ref[i + 1], flat_ring, 1
            )
            wide = dot(value, spread0)
            lift0_ref[z + 1, pl.ds(0, 64, 2), :] = wide
            lift0_ref[z + 1, pl.ds(1, 64, 2), :] = wide
        for z in range(-2, 6):
            u0_ref[z + 2] = (
                start_of(b_at(z, c), b_at(z - 1, c), b_at(z + 1, c), flat_ring, 0)
                + lift0_ref[z // 2 + 1]
            )
        for z in range(-1, 5):
            i = z + 2
            v0_ref[z + 1] = sweep_of(
                b_at(z, c), u0_ref[i], u0_ref[i - 1], u0_ref[i + 1], flat_ring, 0
            )
        for z in range(CZ):
            i = z + 1
            value = sweep_of(
                own_ref[z, c], v0_ref[i], v0_ref[i - 1], v0_ref[i + 1], flat_ring, 0
            )
            vel_ref[z, c] = value
            rounded = value.astype(BF16).astype(F32)
            ext_ref[3 * z + c, 0:128, :] = rounded
            ext_ref[3 * z + c, 128:144, :] = rounded[0:16]
        return carry

    lax.fori_loop(0, 3, component, 0)
    lane = iota((8, 128), 1)
    sub = iota((8, 128), 0)

    part = [(lane // BOX) % CZ == k for k in range(CZ)]

    def gather(order, head, base_y):
        base_x = jnp.maximum(head - 1, 0)
        shift = base_x & 7
        row = pl.multiple_of(base_x - shift, 8)
        late = sub >= shift
        values = []
        for k in range(CZ):
            step = (HALF * order + BOX * k - base_y) & 127
            line = []
            for c in range(3):
                tiles = [ext_ref[3 * k + c, pl.ds(row + 8 * n, 8), :] for n in range(3)]
                for n in range(2):
                    value = jnp.where(late, tiles[n], tiles[n + 1])
                    line.append(pltpu.roll(value, step, 1))
            values.append(line)
        return (8 - shift) & 7, values

    group = together(pay_ref.shape[0], 8)

    def several(step, carry):
        found = []
        for n in range(group):
            for order in range(2):
                at = 8 * (step * group + n) + 4 * order
                found.append(gather(order, meta_ref[at], meta_ref[at + 1]))
        for n in range(group):
            pieces = []
            for m in range(6):
                both = []
                for order in range(2):
                    back, values = found[2 * n + order]
                    packed = values[0][m]
                    for k in range(1, CZ):
                        packed = jnp.where(part[k], values[k][m], packed)
                    both.append(pltpu.roll(packed, back, 0))
                pieces.append(jnp.where(lane < HALF, both[0], both[1]))
            pay_ref[step * group + n] = jnp.concatenate(pieces, axis=0).astype(BF16)
        return carry

    lax.fori_loop(0, pay_ref.shape[0] // group, several, 0)


def way_up(me, meta, lift, blocks, pairs, low, own, high, slots):
    return call(
        up_kernel,
        (
            shaped(own.shape, F32, False),
            shaped((slots, ROWS, 128), BF16),
        ),
        [SMEM, SMEM] + [VMEM] * 10,
        [
            pltpu.VMEM((5 * LOCAL, 24, 128), F32),
            pltpu.VMEM((480, 128), F32),
            pltpu.VMEM((6, 32, 128), F32),
            pltpu.VMEM((3, 320, 128), F32),
            pltpu.VMEM((6, 64, 128), F32),
            pltpu.VMEM((8, 64, 128), F32),
            pltpu.VMEM((6, 64, 128), F32),
            pltpu.VMEM((4, 128, 128), F32),
            pltpu.VMEM((8, 128, 128), F32),
            pltpu.VMEM((6, 128, 128), F32),
            pltpu.VMEM((12, 144, 128), F32),
            pltpu.VMEM((6, 128, 128), F32),
        ],
    )(me, meta, *map(near, (lift, *blocks, pairs, low, own, high)))


def read_kernel(dest_ref, pay_ref, pos_ref, out_ref, stage_ref, count_ref, wave_ref):
    slots = pay_ref.shape[0]

    def widen(t, carry):
        count_ref[t] = 0
        stage_ref[t] = pay_ref[t].astype(F32)
        return carry

    lax.fori_loop(0, slots, widen, 0, unroll=4)
    lane = iota((8, 128), 1)

    group = together(pos_ref.shape[1], 16)

    def one(first, n, target, order):
        block = first + n
        weight_x, weight_y, weight_z = box_weights(wave_ref, n)
        mine = lane // HALF == order
        left = []
        for m in range(6):
            packed = stage_ref[target, 8 * m : 8 * m + 8, :]
            left.append(jnp.where(mine, packed, pltpu.roll(packed, HALF, 1)))
        left = jnp.concatenate(left, axis=0).astype(BF16)
        right = jnp.concatenate(by_levels(weight_y, weight_z), axis=0)
        spread = lax.dot_general(
            left, right, (((1,), (0,)), ((), ())), preferred_element_type=F32
        )
        for c in range(3):
            value = spread[BOX * c : BOX * c + BOX] * weight_x
            out_ref[c, pl.ds(block, 1), :] = jnp.sum(value, axis=0, keepdims=True)

    def several(step, carry):
        places = []
        for n in range(group):
            target = dest_ref[0, step * group + n]
            order = count_ref[target]
            count_ref[target] = order + 1
            places.append((target, order))
        waves(pos_ref, step * group, group, wave_ref)
        for n in range(group):
            one(step * group, n, *places[n])
        return carry

    lax.fori_loop(0, pos_ref.shape[1] // group, several, 0)


def read(dest, payload, positions):
    slots = payload.shape[0]
    return call(
        read_kernel,
        shaped(positions.shape, F32, False),
        [SMEM, VMEM, VMEM],
        [
            pltpu.VMEM((slots, ROWS, 128), F32),
            pltpu.SMEM((slots,), jnp.int32),
            pltpu.VMEM((9, together(positions.shape[1], 16), 256), F32),
        ],
    )(far(dest), near(payload), near(positions))


def moved(value, step):
    size = lax.axis_size(AX)
    return lax.ppermute(value, AX, [(i, (i + step) % size) for i in range(size)])


def exchanged(value, axes=AX):
    return lax.all_to_all(value, axes, split_axis=0, concat_axis=0, tiled=True)


def shards(marker_positions, marker_forces, dest_slab, base_cells, fluid_source):
    slots = lax.axis_size(AX)
    positions = marker_positions.transpose(1, 0, 2)
    forces = marker_forces.transpose(1, 0, 2)
    dest = dest_slab.T
    me = lax.axis_index(AX).astype(jnp.int32).reshape(1)
    payload = exchanged(build(dest, base_cells.T, positions, forces, fluid_source, slots))
    meta = payload[:, 0:1, ::BOX].astype(jnp.int32).reshape(8 * slots)
    source, up, down, up2, down2, lift = place(meta, payload, fluid_source)
    m1, m2 = moved(up, 1), moved(up2, 2)
    p1, p2 = moved(down, -1), moved(down2, -2)
    pairs, share, rise, sink = middle_down(source, up, down, m1, p1, m2, p2)
    middle = exchanged(share, AX[1])
    low, high = moved(rise, 1), moved(sink, -1)
    away = middle.astype(BF16)
    above = [moved(middle, -LOCAL), moved(away, -2 * LOCAL)]
    below = [moved(away, 2 * LOCAL), moved(middle, LOCAL)]
    blocks = [*below, middle, *above]
    velocity, picked = way_up(me, meta, lift, blocks, pairs, low, source, high, slots)
    out = read(dest, exchanged(picked), positions)
    return velocity, out.transpose(1, 0, 2)


def solution(mesh):
    torus = Mesh(mesh.devices.reshape(-1, LOCAL), AX)
    return jax.shard_map(
        shards,
        mesh=torus,
        in_specs=(P(AX), P(AX), P(AX), P(AX), P(AX)),
        out_specs=(P(AX), P(AX)),
        check_vma=False,
    )
```

```python
import math

import jax
import jax.numpy as jnp
from jax import lax
from jax.experimental import pallas as pl
from jax.experimental.pallas import tpu as pltpu
from jax.sharding import Mesh
from jax.sharding import PartitionSpec as P

AX = ("hi", "lo")
LOCAL = 8
BOX = 16
CZ = 4
HALF = CZ * BOX
ROWS = 3 * BOX
SCREEN = 1.0 / 64.0
RELAX = 2.0 / 3.0
INTERPRET = False
F32 = jnp.float32
BF16 = jnp.bfloat16
HIGH = lax.Precision.HIGHEST


def level(index):
    q = 0.25**index
    return q, SCREEN + 6.0 * q, RELAX / (SCREEN + 6.0 * q)


def call(body, out_shape, in_specs=None, scratch=(), megabytes=24):
    options = {} if in_specs is None else {"in_specs": in_specs}
    return pl.pallas_call(
        body,
        out_shape=out_shape,
        scratch_shapes=list(scratch),
        interpret=INTERPRET,
        compiler_params=pltpu.CompilerParams(vmem_limit_bytes=megabytes << 20),
        **options,
    )


def shaped(shape, dtype, near=True):
    if near and not INTERPRET:
        return pltpu.VMEM(shape, dtype)
    return jax.ShapeDtypeStruct(shape, dtype)


def near(value):
    return value if INTERPRET else pltpu.with_memory_space_constraint(value, pltpu.VMEM)


VMEM = pl.BlockSpec(memory_space=pltpu.VMEM)
SMEM = pl.BlockSpec(memory_space=pltpu.SMEM)


def far(value):
    return value if INTERPRET else pltpu.with_memory_space_constraint(value, pltpu.HBM)


def iota(shape, dim):
    return lax.broadcasted_iota(jnp.int32, shape, dim)


COS = (
    0.9999999999524891,
    -1.2337005406331254,
    0.2536692036544627,
    -0.02086006949632079,
    0.0009036280586426939,
)
SIN = (
    1.5707963267880989,
    -0.6459640961467292,
    0.07969258272440714,
    -0.004681266248964948,
    0.00015820628792786513,
)


def polynomial(coefficients, x):
    value = x * coefficients[-1] + coefficients[-2]
    for coefficient in coefficients[-3::-1]:
        value = value * x + coefficient
    return value


def split(value):
    high = value.astype(BF16)
    return high, (value - high.astype(F32)).astype(BF16)


def waves(pos_ref, first, group, wave_ref):
    rows = pl.ds(pl.multiple_of(first, group), group)
    for axis in range(3):
        point = pos_ref[axis, rows, :]
        point = 2.0 + (BOX - 5) * point if axis < 2 else (CZ - 1) * point
        nearest = jnp.floor(point + 0.5)
        rest = point - nearest
        square = rest * rest
        even = polynomial(COS, square)
        odd = polynomial(SIN, square) * rest
        quarter = nearest.astype(jnp.int32) & 3
        swap = (quarter & 1) == 1
        cosine = jnp.where(swap, odd, even)
        sine = jnp.where(swap, even, odd)
        wave_ref[3 * axis] = point
        wave_ref[3 * axis + 1] = jnp.where((quarter == 1) | (quarter == 2), -cosine, cosine)
        wave_ref[3 * axis + 2] = jnp.where(quarter >= 2, -sine, sine)


def box_weights(wave_ref, block):
    row = slice(block, block + 1)
    cell = iota((8, 256), 0)
    sign = jnp.where(cell % 4 < 2, 0.25, -0.25)
    weights = []
    for axis in range(3):
        point, cosine, sine = (wave_ref[3 * axis + n, row, :] for n in range(3))
        pattern = jnp.where(cell % 2 == 0, cosine, sine) * sign + 0.25
        parts = []
        for first in range(0, BOX if axis < 2 else 8, 8):
            offset = point - (cell + first).astype(F32)
            parts.append(jnp.where(jnp.abs(offset) < 2.0, pattern, 0.0))
        weights.append(jnp.concatenate(parts, axis=0) if axis < 2 else parts[0])
    return weights


def by_levels(weight_y, weight_z):
    return split(jnp.concatenate([weight_z[k : k + 1] * weight_y for k in range(CZ)], axis=0))


PIECES = (2 * BOX, 3 * BOX, 3 * BOX - 1)


def together(count, most):
    return math.gcd(count, most)


def build_kernel(
    dest_ref, base_ref, pos_ref, frc_ref, fluid_ref, out_ref, stage_ref, count_ref, wave_ref
):
    slots = out_ref.shape[0]
    blocks = pos_ref.shape[1]
    group = together(blocks, 32)

    def clear(t, carry):
        count_ref[t] = 0
        stage_ref[t, 0:8, :] = jnp.zeros((8, 128), F32)
        return carry

    lax.fori_loop(0, slots, clear, 0, unroll=4)
    lane = iota((8, 128), 1)
    top = iota((8, 128), 0) == 0

    def one(first, n):
        block = first + n
        weight_x, weight_y, weight_z = box_weights(wave_ref, n)
        loaded = [frc_ref[c, pl.ds(block, 1), :] * weight_x for c in range(3)]
        high, low = split(jnp.concatenate(loaded, axis=0))
        right = jnp.concatenate(by_levels(weight_y, weight_z), axis=0)
        dims = (((1,), (1,)), ((), ()))
        box = lax.dot_general(high, right, dims, preferred_element_type=F32)
        box = box + lax.dot_general(low, right, dims, preferred_element_type=F32)
        box = box + pltpu.roll(box, HALF, 1)
        base_x = base_ref[0, block].astype(F32) + 1.0
        base_y = base_ref[1, block].astype(F32)
        tiles = [box[8 * n : 8 * n + 8] for n in range(6)]
        rounded = [tile.astype(BF16).astype(F32) for tile in tiles]
        sums = [rounded[2 * c] + rounded[2 * c + 1] for c in range(3)]
        tiles[0] = jnp.where(top & (lane % HALF == 0), base_x, tiles[0])
        tiles[0] = jnp.where(top & (lane % HALF == BOX), base_y, tiles[0])
        return tiles, sums

    def several(step, carry):
        results = []
        waves(pos_ref, step * group, group, wave_ref)
        for n in range(group):
            tiles, sums = one(step * group, n)
            results.append(tiles)
            carry = tuple(a + b for a, b in zip(carry, sums))
        for n in range(group):
            target = dest_ref[0, step * group + n]
            order = count_ref[target]
            count_ref[target] = order + 1
            mine = lane // HALF == order
            for m in range(6):
                rows = slice(8 * m, 8 * m + 8)
                stage_ref[target, rows, :] = jnp.where(
                    mine, results[n][m], stage_ref[target, rows, :]
                )
        return carry

    fluid = []
    for c in range(3):
        column = fluid_ref[0, c] + fluid_ref[1, c] + (fluid_ref[2, c] + fluid_ref[3, c])
        fluid.append(jnp.sum(column.reshape(16, 8, 128), axis=0))
    zero = jnp.zeros((8, 128), F32)
    boxes = lax.fori_loop(0, blocks // group, several, (zero, zero, zero))
    fluid = [a + 0.5 * b for a, b in zip(fluid, boxes)]
    pieces = []
    for c in range(3):
        rest = jnp.broadcast_to(jnp.sum(fluid[c], axis=(0, 1), keepdims=True), (8, 128))
        marked = jnp.zeros((8, 128), F32)
        for place_of in PIECES:
            part = rest.astype(BF16).astype(F32)
            marked = jnp.where(lane == place_of, part, marked)
            rest = rest - part
        pieces.append(marked)
    held = top & ((lane == PIECES[0]) | (lane == PIECES[1]) | (lane == PIECES[2]))

    def finish(t, carry):
        tiles = []
        for c in range(3):
            row = BOX * c
            tiles.append(jnp.where(held, pieces[c], stage_ref[t, row : row + 8, :]))
            tiles.append(stage_ref[t, row + 8 : row + BOX, :])
        out_ref[t] = jnp.concatenate(tiles, axis=0).astype(BF16)
        return carry

    lax.fori_loop(0, slots, finish, 0, unroll=4)


def build(dest, base, positions, forces, fluid, slots):
    return call(
        build_kernel,
        shaped((slots, ROWS, 128), BF16),
        [SMEM, SMEM, VMEM, VMEM, VMEM],
        [
            pltpu.VMEM((slots, ROWS, 128), F32),
            pltpu.SMEM((slots,), jnp.int32),
            pltpu.VMEM((9, together(positions.shape[1], 32), 256), F32),
        ],
    )(*map(far, (dest, base, positions, forces, fluid)))


def flat_ring(x):
    rows = x.shape[-2]
    ax = x.ndim - 2
    return (
        pltpu.roll(x, 1, ax)
        + pltpu.roll(x, rows - 1, ax)
        + (pltpu.roll(x, 1, ax + 1) + pltpu.roll(x, 127, ax + 1))
    )


def group_ring(x):
    rows = x.shape[-2]
    ax = x.ndim - 2
    lane = iota(x.shape, ax + 1) & 31
    before = jnp.where(lane == 0, pltpu.roll(x, 97, ax + 1), pltpu.roll(x, 1, ax + 1))
    after = jnp.where(lane == 31, pltpu.roll(x, 31, ax + 1), pltpu.roll(x, 127, ax + 1))
    return pltpu.roll(x, 1, ax) + pltpu.roll(x, rows - 1, ax) + (before + after)


def start_of(b, below, above, ring, index):
    q, _, w = level(index)
    return w * ((4.0 / 3.0) * b + (w * q) * (ring(b) + (below + above)))


def left_of(b, u, below, above, ring, index):
    q, diag, _ = level(index)
    return b - diag * u + q * (ring(u) + (below + above))


def sweep_of(b, u, below, above, ring, index):
    q, _, w = level(index)
    return (1.0 - RELAX) * u + (w * b + (w * q) * (ring(u) + (below + above)))


def dot(left, right):
    return lax.dot_general(
        left, right, (((1,), (0,)), ((), ())), precision=HIGH, preferred_element_type=F32
    )


def lanes(test):
    return test(iota((128, 128), 0), iota((128, 128), 1))


def place_kernel(
    meta_ref, pay_ref, fluid_ref,
    src_ref, up_ref, down_ref, up2_ref, down2_ref, lift_ref,
    grid_ref, u_ref, sum_ref,
):
    slots = pay_ref.shape[0]
    lane = iota((8, 128), 1)
    sub = iota((8, 128), 0)
    for z in range(CZ):
        for c in range(3):
            grid_ref[3 * z + c, 0:128, :] = fluid_ref[z, c]
            grid_ref[3 * z + c, 128:144, :] = jnp.zeros((16, 128), F32)

    def turned(tile, order, head, base_y):
        base_x = jnp.maximum(head - 1, 0)
        shift = base_x & 7
        row = pl.multiple_of(base_x - shift, 8)
        window = (lane - base_y) & 127
        inside = (window >= 1) & (window <= BOX - 2) & (head > 0)
        late = inside & (sub >= shift)
        early = inside & (sub < shift)
        pieces = [pltpu.roll(tile[8 * n : 8 * n + 8], shift, 0) for n in range(6)]
        values = []
        for k in range(CZ):
            step = (base_y - HALF * order - BOX * k) & 127
            values.append([pltpu.roll(piece, step, 1) for piece in pieces])
        return row, late, early, values

    def add(row, late, early, values):
        for k in range(CZ):
            for c in range(3):
                first, second = values[k][2 * c], values[k][2 * c + 1]
                kc = 3 * k + c
                grid_ref[kc, pl.ds(row, 8), :] += jnp.where(late, first, 0.0)
                grid_ref[kc, pl.ds(row + 8, 8), :] += jnp.where(
                    early, first, jnp.where(late, second, 0.0)
                )
                grid_ref[kc, pl.ds(row + 16, 8), :] += jnp.where(early, second, 0.0)

    group = together(slots, 16)

    def several(step, carry):
        found = []
        for n in range(group):
            d = step * group + n
            tile = pay_ref[d].astype(F32)
            carry = tuple(
                carry[c] + jnp.where(held, tile[BOX * c : BOX * c + 8], 0.0) for c in range(3)
            )
            for order in range(2):
                at = 8 * d + 4 * order
                found.append(turned(tile, order, meta_ref[at], meta_ref[at + 1]))
        for one in found:
            add(*one)
        return carry

    held = (sub == 0) & ((lane == PIECES[0]) | (lane == PIECES[1]) | (lane == PIECES[2]))
    zero = jnp.zeros((8, 128), F32)
    totals = lax.fori_loop(0, slots // group, several, (zero, zero, zero))
    factor = (1.0 - level(3)[2] * SCREEN) ** 6 / SCREEN
    for index in range(3):
        factor = factor * (1.0 - level(index)[2] * SCREEN) ** 2
    scale = factor / (slots * CZ * 128.0 * 128.0)
    lift_ref[...] = zero
    for c in range(3):
        total = jnp.sum(totals[c], axis=(0, 1), keepdims=True)
        lift_ref[c : c + 1, :] = jnp.broadcast_to(total * scale, (1, 128))
    pool = [
        jnp.where(lanes(lambda r, l: (r // 2 == (l & 63)) & (l // 64 == half)), 0.125, 0.0)
        for half in range(2)
    ]
    q, _, w = level(0)
    spill_up, spill_down = [], []
    for c in range(3):
        for z in range(CZ):
            kc = 3 * z + c
            grid_ref[kc, 0:16, :] += grid_ref[kc, 128:144, :]
            src_ref[z, c] = grid_ref[kc, 0:128, :]

        def b_at(z):
            return src_ref[z, c] if 0 <= z < CZ else 0.0

        for z in range(CZ):
            u_ref[z + 1] = start_of(src_ref[z, c], b_at(z - 1), b_at(z + 1), flat_ring, 0)
        u_ref[0] = (w * w * q) * src_ref[0, c]
        u_ref[CZ + 1] = (w * w * q) * src_ref[CZ - 1, c]

        def left(z):
            if z == -2:
                return q * u_ref[0]
            if z == CZ + 1:
                return q * u_ref[CZ + 1]
            below = u_ref[z] if z > -1 else 0.0
            above = u_ref[z + 2] if z < CZ else 0.0
            return left_of(b_at(z), u_ref[z + 1], below, above, flat_ring, 0)

        rows = []
        for pair in range(-1, 3):
            sum_ref[...] = left(2 * pair) + left(2 * pair + 1)
            rows.append(sum_ref[pl.ds(0, 64, 2), :] + sum_ref[pl.ds(1, 64, 2), :])
        own = dot(rows[1], pool[0]) + dot(rows[2], pool[1])
        up_ref[c] = own
        down_ref[c] = own
        spill_down.append(dot(rows[0], pool[c % 2]))
        spill_up.append(dot(rows[3], pool[c % 2]))
    for ref, far_ref, spill in ((up_ref, up2_ref, spill_up), (down_ref, down2_ref, spill_down)):
        both = spill[0] + spill[1]
        ref[3] = both
        ref[4] = spill[2]
        far_ref[0] = both.astype(BF16)
        far_ref[1] = spill[2].astype(BF16)


def place(meta, payload, fluid):
    return call(
        place_kernel,
        (
            shaped(fluid.shape, F32),
            shaped((5, 64, 128), F32),
            shaped((5, 64, 128), F32),
            shaped((2, 64, 128), BF16),
            shaped((2, 64, 128), BF16),
            shaped((8, 128), F32),
        ),
        [SMEM, VMEM, VMEM],
        [
            pltpu.VMEM((12, 144, 128), F32),
            pltpu.VMEM((CZ + 2, 128, 128), F32),
            pltpu.VMEM((128, 128), F32),
        ],
    )(meta, near(payload), near(fluid))


def both_layers(tile):
    lane = iota(tile.shape, tile.ndim - 1)
    turned = pltpu.roll(tile, 64, tile.ndim - 1)
    return jnp.where(lane < 64, tile, turned), jnp.where(lane < 64, turned, tile)


def pack_coarse(value):
    last = value[24:32]
    lane = iota((8, 128), 1)
    return [
        jnp.where(lane < 96, value[8 * c : 8 * c + 8], pltpu.roll(last, 96 - 32 * c, 1))
        for c in range(3)
    ]


def unpack_coarse(tile):
    lane = iota((8, 128), 1)
    last = jnp.zeros((8, 128), F32)
    rows = []
    for c in range(3):
        piece = tile[8 * c : 8 * c + 8]
        turned = pltpu.roll(piece, (32 * c - 96) % 128, 1)
        last = jnp.where(lane // 32 == c, turned, last)
        rows.append(jnp.where(lane < 96, piece, 0.0))
    return jnp.concatenate(rows + [last], axis=0)


def spilled(ref, c, first=0):
    return both_layers(ref[first + c // 2].astype(F32))[c % 2]


U_ROW = 12 * 128


def middle_kernel(
    src_ref, up_ref, down_ref, m1_ref, p1_ref, m2_ref, p2_ref,
    pairs_ref, out_ref, rise_ref, sink_ref, sum_ref,
):
    total = None
    for ref, order in ((rise_ref, (3, 2, 1)), (sink_ref, (0, 1, 2))):
        for c in range(3):
            parts = split(src_ref[order[0], c])
            parts += tuple(src_ref[z, c].astype(BF16) for z in order[1:])
            for n in range(4):
                ref[128 * (3 * n + c) : 128 * (3 * n + c + 1), :] = parts[n]
    lane = iota((64, 128), 1)
    for c in range(3):
        m1, own, p1 = both_layers(m1_ref[c]), both_layers(up_ref[c]), both_layers(p1_ref[c])
        b = [
            m1[0] + spilled(m2_ref, c),
            m1[1] + spilled(down_ref, c, 3),
            own[0] + spilled(m1_ref, c, 3),
            own[1] + spilled(p1_ref, c, 3),
            p1[0] + spilled(up_ref, c, 3),
            p1[1] + spilled(p2_ref, c),
        ]
        for j in range(3):
            pairs_ref[j, c] = jnp.where(lane < 64, b[2 * j], b[2 * j + 1])
        u = [start_of(b[i], b[i - 1], b[i + 1], flat_ring, 1) for i in range(1, 5)]
        rows = slice(U_ROW + 64 * c, U_ROW + 64 * c + 64)
        rise_ref[rows, :] = jnp.where(lane < 64, u[0], u[1]).astype(BF16)
        sink_ref[rows, :] = jnp.where(lane < 64, u[2], u[3]).astype(BF16)
        left = [left_of(b[i + 1], u[i], u[i - 1], u[i + 1], flat_ring, 1) for i in (1, 2)]
        sum_ref[...] = left[0] + left[1]
        rows = sum_ref[pl.ds(0, 32, 2), :] + sum_ref[pl.ds(1, 32, 2), :]
        pool = jnp.where(
            lanes(lambda r, l: (r // 2 == (l & 31)) & (l // 32 == c) & (r < 64)), 0.125, 0.0
        )
        part = dot(rows, pool)
        total = part if total is None else total + part
    packed = jnp.concatenate(pack_coarse(total), axis=0)
    for d in range(out_ref.shape[0]):
        out_ref[d] = packed


def middle_down(source, up, down, m1, p1, m2, p2):
    return call(
        middle_kernel,
        (
            shaped((3, 3, 64, 128), F32),
            shaped((LOCAL, 24, 128), F32),
            shaped((U_ROW + 192, 128), BF16),
            shaped((U_ROW + 192, 128), BF16),
        ),
        None,
        [pltpu.VMEM((64, 128), F32)],
    )(*map(near, (source, up, down, m1, p1, m2, p2)))


def inner(x):
    return x[1:-1]


def coarse_part(me, blocks, lift_ref, window_ref, pool_ref, final_ref):
    parity = me % 2
    first = me % LOCAL - parity
    for n, ref in enumerate(blocks):
        window_ref[LOCAL * n : LOCAL * n + LOCAL] = ref[...].astype(F32)
    b2 = jnp.stack([unpack_coarse(window_ref[first + t]) for t in range(34)])
    group = iota((1, 128), 1) // 32
    lift = jnp.zeros((1, 128), F32)
    for c in range(3):
        lift = jnp.where(group == c, lift_ref[c : c + 1, :], lift)
    _, _, w3 = level(3)
    u2 = start_of(inner(b2), b2[:-2], b2[2:], group_ring, 2)
    r2 = left_of(b2[2:-2], inner(u2), u2[:-2], u2[2:], group_ring, 2)
    pairs = r2.reshape(15, 2, 32, 128)
    pool_ref[...] = (pairs[:, 0] + pairs[:, 1]).reshape(480, 128)
    rows = pool_ref[pl.ds(0, 240, 2), :] + pool_ref[pl.ds(1, 240, 2), :]
    pool = jnp.where(
        lanes(lambda r, l: ((r & 31) // 2 == (l & 15)) & (r // 32 == l // 32)), 0.125, 0.0
    )
    b3 = dot(rows, pool).reshape(15, 16, 128)
    u3 = w3 * b3
    for _ in range(5):
        b3 = inner(b3)
        u3 = sweep_of(b3, inner(u3), u3[:-2], u3[2:], group_ring, 3)
    u3 = (u3 + lift[None]).reshape(80, 128)
    spread = jnp.where(
        lanes(lambda r, l: ((l & 31) // 2 == (r & 31)) & (r // 32 == l // 32)), 1.0, 0.0
    )
    wide = dot(u3, spread)
    pool_ref[pl.ds(0, 80, 2), :] = wide
    pool_ref[pl.ds(1, 80, 2), :] = wide
    lifted = pool_ref[0:160, :].reshape(5, 1, 32, 128)
    u = (u2[11:21].reshape(5, 2, 32, 128) + lifted).reshape(10, 32, 128)
    u = sweep_of(b2[13:21], inner(u), u[:-2], u[2:], group_ring, 2)
    u = sweep_of(b2[14:20], inner(u), u[:-2], u[2:], group_ring, 2)
    final_ref[...] = u
    return jnp.concatenate([final_ref[parity + h] for h in range(5)], axis=0)


def up_kernel(
    me_ref, meta_ref, lift_ref, g0_ref, g1_ref, g2_ref, g3_ref, g4_ref,
    pairs_ref, low_ref, own_ref, high_ref, vel_ref, pay_ref,
    window_ref, pool_ref, final_ref, lift1_ref, b1_ref, u1_ref, v1_ref, lift0_ref, u0_ref,
    v0_ref, ext_ref, halo_ref,
):
    blocks = (g0_ref, g1_ref, g2_ref, g3_ref, g4_ref)
    coarse = coarse_part(me_ref[0], blocks, lift_ref, window_ref, pool_ref, final_ref)
    for c in range(3):
        spread = jnp.where(lanes(lambda r, l: r == 32 * c + (l & 63) // 2), 1.0, 0.0)
        wide = dot(coarse, spread)
        lift1_ref[c, pl.ds(0, 160, 2), :] = wide
        lift1_ref[c, pl.ds(1, 160, 2), :] = wide
    spread0 = jnp.where(lanes(lambda r, l: r == l // 2), 1.0, 0.0)

    def b_at(z, c):
        if 0 <= z < CZ:
            return own_ref[z, c]
        return halo_ref[z + 3 if z < 0 else z - 1]

    def component(c, carry):
        for ref, order in ((low_ref, (2, 1, 0)), (high_ref, (3, 4, 5))):
            planes = [
                ref[pl.ds(pl.multiple_of(128 * (3 * n + c), 128), 128), :].astype(F32)
                for n in range(4)
            ]
            halo_ref[order[0]] = planes[0] + planes[1]
            halo_ref[order[1]] = planes[2]
            halo_ref[order[2]] = planes[3]
        for j in range(3):
            b1_ref[2 * j], b1_ref[2 * j + 1] = both_layers(pairs_ref[j, c])
        rows = pl.ds(pl.multiple_of(U_ROW + 64 * c, 64), 64)
        u1 = list(both_layers(low_ref[rows, :].astype(F32)))
        for i in range(1, 5):
            u1.append(start_of(b1_ref[i], b1_ref[i - 1], b1_ref[i + 1], flat_ring, 1))
        u1.extend(both_layers(high_ref[rows, :].astype(F32)))
        for z in range(-3, 5):
            h = z // 2 + 2
            u1_ref[z + 3] = u1[z + 3] + lift1_ref[c, 64 * h : 64 * h + 64, :]
        for z in range(-2, 4):
            i = z + 3
            v1_ref[z + 2] = sweep_of(
                b1_ref[z + 2], u1_ref[i], u1_ref[i - 1], u1_ref[i + 1], flat_ring, 1
            )
        for z in range(-1, 3):
            i = z + 2
            value = sweep_of(
                b1_ref[z + 2], v1_ref[i], v1_ref[i - 1], v1_ref[i + 1], flat_ring, 1
            )
            wide = dot(value, spread0)
            lift0_ref[z + 1, pl.ds(0, 64, 2), :] = wide
            lift0_ref[z + 1, pl.ds(1, 64, 2), :] = wide
        for z in range(-2, 6):
            u0_ref[z + 2] = (
                start_of(b_at(z, c), b_at(z - 1, c), b_at(z + 1, c), flat_ring, 0)
                + lift0_ref[z // 2 + 1]
            )
        for z in range(-1, 5):
            i = z + 2
            v0_ref[z + 1] = sweep_of(
                b_at(z, c), u0_ref[i], u0_ref[i - 1], u0_ref[i + 1], flat_ring, 0
            )
        for z in range(CZ):
            i = z + 1
            value = sweep_of(
                own_ref[z, c], v0_ref[i], v0_ref[i - 1], v0_ref[i + 1], flat_ring, 0
            )
            vel_ref[z, c] = value
            rounded = value.astype(BF16).astype(F32)
            ext_ref[3 * z + c, 0:128, :] = rounded
            ext_ref[3 * z + c, 128:144, :] = rounded[0:16]
        return carry

    lax.fori_loop(0, 3, component, 0)
    lane = iota((8, 128), 1)
    sub = iota((8, 128), 0)

    part = [(lane // BOX) % CZ == k for k in range(CZ)]

    def gather(order, head, base_y):
        base_x = jnp.maximum(head - 1, 0)
        shift = base_x & 7
        row = pl.multiple_of(base_x - shift, 8)
        late = sub >= shift
        values = []
        for k in range(CZ):
            step = (HALF * order + BOX * k - base_y) & 127
            line = []
            for c in range(3):
                tiles = [ext_ref[3 * k + c, pl.ds(row + 8 * n, 8), :] for n in range(3)]
                for n in range(2):
                    value = jnp.where(late, tiles[n], tiles[n + 1])
                    line.append(pltpu.roll(value, step, 1))
            values.append(line)
        return (8 - shift) & 7, values

    group = together(pay_ref.shape[0], 16)

    def several(step, carry):
        found = []
        for n in range(group):
            for order in range(2):
                at = 8 * (step * group + n) + 4 * order
                found.append(gather(order, meta_ref[at], meta_ref[at + 1]))
        for n in range(group):
            pieces = []
            for m in range(6):
                both = []
                for order in range(2):
                    back, values = found[2 * n + order]
                    packed = values[0][m]
                    for k in range(1, CZ):
                        packed = jnp.where(part[k], values[k][m], packed)
                    both.append(pltpu.roll(packed, back, 0))
                pieces.append(jnp.where(lane < HALF, both[0], both[1]))
            pay_ref[step * group + n] = jnp.concatenate(pieces, axis=0).astype(BF16)
        return carry

    lax.fori_loop(0, pay_ref.shape[0] // group, several, 0)


def way_up(me, meta, lift, blocks, pairs, low, own, high, slots):
    return call(
        up_kernel,
        (
            shaped(own.shape, F32, False),
            shaped((slots, ROWS, 128), BF16),
        ),
        [SMEM, SMEM] + [VMEM] * 10,
        [
            pltpu.VMEM((5 * LOCAL, 24, 128), F32),
            pltpu.VMEM((480, 128), F32),
            pltpu.VMEM((6, 32, 128), F32),
            pltpu.VMEM((3, 320, 128), F32),
            pltpu.VMEM((6, 64, 128), F32),
            pltpu.VMEM((8, 64, 128), F32),
            pltpu.VMEM((6, 64, 128), F32),
            pltpu.VMEM((4, 128, 128), F32),
            pltpu.VMEM((8, 128, 128), F32),
            pltpu.VMEM((6, 128, 128), F32),
            pltpu.VMEM((12, 144, 128), F32),
            pltpu.VMEM((6, 128, 128), F32),
        ],
    )(me, meta, *map(near, (lift, *blocks, pairs, low, own, high)))


def read_kernel(dest_ref, pay_ref, pos_ref, out_ref, stage_ref, count_ref, wave_ref):
    slots = pay_ref.shape[0]

    def widen(t, carry):
        count_ref[t] = 0
        stage_ref[t] = pay_ref[t].astype(F32)
        return carry

    lax.fori_loop(0, slots, widen, 0, unroll=4)
    lane = iota((8, 128), 1)

    group = together(pos_ref.shape[1], 32)

    def one(first, n, target, order):
        block = first + n
        weight_x, weight_y, weight_z = box_weights(wave_ref, n)
        mine = lane // HALF == order
        left = []
        for m in range(6):
            packed = stage_ref[target, 8 * m : 8 * m + 8, :]
            left.append(jnp.where(mine, packed, pltpu.roll(packed, HALF, 1)))
        left = jnp.concatenate(left, axis=0).astype(BF16)
        right = jnp.concatenate(by_levels(weight_y, weight_z), axis=0)
        spread = lax.dot_general(
            left, right, (((1,), (0,)), ((), ())), preferred_element_type=F32
        )
        for c in range(3):
            value = spread[BOX * c : BOX * c + BOX] * weight_x
            out_ref[c, pl.ds(block, 1), :] = jnp.sum(value, axis=0, keepdims=True)

    def several(step, carry):
        places = []
        for n in range(group):
            target = dest_ref[0, step * group + n]
            order = count_ref[target]
            count_ref[target] = order + 1
            places.append((target, order))
        waves(pos_ref, step * group, group, wave_ref)
        for n in range(group):
            one(step * group, n, *places[n])
        return carry

    lax.fori_loop(0, pos_ref.shape[1] // group, several, 0)


def read(dest, payload, positions):
    slots = payload.shape[0]
    return call(
        read_kernel,
        shaped(positions.shape, F32, False),
        [SMEM, VMEM, VMEM],
        [
            pltpu.VMEM((slots, ROWS, 128), F32),
            pltpu.SMEM((slots,), jnp.int32),
            pltpu.VMEM((9, together(positions.shape[1], 32), 256), F32),
        ],
    )(far(dest), near(payload), near(positions))


def moved(value, step):
    size = lax.axis_size(AX)
    return lax.ppermute(value, AX, [(i, (i + step) % size) for i in range(size)])


def exchanged(value, axes=AX):
    return lax.all_to_all(value, axes, split_axis=0, concat_axis=0, tiled=True)


def shards(marker_positions, marker_forces, dest_slab, base_cells, fluid_source):
    slots = lax.axis_size(AX)
    positions = marker_positions.transpose(1, 0, 2)
    forces = marker_forces.transpose(1, 0, 2)
    dest = dest_slab.T
    me = lax.axis_index(AX).astype(jnp.int32).reshape(1)
    payload = exchanged(build(dest, base_cells.T, positions, forces, fluid_source, slots))
    meta = payload[:, 0:1, ::BOX].astype(jnp.int32).reshape(8 * slots)
    source, up, down, up2, down2, lift = place(meta, payload, fluid_source)
    m1, m2 = moved(up, 1), moved(up2, 2)
    p1, p2 = moved(down, -1), moved(down2, -2)
    pairs, share, rise, sink = middle_down(source, up, down, m1, p1, m2, p2)
    middle = exchanged(share, AX[1])
    low, high = moved(rise, 1), moved(sink, -1)
    away = middle.astype(BF16)
    above = [moved(middle, -LOCAL), moved(away, -2 * LOCAL)]
    below = [moved(away, 2 * LOCAL), moved(middle, LOCAL)]
    blocks = [*below, middle, *above]
    velocity, picked = way_up(me, meta, lift, blocks, pairs, low, source, high, slots)
    out = read(dest, exchanged(picked), positions)
    return velocity, out.transpose(1, 0, 2)


def solution(mesh):
    torus = Mesh(mesh.devices.reshape(-1, LOCAL), AX)
    return jax.shard_map(
        shards,
        mesh=torus,
        in_specs=(P(AX), P(AX), P(AX), P(AX), P(AX)),
        out_specs=(P(AX), P(AX)),
        check_vma=False,
    )
```

```python
import math

import jax
import jax.numpy as jnp
from jax import lax
from jax.experimental import pallas as pl
from jax.experimental.pallas import tpu as pltpu
from jax.sharding import Mesh
from jax.sharding import PartitionSpec as P

AX = ("hi", "lo")
LOCAL = 8
BOX = 16
CZ = 4
HALF = CZ * BOX
ROWS = 3 * BOX
SCREEN = 1.0 / 64.0
RELAX = 2.0 / 3.0
INTERPRET = False
F32 = jnp.float32
BF16 = jnp.bfloat16
HIGH = lax.Precision.HIGHEST


def level(index):
    q = 0.25**index
    return q, SCREEN + 6.0 * q, RELAX / (SCREEN + 6.0 * q)


def call(body, out_shape, in_specs=None, scratch=(), megabytes=24):
    options = {} if in_specs is None else {"in_specs": in_specs}
    return pl.pallas_call(
        body,
        out_shape=out_shape,
        scratch_shapes=list(scratch),
        interpret=INTERPRET,
        compiler_params=pltpu.CompilerParams(vmem_limit_bytes=megabytes << 20),
        **options,
    )


def shaped(shape, dtype, near=True):
    if near and not INTERPRET:
        return pltpu.VMEM(shape, dtype)
    return jax.ShapeDtypeStruct(shape, dtype)


def near(value):
    return value if INTERPRET else pltpu.with_memory_space_constraint(value, pltpu.VMEM)


VMEM = pl.BlockSpec(memory_space=pltpu.VMEM)
SMEM = pl.BlockSpec(memory_space=pltpu.SMEM)


def far(value):
    return value if INTERPRET else pltpu.with_memory_space_constraint(value, pltpu.HBM)


def iota(shape, dim):
    return lax.broadcasted_iota(jnp.int32, shape, dim)


COS = (
    0.9999999999524891,
    -1.2337005406331254,
    0.2536692036544627,
    -0.02086006949632079,
    0.0009036280586426939,
)
SIN = (
    1.5707963267880989,
    -0.6459640961467292,
    0.07969258272440714,
    -0.004681266248964948,
    0.00015820628792786513,
)


def polynomial(coefficients, x):
    value = x * coefficients[-1] + coefficients[-2]
    for coefficient in coefficients[-3::-1]:
        value = value * x + coefficient
    return value


def split(value):
    high = value.astype(BF16)
    return high, (value - high.astype(F32)).astype(BF16)


def waves(pos_ref, first, group, wave_ref):
    rows = pl.ds(pl.multiple_of(first, group), group)
    for axis in range(3):
        point = pos_ref[axis, rows, :]
        point = 2.0 + (BOX - 5) * point if axis < 2 else (CZ - 1) * point
        nearest = jnp.floor(point + 0.5)
        rest = point - nearest
        square = rest * rest
        even = polynomial(COS, square)
        odd = polynomial(SIN, square) * rest
        quarter = nearest.astype(jnp.int32) & 3
        swap = (quarter & 1) == 1
        cosine = jnp.where(swap, odd, even)
        sine = jnp.where(swap, even, odd)
        wave_ref[3 * axis] = point
        wave_ref[3 * axis + 1] = jnp.where((quarter == 1) | (quarter == 2), -cosine, cosine)
        wave_ref[3 * axis + 2] = jnp.where(quarter >= 2, -sine, sine)


def box_weights(wave_ref, block):
    row = slice(block, block + 1)
    cell = iota((8, 256), 0)
    sign = jnp.where(cell % 4 < 2, 0.25, -0.25)
    weights = []
    for axis in range(3):
        point, cosine, sine = (wave_ref[3 * axis + n, row, :] for n in range(3))
        pattern = jnp.where(cell % 2 == 0, cosine, sine) * sign + 0.25
        parts = []
        for first in range(0, BOX if axis < 2 else 8, 8):
            offset = point - (cell + first).astype(F32)
            parts.append(jnp.where(jnp.abs(offset) < 2.0, pattern, 0.0))
        weights.append(jnp.concatenate(parts, axis=0) if axis < 2 else parts[0])
    return weights


def by_levels(weight_y, weight_z):
    return split(jnp.concatenate([weight_z[k : k + 1] * weight_y for k in range(CZ)], axis=0))


PIECES = (2 * BOX, 3 * BOX, 3 * BOX - 1)


def together(count, most):
    return math.gcd(count, most)


def build_kernel(
    dest_ref, base_ref, pos_ref, frc_ref, fluid_ref, out_ref, stage_ref, count_ref, wave_ref
):
    slots = out_ref.shape[0]
    blocks = pos_ref.shape[1]
    group = together(blocks, 64)

    def clear(t, carry):
        count_ref[t] = 0
        stage_ref[t, 0:8, :] = jnp.zeros((8, 128), F32)
        return carry

    lax.fori_loop(0, slots, clear, 0, unroll=4)
    lane = iota((8, 128), 1)
    top = iota((8, 128), 0) == 0

    def one(first, n):
        block = first + n
        weight_x, weight_y, weight_z = box_weights(wave_ref, n)
        loaded = [frc_ref[c, pl.ds(block, 1), :] * weight_x for c in range(3)]
        high, low = split(jnp.concatenate(loaded, axis=0))
        right = jnp.concatenate(by_levels(weight_y, weight_z), axis=0)
        dims = (((1,), (1,)), ((), ()))
        box = lax.dot_general(high, right, dims, preferred_element_type=F32)
        box = box + lax.dot_general(low, right, dims, preferred_element_type=F32)
        box = box + pltpu.roll(box, HALF, 1)
        base_x = base_ref[0, block].astype(F32) + 1.0
        base_y = base_ref[1, block].astype(F32)
        tiles = [box[8 * n : 8 * n + 8] for n in range(6)]
        rounded = [tile.astype(BF16).astype(F32) for tile in tiles]
        sums = [rounded[2 * c] + rounded[2 * c + 1] for c in range(3)]
        tiles[0] = jnp.where(top & (lane % HALF == 0), base_x, tiles[0])
        tiles[0] = jnp.where(top & (lane % HALF == BOX), base_y, tiles[0])
        return tiles, sums

    def several(step, carry):
        results = []
        waves(pos_ref, step * group, group, wave_ref)
        for n in range(group):
            tiles, sums = one(step * group, n)
            results.append(tiles)
            carry = tuple(a + b for a, b in zip(carry, sums))
        for n in range(group):
            target = dest_ref[0, step * group + n]
            order = count_ref[target]
            count_ref[target] = order + 1
            mine = lane // HALF == order
            for m in range(6):
                rows = slice(8 * m, 8 * m + 8)
                stage_ref[target, rows, :] = jnp.where(
                    mine, results[n][m], stage_ref[target, rows, :]
                )
        return carry

    fluid = []
    for c in range(3):
        column = fluid_ref[0, c] + fluid_ref[1, c] + (fluid_ref[2, c] + fluid_ref[3, c])
        fluid.append(jnp.sum(column.reshape(16, 8, 128), axis=0))
    zero = jnp.zeros((8, 128), F32)
    boxes = lax.fori_loop(0, blocks // group, several, (zero, zero, zero))
    fluid = [a + 0.5 * b for a, b in zip(fluid, boxes)]
    pieces = []
    for c in range(3):
        rest = jnp.broadcast_to(jnp.sum(fluid[c], axis=(0, 1), keepdims=True), (8, 128))
        marked = jnp.zeros((8, 128), F32)
        for place_of in PIECES:
            part = rest.astype(BF16).astype(F32)
            marked = jnp.where(lane == place_of, part, marked)
            rest = rest - part
        pieces.append(marked)
    held = top & ((lane == PIECES[0]) | (lane == PIECES[1]) | (lane == PIECES[2]))

    def finish(t, carry):
        tiles = []
        for c in range(3):
            row = BOX * c
            tiles.append(jnp.where(held, pieces[c], stage_ref[t, row : row + 8, :]))
            tiles.append(stage_ref[t, row + 8 : row + BOX, :])
        out_ref[t] = jnp.concatenate(tiles, axis=0).astype(BF16)
        return carry

    lax.fori_loop(0, slots, finish, 0, unroll=4)


def build(dest, base, positions, forces, fluid, slots):
    return call(
        build_kernel,
        shaped((slots, ROWS, 128), BF16),
        [SMEM, SMEM, VMEM, VMEM, VMEM],
        [
            pltpu.VMEM((slots, ROWS, 128), F32),
            pltpu.SMEM((slots,), jnp.int32),
            pltpu.VMEM((9, together(positions.shape[1], 64), 256), F32),
        ],
    )(*map(far, (dest, base, positions, forces, fluid)))


def flat_ring(x):
    rows = x.shape[-2]
    ax = x.ndim - 2
    return (
        pltpu.roll(x, 1, ax)
        + pltpu.roll(x, rows - 1, ax)
        + (pltpu.roll(x, 1, ax + 1) + pltpu.roll(x, 127, ax + 1))
    )


def group_ring(x):
    rows = x.shape[-2]
    ax = x.ndim - 2
    lane = iota(x.shape, ax + 1) & 31
    before = jnp.where(lane == 0, pltpu.roll(x, 97, ax + 1), pltpu.roll(x, 1, ax + 1))
    after = jnp.where(lane == 31, pltpu.roll(x, 31, ax + 1), pltpu.roll(x, 127, ax + 1))
    return pltpu.roll(x, 1, ax) + pltpu.roll(x, rows - 1, ax) + (before + after)


def start_of(b, below, above, ring, index):
    q, _, w = level(index)
    return w * ((4.0 / 3.0) * b + (w * q) * (ring(b) + (below + above)))


def left_of(b, u, below, above, ring, index):
    q, diag, _ = level(index)
    return b - diag * u + q * (ring(u) + (below + above))


def sweep_of(b, u, below, above, ring, index):
    q, _, w = level(index)
    return (1.0 - RELAX) * u + (w * b + (w * q) * (ring(u) + (below + above)))


def dot(left, right):
    return lax.dot_general(
        left, right, (((1,), (0,)), ((), ())), precision=HIGH, preferred_element_type=F32
    )


def lanes(test):
    return test(iota((128, 128), 0), iota((128, 128), 1))


def place_kernel(
    meta_ref, pay_ref, fluid_ref,
    src_ref, up_ref, down_ref, up2_ref, down2_ref, lift_ref,
    grid_ref, u_ref, sum_ref,
):
    slots = pay_ref.shape[0]
    lane = iota((8, 128), 1)
    sub = iota((8, 128), 0)
    for z in range(CZ):
        for c in range(3):
            grid_ref[3 * z + c, 0:128, :] = fluid_ref[z, c]
            grid_ref[3 * z + c, 128:144, :] = jnp.zeros((16, 128), F32)

    def turned(tile, order, head, base_y):
        base_x = jnp.maximum(head - 1, 0)
        shift = base_x & 7
        row = pl.multiple_of(base_x - shift, 8)
        window = (lane - base_y) & 127
        inside = (window >= 1) & (window <= BOX - 2) & (head > 0)
        late = inside & (sub >= shift)
        early = inside & (sub < shift)
        pieces = [pltpu.roll(tile[8 * n : 8 * n + 8], shift, 0) for n in range(6)]
        values = []
        for k in range(CZ):
            step = (base_y - HALF * order - BOX * k) & 127
            values.append([pltpu.roll(piece, step, 1) for piece in pieces])
        return row, late, early, values

    def add(row, late, early, values):
        for k in range(CZ):
            for c in range(3):
                first, second = values[k][2 * c], values[k][2 * c + 1]
                kc = 3 * k + c
                grid_ref[kc, pl.ds(row, 8), :] += jnp.where(late, first, 0.0)
                grid_ref[kc, pl.ds(row + 8, 8), :] += jnp.where(
                    early, first, jnp.where(late, second, 0.0)
                )
                grid_ref[kc, pl.ds(row + 16, 8), :] += jnp.where(early, second, 0.0)

    group = together(slots, 32)

    def several(step, carry):
        found = []
        for n in range(group):
            d = step * group + n
            tile = pay_ref[d].astype(F32)
            carry = tuple(
                carry[c] + jnp.where(held, tile[BOX * c : BOX * c + 8], 0.0) for c in range(3)
            )
            for order in range(2):
                at = 8 * d + 4 * order
                found.append(turned(tile, order, meta_ref[at], meta_ref[at + 1]))
        for one in found:
            add(*one)
        return carry

    held = (sub == 0) & ((lane == PIECES[0]) | (lane == PIECES[1]) | (lane == PIECES[2]))
    zero = jnp.zeros((8, 128), F32)
    totals = lax.fori_loop(0, slots // group, several, (zero, zero, zero))
    factor = (1.0 - level(3)[2] * SCREEN) ** 6 / SCREEN
    for index in range(3):
        factor = factor * (1.0 - level(index)[2] * SCREEN) ** 2
    scale = factor / (slots * CZ * 128.0 * 128.0)
    lift_ref[...] = zero
    for c in range(3):
        total = jnp.sum(totals[c], axis=(0, 1), keepdims=True)
        lift_ref[c : c + 1, :] = jnp.broadcast_to(total * scale, (1, 128))
    pool = [
        jnp.where(lanes(lambda r, l: (r // 2 == (l & 63)) & (l // 64 == half)), 0.125, 0.0)
        for half in range(2)
    ]
    q, _, w = level(0)
    spill_up, spill_down = [], []
    for c in range(3):
        for z in range(CZ):
            kc = 3 * z + c
            grid_ref[kc, 0:16, :] += grid_ref[kc, 128:144, :]
            src_ref[z, c] = grid_ref[kc, 0:128, :]

        def b_at(z):
            return src_ref[z, c] if 0 <= z < CZ else 0.0

        for z in range(CZ):
            u_ref[z + 1] = start_of(src_ref[z, c], b_at(z - 1), b_at(z + 1), flat_ring, 0)
        u_ref[0] = (w * w * q) * src_ref[0, c]
        u_ref[CZ + 1] = (w * w * q) * src_ref[CZ - 1, c]

        def left(z):
            if z == -2:
                return q * u_ref[0]
            if z == CZ + 1:
                return q * u_ref[CZ + 1]
            below = u_ref[z] if z > -1 else 0.0
            above = u_ref[z + 2] if z < CZ else 0.0
            return left_of(b_at(z), u_ref[z + 1], below, above, flat_ring, 0)

        rows = []
        for pair in range(-1, 3):
            sum_ref[...] = left(2 * pair) + left(2 * pair + 1)
            rows.append(sum_ref[pl.ds(0, 64, 2), :] + sum_ref[pl.ds(1, 64, 2), :])
        own = dot(rows[1], pool[0]) + dot(rows[2], pool[1])
        up_ref[c] = own
        down_ref[c] = own
        spill_down.append(dot(rows[0], pool[c % 2]))
        spill_up.append(dot(rows[3], pool[c % 2]))
    for ref, far_ref, spill in ((up_ref, up2_ref, spill_up), (down_ref, down2_ref, spill_down)):
        both = spill[0] + spill[1]
        ref[3] = both
        ref[4] = spill[2]
        far_ref[0] = both.astype(BF16)
        far_ref[1] = spill[2].astype(BF16)


def place(meta, payload, fluid):
    return call(
        place_kernel,
        (
            shaped(fluid.shape, F32),
            shaped((5, 64, 128), F32),
            shaped((5, 64, 128), F32),
            shaped((2, 64, 128), BF16),
            shaped((2, 64, 128), BF16),
            shaped((8, 128), F32),
        ),
        [SMEM, VMEM, VMEM],
        [
            pltpu.VMEM((12, 144, 128), F32),
            pltpu.VMEM((CZ + 2, 128, 128), F32),
            pltpu.VMEM((128, 128), F32),
        ],
    )(meta, near(payload), near(fluid))


def both_layers(tile):
    lane = iota(tile.shape, tile.ndim - 1)
    turned = pltpu.roll(tile, 64, tile.ndim - 1)
    return jnp.where(lane < 64, tile, turned), jnp.where(lane < 64, turned, tile)


def pack_coarse(value):
    last = value[24:32]
    lane = iota((8, 128), 1)
    return [
        jnp.where(lane < 96, value[8 * c : 8 * c + 8], pltpu.roll(last, 96 - 32 * c, 1))
        for c in range(3)
    ]


def unpack_coarse(tile):
    lane = iota((8, 128), 1)
    last = jnp.zeros((8, 128), F32)
    rows = []
    for c in range(3):
        piece = tile[8 * c : 8 * c + 8]
        turned = pltpu.roll(piece, (32 * c - 96) % 128, 1)
        last = jnp.where(lane // 32 == c, turned, last)
        rows.append(jnp.where(lane < 96, piece, 0.0))
    return jnp.concatenate(rows + [last], axis=0)


def spilled(ref, c, first=0):
    return both_layers(ref[first + c // 2].astype(F32))[c % 2]


U_ROW = 12 * 128


def middle_kernel(
    src_ref, up_ref, down_ref, m1_ref, p1_ref, m2_ref, p2_ref,
    pairs_ref, out_ref, rise_ref, sink_ref, sum_ref,
):
    total = None
    for ref, order in ((rise_ref, (3, 2, 1)), (sink_ref, (0, 1, 2))):
        for c in range(3):
            parts = split(src_ref[order[0], c])
            parts += tuple(src_ref[z, c].astype(BF16) for z in order[1:])
            for n in range(4):
                ref[128 * (3 * n + c) : 128 * (3 * n + c + 1), :] = parts[n]
    lane = iota((64, 128), 1)
    for c in range(3):
        m1, own, p1 = both_layers(m1_ref[c]), both_layers(up_ref[c]), both_layers(p1_ref[c])
        b = [
            m1[0] + spilled(m2_ref, c),
            m1[1] + spilled(down_ref, c, 3),
            own[0] + spilled(m1_ref, c, 3),
            own[1] + spilled(p1_ref, c, 3),
            p1[0] + spilled(up_ref, c, 3),
            p1[1] + spilled(p2_ref, c),
        ]
        for j in range(3):
            pairs_ref[j, c] = jnp.where(lane < 64, b[2 * j], b[2 * j + 1])
        u = [start_of(b[i], b[i - 1], b[i + 1], flat_ring, 1) for i in range(1, 5)]
        rows = slice(U_ROW + 64 * c, U_ROW + 64 * c + 64)
        rise_ref[rows, :] = jnp.where(lane < 64, u[0], u[1]).astype(BF16)
        sink_ref[rows, :] = jnp.where(lane < 64, u[2], u[3]).astype(BF16)
        left = [left_of(b[i + 1], u[i], u[i - 1], u[i + 1], flat_ring, 1) for i in (1, 2)]
        sum_ref[...] = left[0] + left[1]
        rows = sum_ref[pl.ds(0, 32, 2), :] + sum_ref[pl.ds(1, 32, 2), :]
        pool = jnp.where(
            lanes(lambda r, l: (r // 2 == (l & 31)) & (l // 32 == c) & (r < 64)), 0.125, 0.0
        )
        part = dot(rows, pool)
        total = part if total is None else total + part
    packed = jnp.concatenate(pack_coarse(total), axis=0)
    for d in range(out_ref.shape[0]):
        out_ref[d] = packed


def middle_down(source, up, down, m1, p1, m2, p2):
    return call(
        middle_kernel,
        (
            shaped((3, 3, 64, 128), F32),
            shaped((LOCAL, 24, 128), F32),
            shaped((U_ROW + 192, 128), BF16),
            shaped((U_ROW + 192, 128), BF16),
        ),
        None,
        [pltpu.VMEM((64, 128), F32)],
    )(*map(near, (source, up, down, m1, p1, m2, p2)))


def inner(x):
    return x[1:-1]


def coarse_part(me, blocks, lift_ref, window_ref, pool_ref, final_ref):
    parity = me % 2
    first = me % LOCAL - parity
    for n, ref in enumerate(blocks):
        window_ref[LOCAL * n : LOCAL * n + LOCAL] = ref[...].astype(F32)
    b2 = jnp.stack([unpack_coarse(window_ref[first + t]) for t in range(34)])
    group = iota((1, 128), 1) // 32
    lift = jnp.zeros((1, 128), F32)
    for c in range(3):
        lift = jnp.where(group == c, lift_ref[c : c + 1, :], lift)
    _, _, w3 = level(3)
    u2 = start_of(inner(b2), b2[:-2], b2[2:], group_ring, 2)
    r2 = left_of(b2[2:-2], inner(u2), u2[:-2], u2[2:], group_ring, 2)
    pairs = r2.reshape(15, 2, 32, 128)
    pool_ref[...] = (pairs[:, 0] + pairs[:, 1]).reshape(480, 128)
    rows = pool_ref[pl.ds(0, 240, 2), :] + pool_ref[pl.ds(1, 240, 2), :]
    pool = jnp.where(
        lanes(lambda r, l: ((r & 31) // 2 == (l & 15)) & (r // 32 == l // 32)), 0.125, 0.0
    )
    b3 = dot(rows, pool).reshape(15, 16, 128)
    u3 = w3 * b3
    for _ in range(5):
        b3 = inner(b3)
        u3 = sweep_of(b3, inner(u3), u3[:-2], u3[2:], group_ring, 3)
    u3 = (u3 + lift[None]).reshape(80, 128)
    spread = jnp.where(
        lanes(lambda r, l: ((l & 31) // 2 == (r & 31)) & (r // 32 == l // 32)), 1.0, 0.0
    )
    wide = dot(u3, spread)
    pool_ref[pl.ds(0, 80, 2), :] = wide
    pool_ref[pl.ds(1, 80, 2), :] = wide
    lifted = pool_ref[0:160, :].reshape(5, 1, 32, 128)
    u = (u2[11:21].reshape(5, 2, 32, 128) + lifted).reshape(10, 32, 128)
    u = sweep_of(b2[13:21], inner(u), u[:-2], u[2:], group_ring, 2)
    u = sweep_of(b2[14:20], inner(u), u[:-2], u[2:], group_ring, 2)
    final_ref[...] = u
    return jnp.concatenate([final_ref[parity + h] for h in range(5)], axis=0)


def up_kernel(
    me_ref, meta_ref, lift_ref, g0_ref, g1_ref, g2_ref, g3_ref, g4_ref,
    pairs_ref, low_ref, own_ref, high_ref, vel_ref, pay_ref,
    window_ref, pool_ref, final_ref, lift1_ref, b1_ref, u1_ref, v1_ref, lift0_ref, u0_ref,
    v0_ref, ext_ref, halo_ref,
):
    blocks = (g0_ref, g1_ref, g2_ref, g3_ref, g4_ref)
    coarse = coarse_part(me_ref[0], blocks, lift_ref, window_ref, pool_ref, final_ref)
    for c in range(3):
        spread = jnp.where(lanes(lambda r, l: r == 32 * c + (l & 63) // 2), 1.0, 0.0)
        wide = dot(coarse, spread)
        lift1_ref[c, pl.ds(0, 160, 2), :] = wide
        lift1_ref[c, pl.ds(1, 160, 2), :] = wide
    spread0 = jnp.where(lanes(lambda r, l: r == l // 2), 1.0, 0.0)

    def b_at(z, c):
        if 0 <= z < CZ:
            return own_ref[z, c]
        return halo_ref[z + 3 if z < 0 else z - 1]

    def component(c, carry):
        for ref, order in ((low_ref, (2, 1, 0)), (high_ref, (3, 4, 5))):
            planes = [
                ref[pl.ds(pl.multiple_of(128 * (3 * n + c), 128), 128), :].astype(F32)
                for n in range(4)
            ]
            halo_ref[order[0]] = planes[0] + planes[1]
            halo_ref[order[1]] = planes[2]
            halo_ref[order[2]] = planes[3]
        for j in range(3):
            b1_ref[2 * j], b1_ref[2 * j + 1] = both_layers(pairs_ref[j, c])
        rows = pl.ds(pl.multiple_of(U_ROW + 64 * c, 64), 64)
        u1 = list(both_layers(low_ref[rows, :].astype(F32)))
        for i in range(1, 5):
            u1.append(start_of(b1_ref[i], b1_ref[i - 1], b1_ref[i + 1], flat_ring, 1))
        u1.extend(both_layers(high_ref[rows, :].astype(F32)))
        for z in range(-3, 5):
            h = z // 2 + 2
            u1_ref[z + 3] = u1[z + 3] + lift1_ref[c, 64 * h : 64 * h + 64, :]
        for z in range(-2, 4):
            i = z + 3
            v1_ref[z + 2] = sweep_of(
                b1_ref[z + 2], u1_ref[i], u1_ref[i - 1], u1_ref[i + 1], flat_ring, 1
            )
        for z in range(-1, 3):
            i = z + 2
            value = sweep_of(
                b1_ref[z + 2], v1_ref[i], v1_ref[i - 1], v1_ref[i + 1], flat_ring, 1
            )
            wide = dot(value, spread0)
            lift0_ref[z + 1, pl.ds(0, 64, 2), :] = wide
            lift0_ref[z + 1, pl.ds(1, 64, 2), :] = wide
        for z in range(-2, 6):
            u0_ref[z + 2] = (
                start_of(b_at(z, c), b_at(z - 1, c), b_at(z + 1, c), flat_ring, 0)
                + lift0_ref[z // 2 + 1]
            )
        for z in range(-1, 5):
            i = z + 2
            v0_ref[z + 1] = sweep_of(
                b_at(z, c), u0_ref[i], u0_ref[i - 1], u0_ref[i + 1], flat_ring, 0
            )
        for z in range(CZ):
            i = z + 1
            value = sweep_of(
                own_ref[z, c], v0_ref[i], v0_ref[i - 1], v0_ref[i + 1], flat_ring, 0
            )
            vel_ref[z, c] = value
            rounded = value.astype(BF16).astype(F32)
            ext_ref[3 * z + c, 0:128, :] = rounded
            ext_ref[3 * z + c, 128:144, :] = rounded[0:16]
        return carry

    lax.fori_loop(0, 3, component, 0)
    lane = iota((8, 128), 1)
    sub = iota((8, 128), 0)

    part = [(lane // BOX) % CZ == k for k in range(CZ)]

    def gather(order, head, base_y):
        base_x = jnp.maximum(head - 1, 0)
        shift = base_x & 7
        row = pl.multiple_of(base_x - shift, 8)
        late = sub >= shift
        values = []
        for k in range(CZ):
            step = (HALF * order + BOX * k - base_y) & 127
            line = []
            for c in range(3):
                tiles = [ext_ref[3 * k + c, pl.ds(row + 8 * n, 8), :] for n in range(3)]
                for n in range(2):
                    value = jnp.where(late, tiles[n], tiles[n + 1])
                    line.append(pltpu.roll(value, step, 1))
            values.append(line)
        return (8 - shift) & 7, values

    group = together(pay_ref.shape[0], 32)

    def several(step, carry):
        found = []
        for n in range(group):
            for order in range(2):
                at = 8 * (step * group + n) + 4 * order
                found.append(gather(order, meta_ref[at], meta_ref[at + 1]))
        for n in range(group):
            pieces = []
            for m in range(6):
                both = []
                for order in range(2):
                    back, values = found[2 * n + order]
                    packed = values[0][m]
                    for k in range(1, CZ):
                        packed = jnp.where(part[k], values[k][m], packed)
                    both.append(pltpu.roll(packed, back, 0))
                pieces.append(jnp.where(lane < HALF, both[0], both[1]))
            pay_ref[step * group + n] = jnp.concatenate(pieces, axis=0).astype(BF16)
        return carry

    lax.fori_loop(0, pay_ref.shape[0] // group, several, 0)


def way_up(me, meta, lift, blocks, pairs, low, own, high, slots):
    return call(
        up_kernel,
        (
            shaped(own.shape, F32, False),
            shaped((slots, ROWS, 128), BF16),
        ),
        [SMEM, SMEM] + [VMEM] * 10,
        [
            pltpu.VMEM((5 * LOCAL, 24, 128), F32),
            pltpu.VMEM((480, 128), F32),
            pltpu.VMEM((6, 32, 128), F32),
            pltpu.VMEM((3, 320, 128), F32),
            pltpu.VMEM((6, 64, 128), F32),
            pltpu.VMEM((8, 64, 128), F32),
            pltpu.VMEM((6, 64, 128), F32),
            pltpu.VMEM((4, 128, 128), F32),
            pltpu.VMEM((8, 128, 128), F32),
            pltpu.VMEM((6, 128, 128), F32),
            pltpu.VMEM((12, 144, 128), F32),
            pltpu.VMEM((6, 128, 128), F32),
        ],
    )(me, meta, *map(near, (lift, *blocks, pairs, low, own, high)))


def read_kernel(dest_ref, pay_ref, pos_ref, out_ref, stage_ref, count_ref, wave_ref):
    slots = pay_ref.shape[0]

    def widen(t, carry):
        count_ref[t] = 0
        stage_ref[t] = pay_ref[t].astype(F32)
        return carry

    lax.fori_loop(0, slots, widen, 0, unroll=4)
    lane = iota((8, 128), 1)

    group = together(pos_ref.shape[1], 32)

    def one(first, n, target, order):
        block = first + n
        weight_x, weight_y, weight_z = box_weights(wave_ref, n)
        mine = lane // HALF == order
        left = []
        for m in range(6):
            packed = stage_ref[target, 8 * m : 8 * m + 8, :]
            left.append(jnp.where(mine, packed, pltpu.roll(packed, HALF, 1)))
        left = jnp.concatenate(left, axis=0).astype(BF16)
        right = jnp.concatenate(by_levels(weight_y, weight_z), axis=0)
        spread = lax.dot_general(
            left, right, (((1,), (0,)), ((), ())), preferred_element_type=F32
        )
        for c in range(3):
            value = spread[BOX * c : BOX * c + BOX] * weight_x
            out_ref[c, pl.ds(block, 1), :] = jnp.sum(value, axis=0, keepdims=True)

    def several(step, carry):
        places = []
        for n in range(group):
            target = dest_ref[0, step * group + n]
            order = count_ref[target]
            count_ref[target] = order + 1
            places.append((target, order))
        waves(pos_ref, step * group, group, wave_ref)
        for n in range(group):
            one(step * group, n, *places[n])
        return carry

    lax.fori_loop(0, pos_ref.shape[1] // group, several, 0)


def read(dest, payload, positions):
    slots = payload.shape[0]
    return call(
        read_kernel,
        shaped(positions.shape, F32, False),
        [SMEM, VMEM, VMEM],
        [
            pltpu.VMEM((slots, ROWS, 128), F32),
            pltpu.SMEM((slots,), jnp.int32),
            pltpu.VMEM((9, together(positions.shape[1], 32), 256), F32),
        ],
    )(far(dest), near(payload), near(positions))


def moved(value, step):
    size = lax.axis_size(AX)
    return lax.ppermute(value, AX, [(i, (i + step) % size) for i in range(size)])


def exchanged(value, axes=AX):
    return lax.all_to_all(value, axes, split_axis=0, concat_axis=0, tiled=True)


def shards(marker_positions, marker_forces, dest_slab, base_cells, fluid_source):
    slots = lax.axis_size(AX)
    positions = marker_positions.transpose(1, 0, 2)
    forces = marker_forces.transpose(1, 0, 2)
    dest = dest_slab.T
    me = lax.axis_index(AX).astype(jnp.int32).reshape(1)
    payload = exchanged(build(dest, base_cells.T, positions, forces, fluid_source, slots))
    meta = payload[:, 0:1, ::BOX].astype(jnp.int32).reshape(8 * slots)
    source, up, down, up2, down2, lift = place(meta, payload, fluid_source)
    m1, m2 = moved(up, 1), moved(up2, 2)
    p1, p2 = moved(down, -1), moved(down2, -2)
    pairs, share, rise, sink = middle_down(source, up, down, m1, p1, m2, p2)
    middle = exchanged(share, AX[1])
    low, high = moved(rise, 1), moved(sink, -1)
    away = middle.astype(BF16)
    above = [moved(middle, -LOCAL), moved(away, -2 * LOCAL)]
    below = [moved(away, 2 * LOCAL), moved(middle, LOCAL)]
    blocks = [*below, middle, *above]
    velocity, picked = way_up(me, meta, lift, blocks, pairs, low, source, high, slots)
    out = read(dest, exchanged(picked), positions)
    return velocity, out.transpose(1, 0, 2)


def solution(mesh):
    torus = Mesh(mesh.devices.reshape(-1, LOCAL), AX)
    return jax.shard_map(
        shards,
        mesh=torus,
        in_specs=(P(AX), P(AX), P(AX), P(AX), P(AX)),
        out_specs=(P(AX), P(AX)),
        check_vma=False,
    )
```
